32 devices in a mesh: grp: 4 (over x, core), gx: 2 (over y), gy: 4 (over z).
Axes of the slice: x: 2, y: 2, z: 4, core: 2. Of those that a mesh axis runs over, the one named last changes fastest.
Arguments:
- pressure: float32 [24, 128, 1024], P(None, ('grp', 'gy'), 'gx'), may hold values from -2 to 0.2
- soil_class: int32 [24, 128, 1024], P(None, ('grp', 'gy'), 'gx'), may hold values from 0 to 11
- capacity_range: float32 [12], replicated, may hold values from 0.25 to 0.45
- inverse_entry: float32 [12], replicated, may hold values from 0.3 to 3
- shape_index: float32 [12], replicated, may hold values from 1.3 to 2.5
- conductivity: float32 [12], replicated, may hold values from 0.05 to 1
- depth: float32 [128, 1024], P('grp', ('gx', 'gy')), may hold values from 0 to 2
- elevation: float32 [128, 1024], P('grp', ('gx', 'gy')), may hold values from -4 to 4
- roughness: float32 [128, 1024], P('grp', ('gx', 'gy')), may hold values from 2 to 8
- rain: float32 [128, 1024], P('grp', ('gx', 'gy')), may hold values from 0.1 to 1
- land_mask: int32 [128, 1024], P('grp', ('gx', 'gy')), may hold values 0 or 1
- channel_mask: int32 [128, 1024], P('grp', ('gx', 'gy')), may hold values 0 or 1
Outputs:
- head: float32 [24, 128, 1024], P(None, ('grp', 'gy'), 'gx')
- water: float32 [128, 1024], P('grp', ('gx', 'gy'))
The draws below stay inside these ranges and needn't reach their ends.
All inputs are finite; a program needn't handle non-finite values. No bound on the sum of `land_mask` or of `channel_mask` on one device may be relied on, other than what follows from the above.
Results may differ from the reference program's by a relative error of at most 0.0003.
Values sent between devices are 32-bit elements; how exact they have to be, the bound alone decides.
No kernel may reach another device: no remote copies, remote signals or barrier semaphores. Data moves between devices by JAX's collectives and lax.ppermute only.
A program may use at most 64 MiB of HBM per device.

```python
import math
import jax
import jax.numpy as jnp

NZ = 24
NCLASS = 12
SWEEPS = 2
PASSES = 3
NX = 128
NY = 1024


def touch_ends(entries, key, low, top_value):
    longest = entries.shape.index(max(entries.shape))
    spots = []
    for shift in (0, 1):
        where = [jax.random.randint(jax.random.fold_in(key, axis), (), 0, length) for axis, length in enumerate(entries.shape)]
        where[longest] = (where[longest] + shift) % entries.shape[longest]
        spots.append(tuple(where))
    return entries.at[spots[0]].set(low).at[spots[1]].set(top_value)


def shard_levels(rng, shape, pieces, smallest, largest):
    level, own = 1.0, jax.random.fold_in(rng, 6)
    for dim, shards_of in pieces:
        heights = jnp.exp(jax.random.uniform(jax.random.fold_in(own, dim), (shards_of,), jnp.float32, smallest / len(pieces), largest / len(pieces)))
        level = level * jnp.repeat(heights, shape[dim] // shards_of).reshape([-1 if axis == dim else 1 for axis in range(len(shape))])
    return level


def scatter_about(own_key, extent, scale, reach, cuts=(), kind=jnp.bfloat16):
    level = shard_levels(own_key, extent, cuts, -0.22, 0.18) if cuts else 1.0
    drawn = jax.random.normal(own_key, extent, jnp.float32) * scale * level
    return jnp.minimum(jnp.maximum(drawn, -reach), reach).astype(kind)


def setup_inputs(seed: int = 0) -> dict:
    key_list = jax.random.split(jax.random.key(seed), 13)
    pressure = jnp.clip(-2.0 + 2.2 * jax.random.uniform(key_list[0], (NZ, NX, NY), jnp.float32) ** shard_levels(key_list[0], (NZ, NX, NY), ((1, 16), (2, 2)), -0.2, 0.2), -2.0, 0.2)
    soil_class = touch_ends(jax.random.randint(key_list[1], (NZ, NX, NY), 0, NCLASS), jax.random.fold_in(key_list[1], 1), 0, NCLASS - 1).astype(jnp.int32)
    capacity_range = jnp.clip(jax.random.uniform(key_list[2], (NCLASS,), jnp.float32, 0.25, 0.45), 0.25, 0.45)
    inverse_entry = jnp.clip(jnp.exp(jax.random.uniform(key_list[3], (NCLASS,), jnp.float32, math.log(0.3), math.log(3.0))), 0.3, 3.0)
    shape_index = jnp.clip(jax.random.uniform(key_list[4], (NCLASS,), jnp.float32, 1.3, 2.5), 1.3, 2.5)
    conductivity = jnp.clip(jnp.exp(jax.random.uniform(key_list[5], (NCLASS,), jnp.float32, math.log(0.05), math.log(1.0))), 0.05, 1.0)
    depth = jnp.clip(2.0 * jax.random.uniform(key_list[6], (NX, NY), jnp.float32) ** shard_levels(key_list[6], (NX, NY), ((0, 4), (1, 8)), -0.2, 0.2), 0.0, 2.0)
    elevation = scatter_about(key_list[7], (NX, NY), 1.0, 4.0, ((0, 4), (1, 8)), jnp.float32)
    roughness = jnp.clip(jnp.exp(math.log(8.0) - 1.3862944 * jax.random.uniform(key_list[8], (NX, NY), jnp.float32) ** shard_levels(key_list[8], (NX, NY), ((0, 4), (1, 8)), -0.2, 0.2)), 2.0, 8.0)
    rain = jnp.clip(jnp.exp(math.log(1.0) - 2.3025851 * jax.random.uniform(key_list[9], (NX, NY), jnp.float32) ** shard_levels(key_list[9], (NX, NY), ((0, 4), (1, 8)), -0.2, 0.2)), 0.1, 1.0)
    land_mask = touch_ends((jax.random.randint(key_list[10], (NX, NY), 0, 5) < 4).astype(jnp.int32), jax.random.fold_in(key_list[10], 1), 0, 1)
    channel_mask = touch_ends((jax.random.randint(key_list[11], (NX, NY), 0, 8) < 1).astype(jnp.int32), jax.random.fold_in(key_list[11], 1), 0, 1)
    return {"pressure": pressure, "soil_class": soil_class, "capacity_range": capacity_range, "inverse_entry": inverse_entry, "shape_index": shape_index, "conductivity": conductivity, "depth": depth, "elevation": elevation, "roughness": roughness, "rain": rain, "land_mask": land_mask, "channel_mask": channel_mask}


STORAGE = 0.01
LATERAL = 4.0
VERTICAL = 4.0
GRAVITY_STEP = 0.5
SUCTION_FLOOR = 0.01
SLOPE_FLOOR = 0.1
SURFACE_STEP = 0.3
LEAKANCE = 0.5
SOURCE_GAIN = 1.0

def lookup(soil_class, tables):
    results = []
    for table in tables:
        filled = jnp.zeros(soil_class.shape, table.dtype)
        for kind_number in range(table.shape[0]):
            filled = jnp.where(soil_class == kind_number, table[kind_number], filled)
        results.append(filled)
    return results

def closures(pressure, capacity_range, inverse_entry, pore_index, conductivity):
    exponent = 1.0 / (1.0 - pore_index)
    scaled = jnp.maximum(-inverse_entry * pressure, SUCTION_FLOOR)
    log_scaled = jnp.log(scaled)
    log_sum = jnp.log1p(jnp.exp(exponent * log_scaled))
    saturation = jnp.exp(-pore_index * log_sum)
    content = capacity_range * saturation
    capacity = STORAGE + capacity_range * pore_index * exponent * inverse_entry * jnp.exp((exponent - 1.0) * log_scaled - (pore_index + 1.0) * log_sum)
    conduct = conductivity * jnp.sqrt(saturation) * jnp.square(1.0 - jnp.exp(pore_index * (exponent * log_scaled - log_sum)))
    return (content, capacity, conduct)

def update_cells(padded, conduct_pad, capacity, content_gap, source):
    layers = padded.shape[0] - 2
    rows = padded.shape[1] - 2
    cols = padded.shape[2] - 2
    center = padded[1:-1, 1:-1, 1:-1]
    own_conduct = conduct_pad[1:-1, 1:-1, 1:-1]
    numerator = capacity * center - content_gap
    denominator = capacity
    neighbours = ((1, 0, 1, LATERAL, 0.0), (1, 2, 1, LATERAL, 0.0), (1, 1, 0, LATERAL, 0.0), (1, 1, 2, LATERAL, 0.0), (0, 1, 1, VERTICAL, GRAVITY_STEP), (2, 1, 1, VERTICAL, -GRAVITY_STEP))
    for first, second, third, weight, offset in neighbours:
        beside = padded[first:first + layers, second:second + rows, third:third + cols]
        beside_conduct = conduct_pad[first:first + layers, second:second + rows, third:third + cols]
        face_weight = weight * jnp.sqrt(own_conduct * beside_conduct)
        numerator = numerator + face_weight * (beside + offset)
        denominator = denominator + face_weight
    gained = jnp.concatenate([(SOURCE_GAIN * source)[None], jnp.zeros((layers - 1, rows, cols), source.dtype)], axis=0)
    numerator = numerator + gained
    return numerator / denominator

def face_flux(upper_level, lower_level, upper_depth, lower_depth, upper_convey, lower_convey):
    slope = upper_level - lower_level
    upwind = jnp.where(slope >= 0, upper_depth, lower_depth)
    carried = upwind * jnp.cbrt(upwind * upwind)
    return jnp.sqrt(upper_convey * lower_convey) * carried * slope / jnp.sqrt(jnp.maximum(jnp.abs(slope), SLOPE_FLOOR))

def overland(depth_pad, level_pad, convey_pad, leak, top, rain):
    current = depth_pad[1:-1, 1:-1]
    surface = level_pad + depth_pad
    across = face_flux(surface[:-1, 1:-1], surface[1:, 1:-1], depth_pad[:-1, 1:-1], depth_pad[1:, 1:-1], convey_pad[:-1, 1:-1], convey_pad[1:, 1:-1])
    along = face_flux(surface[1:-1, :-1], surface[1:-1, 1:], depth_pad[1:-1, :-1], depth_pad[1:-1, 1:], convey_pad[1:-1, :-1], convey_pad[1:-1, 1:])
    outflow = across[1:] - across[:-1] + (along[:, 1:] - along[:, :-1])
    rate = leak * (current - top)
    return (jnp.maximum(current + SURFACE_STEP * (rain - rate - outflow), 0.0), rate)

def reference(pressure, soil_class, capacity_range, inverse_entry, shape_index, conductivity, depth, elevation, roughness, rain, land_mask, channel_mask):
    pore_table = 1.0 - 1.0 / shape_index
    range_cells, entry_cells, pore_cells, conduct_cells = lookup(soil_class, (capacity_range, inverse_entry, pore_table, conductivity))
    content0, capacity, conduct = closures(pressure, range_cells, entry_cells, pore_cells, conduct_cells)
    top = pressure[0]
    leak = LEAKANCE * land_mask.astype(jnp.float32) * conduct[0]
    convey = (1.0 + channel_mask.astype(jnp.float32)) / roughness
    level_pad = jnp.pad(elevation, 1)
    convey_pad = jnp.pad(convey, 1)
    water = depth
    exchange = jnp.zeros_like(depth)
    for pass_number in range(PASSES):
        water, rate = overland(jnp.pad(water, 1), level_pad, convey_pad, leak, top, rain)
        exchange = exchange + SURFACE_STEP * rate
    head = pressure
    content = content0
    for sweep_number in range(SWEEPS):
        head = update_cells(jnp.pad(head, 1), jnp.pad(conduct, 1), capacity, content - content0, exchange)
        if sweep_number + 1 < SWEEPS:
            content, capacity, conduct = closures(head, range_cells, entry_cells, pore_cells, conduct_cells)
    return (head, water)
```

```python
import jax
import jax.numpy as jnp
from jax import lax
from jax.experimental import pallas as pl
from jax.experimental.pallas import tpu as pltpu
from jax.sharding import PartitionSpec as P

PASSES = 3
STORAGE = 0.01
GRAVITY_STEP = 0.5
SUCTION_FLOOR = 0.01
SLOPE_FLOOR = 0.1
SURFACE_STEP = 0.3
LEAKANCE = 0.5

LANES = 128
SUBS = 8
TOP_LAYERS = 4


def shift(x, axis, step):
    size = lax.axis_size(axis)
    return lax.ppermute(x, axis, [(i, (i + step) % size) for i in range(size)])


def class_tables(capacity_range, inverse_entry, shape_index, conductivity):
    pore = 1.0 - 1.0 / shape_index
    expo = 1.0 / (1.0 - pore)
    rows = [
        -inverse_entry,
        expo,
        pore,
        capacity_range,
        2.0 * jnp.sqrt(conductivity),
        capacity_range * pore * expo * inverse_entry,
        conductivity,
        expo - 1.0,
    ]
    return jnp.pad(jnp.stack(rows), ((0, 0), (0, LANES - shape_index.shape[0])))


def pick(tab_ref, row, idx):
    table = jnp.broadcast_to(tab_ref[row : row + 1, :], idx.shape)
    return jnp.take_along_axis(table, idx, axis=1, mode="promise_in_bounds")


def closure(tab_ref, idx, p):
    logs = jnp.log2(jnp.maximum(pick(tab_ref, 0, idx) * p, SUCTION_FLOOR))
    grown = 1.0 + jnp.exp2(pick(tab_ref, 1, idx) * logs)
    drop = pick(tab_ref, 2, idx) * jnp.log2(grown)
    content = pick(tab_ref, 3, idx) * jnp.exp2(-drop)
    ratio = jnp.exp2(pick(tab_ref, 7, idx) * logs - drop)
    capacity = STORAGE + pick(tab_ref, 5, idx) * ratio / grown
    root = pick(tab_ref, 4, idx) * jnp.exp2(-0.25 * drop) * jnp.abs(1.0 - ratio)
    return content, capacity, root


def lateral(x):
    rows, width = x.shape
    return (
        pltpu.roll(x, 1, 0)
        + pltpu.roll(x, rows - 1, 0)
        + pltpu.roll(x, 1, 1)
        + pltpu.roll(x, width - 1, 1)
    )


def chunks(width):
    return [slice(i, i + LANES) for i in range(0, width, LANES)]


def soil_mask(flags_ref, rows, width, own_rows, own_cols):
    r = lax.broadcasted_iota(jnp.int32, (rows, width), 0)
    c = lax.broadcasted_iota(jnp.int32, (rows, width), 1)
    above = jnp.where(r >= rows - 2, flags_ref[0], 0)
    below = jnp.where((r >= own_rows) & (r < own_rows + 2), flags_ref[1], 0)
    left = jnp.where(c >= width - 2, flags_ref[2], 0)
    right = jnp.where((c >= own_cols) & (c < own_cols + 2), flags_ref[3], 0)
    in_rows = jnp.where(r < own_rows, 1, above + below)
    in_cols = jnp.where(c < own_cols, 1, left + right)
    return (in_rows * in_cols).astype(jnp.float32)


def soil_sweeps(layers, p_ref, c_ref, tab_ref, mask_ref, s, gain, out):
    _, rows, width = p_ref.shape
    h_ref, q_ref, n_ref, d_ref, h2_ref, q2_ref, n2_ref, d2_ref, k_ref = s
    zero = jnp.zeros((rows, width), jnp.float32)
    for ref in (h_ref, q_ref, h2_ref, q2_ref):
        ref[0] = zero
        ref[layers + 1] = zero

    def first(z, carry):
        for ch in chunks(width):
            p = p_ref[z, :, ch]
            content, capacity, root = closure(tab_ref, c_ref[z, :, ch], p)
            root = root * mask_ref[:, ch]
            h_ref[z + 1, :, ch] = root
            q_ref[z + 1, :, ch] = root * p
            n_ref[z, :, ch] = capacity * p
            d_ref[z, :, ch] = capacity
            k_ref[z, :, ch] = content
        return carry

    lax.fori_loop(0, layers, first, 0)

    def sums(z, h, q):
        mid, over, under = h[z + 1], h[z], h[z + 2]
        weights = lateral(mid) + over + under
        flows = lateral(q[z + 1]) + q[z] + q[z + 2] + GRAVITY_STEP * (over - under)
        return mid, weights, flows

    def second(z, carry):
        mid, weights, flows = sums(z, h_ref, q_ref)
        top = n_ref[z] + mid * flows
        if gain is not None:
            top = top + jnp.where(z == 0, 1.0, 0.0) * gain
        q2_ref[z + 1] = top / (d_ref[z] + mid * weights)
        for ch in chunks(width):
            p = q2_ref[z + 1, :, ch]
            content, capacity, root = closure(tab_ref, c_ref[z, :, ch], p)
            root = root * mask_ref[:, ch]
            h2_ref[z + 1, :, ch] = root
            q2_ref[z + 1, :, ch] = root * p
            n2_ref[z, :, ch] = capacity * p - (content - k_ref[z, :, ch])
            d2_ref[z, :, ch] = capacity
        return carry

    lax.fori_loop(0, layers, second, 0)

    def third(z, carry):
        mid, weights, flows = sums(z, h2_ref, q2_ref)
        top = n2_ref[z] + mid * flows
        if gain is not None:
            top = top + jnp.where(z == 0, 1.0, 0.0) * gain
        out(z, top / (d2_ref[z] + mid * weights))
        return carry

    return third


def soil_scratch(layers, rows, width):
    tall = pltpu.VMEM((layers + 2, rows, width), jnp.float32)
    flat = pltpu.VMEM((layers, rows, width), jnp.float32)
    return [tall, tall, flat, flat, tall, tall, flat, flat, flat]


def soil_kernel(flags_ref, tab_ref, p_in, c_in, up_in, down_in, left_in, right_in, out_ref, pe_out, ce_out, pe, ce, mask_ref, *s):
    layers, own, cols = p_in.shape
    _, rows, width = pe.shape
    lane = lax.broadcasted_iota(jnp.int32, (rows, LANES), 1)
    pad = jnp.zeros((rows - own, cols), jnp.float32)

    def build(z, carry):
        for f, (src, dst) in enumerate(((p_in, pe), (c_in, ce))):
            kind = dst.dtype
            dst[z, own:, :cols] = pad.astype(kind)
            dst[z, :own, :cols] = src[z]
            dst[z, own : own + 2, :cols] = down_in[f, z].astype(kind)
            dst[z, rows - 2 :, :cols] = up_in[f, z].astype(kind)
            edge = jnp.zeros((rows, LANES), jnp.float32)
            for col in range(2):
                edge = jnp.where(lane == col, pltpu.roll(right_in[f, col], (LANES + col - z) % LANES, 1), edge)
                spot = LANES - 2 + col
                edge = jnp.where(lane == spot, pltpu.roll(left_in[f, col], (LANES + spot - z) % LANES, 1), edge)
            dst[z, :, cols:] = edge.astype(kind)
        return carry

    lax.fori_loop(0, layers, build, 0)
    mask_ref[...] = soil_mask(flags_ref, rows, width, own, cols)

    def out(z, p):
        out_ref[z] = p[:own, :cols]

    third = soil_sweeps(layers, pe, ce, tab_ref, mask_ref, s, None, out)
    lax.fori_loop(0, layers, third, 0)
    pe_out[...] = pe[:TOP_LAYERS]
    ce_out[...] = ce[:TOP_LAYERS]


def soil_interior(flags, tables, pressure, soil_class, up, down, left, right):
    layers, own, cols = pressure.shape
    rows, width = own + SUBS, cols + LANES
    return pl.pallas_call(
        soil_kernel,
        out_shape=(
            jax.ShapeDtypeStruct(pressure.shape, jnp.float32),
            jax.ShapeDtypeStruct((TOP_LAYERS, rows, width), jnp.float32),
            jax.ShapeDtypeStruct((TOP_LAYERS, rows, width), jnp.int32),
        ),
        in_specs=[pl.BlockSpec(memory_space=pltpu.SMEM)] + [pl.BlockSpec(memory_space=pltpu.VMEM)] * 7,
        out_specs=[pl.BlockSpec(memory_space=pltpu.VMEM)] * 3,
        scratch_shapes=[
            pltpu.VMEM((layers, rows, width), jnp.float32),
            pltpu.VMEM((layers, rows, width), jnp.int32),
            pltpu.VMEM((rows, width), jnp.float32),
        ]
        + soil_scratch(layers, rows, width),
        name="soil_interior",
    )(flags, tables, pressure, soil_class, up, down, left, right)


def last_kernel(
    spot_ref, flags_ref, tab_ref, surf_ref, tops_ref, pe, ce, head_in, head_out, water_ref,
    ex_ref, w_ref, mask_ref, new_ref, sem, *s, own, own_rows, own_cols,
):
    del head_in
    _, rows, width = surf_ref.shape
    block_rows, block_cols = rows - SUBS, width - LANES
    r = lax.broadcasted_iota(jnp.int32, (rows, width), 0)
    c = lax.broadcasted_iota(jnp.int32, (rows, width), 1)
    row_ok = jnp.where(r < block_rows, 1, jnp.where(r >= rows - 3, spot_ref[2], jnp.where(r < block_rows + 3, spot_ref[3], 0)))
    col_ok = jnp.where(c < block_cols, 1, jnp.where(c >= width - 3, flags_ref[2], jnp.where(c < block_cols + 3, flags_ref[3], 0)))
    inside = (row_ok * col_ok).astype(jnp.float32)
    level = surf_ref[1]
    convey = jnp.sqrt(surf_ref[2]) * inside
    leak = surf_ref[3]
    rain = surf_ref[4]
    top = tops_ref[0]

    def across(x):
        return pltpu.roll(x, rows - 1, 0)

    def along(x):
        return pltpu.roll(x, width - 1, 1)

    gates = [convey * across(convey), convey * along(convey)]
    parts = []
    for ch in chunks(width):
        _, _, root = closure(tab_ref, tops_ref[1, :, ch].astype(jnp.int32), top[:, ch])
        parts.append(0.25 * root * root)
    leak = leak * jnp.concatenate(parts, axis=1)
    water = surf_ref[0]
    exchange = jnp.zeros_like(water)
    for _ in range(PASSES):
        surface = level + water
        power = jnp.where(water > 0.0, jnp.exp2((5.0 / 3.0) * jnp.log2(jnp.maximum(water, 1e-30))), 0.0)
        outflow = jnp.zeros_like(water)
        for axis, gate, beside in ((0, gates[0], across), (1, gates[1], along)):
            slope = surface - beside(surface)
            carried = jnp.where(slope >= 0.0, power, beside(power))
            flux = gate * carried * slope * lax.rsqrt(jnp.maximum(jnp.abs(slope), SLOPE_FLOOR))
            outflow = outflow + flux - pltpu.roll(flux, 1, axis)
        rate = leak * (water - top)
        exchange = exchange + SURFACE_STEP * rate
        water = jnp.maximum(water + SURFACE_STEP * (rain - rate - outflow), 0.0)
    ex_ref[...] = exchange
    w_ref[...] = water
    water_ref[...] = w_ref[:block_rows, :block_cols]
    first = pl.multiple_of(spot_ref[0], SUBS)
    after = pl.multiple_of(spot_ref[0] + own, SUBS)
    before = pl.multiple_of(spot_ref[1], SUBS)
    sub = lax.broadcasted_iota(jnp.int32, (SUBS, width), 0)
    rim = jnp.where(sub == SUBS - 1, ex_ref[pl.ds(before, SUBS), :], jnp.where(sub == 0, ex_ref[pl.ds(after, SUBS), :], 0.0))
    gain = jnp.concatenate([ex_ref[pl.ds(first, own), :], rim], axis=0)
    mask_ref[...] = soil_mask(flags_ref, own + SUBS, width, own, block_cols)

    def out(z, p):
        new_ref[z] = p[:own, :block_cols]

    third = soil_sweeps(TOP_LAYERS, pe, ce, tab_ref, mask_ref, s, gain, out)
    lax.fori_loop(0, TOP_LAYERS - 2, third, 0)
    copy = pltpu.make_async_copy(new_ref, head_out.at[: TOP_LAYERS - 2], sem)
    copy.start()
    copy.wait()


def finish(spot, flags, tables, surf, tops, pe, ce, head):
    _, rows, width = surf.shape
    own = head.shape[1]
    block = (rows - SUBS, width - LANES)

    def body(*refs):
        last_kernel(*refs, own=own, own_rows=block[0], own_cols=block[1])

    vmem = pl.BlockSpec(memory_space=pltpu.VMEM)
    smem = pl.BlockSpec(memory_space=pltpu.SMEM)
    return pl.pallas_call(
        body,
        out_shape=(
            jax.ShapeDtypeStruct(head.shape, jnp.float32),
            jax.ShapeDtypeStruct(block, jnp.float32),
        ),
        in_specs=[smem, smem] + [vmem] * 5 + [pl.BlockSpec(memory_space=pl.ANY)],
        out_specs=[pl.BlockSpec(memory_space=pl.ANY), vmem],
        scratch_shapes=[
            pltpu.VMEM((rows, width), jnp.float32),
            pltpu.VMEM((rows, width), jnp.float32),
            pltpu.VMEM((own + SUBS, width), jnp.float32),
            pltpu.VMEM((TOP_LAYERS - 2, own, block[1]), jnp.float32),
            pltpu.SemaphoreType.DMA,
        ]
        + soil_scratch(TOP_LAYERS, own + SUBS, width),
        input_output_aliases={7: 0},
        name="surface_and_top",
    )(spot, flags, tables, surf, tops, pe, ce, head)


def lane_rows(size):
    return -(-size // LANES)


def as_lanes(x):
    if x.shape[-1] % LANES:
        x = jnp.pad(x.reshape(-1), (0, -x.size % LANES))
    return x.reshape(-1, LANES)


def from_lanes(x, shape):
    if shape[-1] % LANES:
        size = 1
        for length in shape:
            size *= length
        x = x.reshape(-1)[:size]
    return x.reshape(shape)


def gx_trade(right, left):
    if lax.axis_size("gx") == 2:
        got = shift(jnp.where(lax.axis_index("gx") == 0, right, left), "gx", 1)
        return got, got
    return shift(right, "gx", 1), shift(left, "gx", -1)


def cyclic_rows(mid, above, below, gap):
    hole = jnp.zeros(mid.shape[:-2] + (gap, mid.shape[-1]), mid.dtype)
    return jnp.concatenate([mid, below, hole, above], axis=-2)


def local(
    pressure, soil_class, capacity_range, inverse_entry, shape_index, conductivity,
    depth, elevation, roughness, rain, land_mask, channel_mask,
):
    ng, nx, ny = (lax.axis_size(a) for a in ("grp", "gx", "gy"))
    ig, ix, iy = (lax.axis_index(a) for a in ("grp", "gx", "gy"))
    layers, own, cols = pressure.shape
    srows, scols = depth.shape
    tables = class_tables(capacity_range, inverse_entry, shape_index, conductivity)
    convey = (1.0 + channel_mask.astype(jnp.float32)) / roughness
    surf = jnp.stack([depth, elevation, convey, LEAKANCE * land_mask.astype(jnp.float32), rain])
    cells = soil_class.astype(jnp.float32)
    tops = jnp.stack([pressure[0], cells[0]])
    both = jnp.stack([pressure, cells])

    def pack(s, t):
        return jnp.concatenate([as_lanes(s), as_lanes(t)], axis=0)

    def unpack(m):
        cut = lane_rows(15 * scols)
        return from_lanes(m[:cut], (5, 3, scols)), from_lanes(m[cut:], (2, 2, cols))

    s_above, t_above = unpack(shift(pack(surf[:, -3:], tops[:, -2:]), "grp", 1))
    s_below, t_below = unpack(shift(pack(surf[:, :3], tops[:, :2]), "grp", -1))
    up = shift(both[:, :, -2:], ("grp", "gy"), 1)
    down = shift(both[:, :, :2], ("grp", "gy"), -1)

    surf_rows = cyclic_rows(surf, s_above, s_below, 2)
    tops_rows = jnp.concatenate([tops, t_below, t_above], axis=1)

    def edges(cut):
        a = surf_rows[:, :, cut(3)].transpose(0, 2, 1).reshape(15, -1)
        b = tops_rows[:, :, cut(2)].transpose(0, 2, 1).reshape(4, -1)
        return a, b

    def pack2(a, b):
        return jnp.concatenate([a, jnp.pad(b, ((0, 0), (0, a.shape[1] - b.shape[1])))], axis=0)

    m_left, m_right = gx_trade(pack2(*edges(lambda n: slice(-n, None))), pack2(*edges(lambda n: slice(0, n))))

    mine = jnp.concatenate(
        [
            as_lanes(surf_rows),
            as_lanes(tops_rows),
            jnp.pad(jnp.concatenate([m_left, m_right]), ((0, 0), (0, -m_left.shape[1] % LANES))).reshape(-1, LANES),
        ]
    )
    every = lax.all_gather(mine, "gy", axis=0, tiled=False)
    n1 = lane_rows(surf_rows.size)
    n2 = n1 + lane_rows(tops_rows.size)
    e_surf = jax.vmap(lambda m: from_lanes(m, (5, srows + SUBS, scols)))(every[:, :n1]).transpose(1, 2, 0, 3).reshape(5, srows + SUBS, ny * scols)
    e_tops = every[:, n1:n2].reshape(ny, 2, own + 4, cols)
    e_m = every[:, n2:].reshape(ny, 2, 19, -1)
    main = e_tops[:, :, :own].transpose(1, 0, 2, 3).reshape(2, srows, cols)
    zeros = jnp.zeros((2, 4, cols), jnp.float32)
    f_tops = jnp.concatenate([main, e_tops[0, :, own : own + 2], zeros, e_tops[-1, :, own + 2 :]], axis=1)

    height = srows + SUBS
    c_left = e_m[-1, 0, :15, :height].reshape(5, 3, height).transpose(0, 2, 1)
    c_right = e_m[0, 1, :15, :height].reshape(5, 3, height).transpose(0, 2, 1)
    hole = jnp.zeros((5, height, LANES - 6), jnp.float32)
    blocks = jnp.concatenate([e_surf, c_right, hole, c_left], axis=2)

    def tops_edge(side):
        t = e_m[:, side, 15:, : own + 4].reshape(ny, 2, 2, own + 4)
        mid = t[..., :own].transpose(1, 0, 3, 2).reshape(2, srows, 2)
        low = t[0, :, :, own : own + 2].transpose(0, 2, 1)
        high = t[-1, :, :, own + 2 :].transpose(0, 2, 1)
        return jnp.concatenate([mid, low, jnp.zeros((2, 4, 2), jnp.float32), high], axis=1)

    top_blocks = jnp.concatenate(
        [f_tops, tops_edge(1), jnp.zeros((2, height, LANES - 4), jnp.float32), tops_edge(0)], axis=2
    )

    soil_rows = cyclic_rows(both, up, down, SUBS - 4)

    def soil_edge(cut):
        a = soil_rows[:, :, :, cut].transpose(0, 3, 2, 1)
        return jnp.pad(a, ((0, 0), (0, 0), (0, 0), (0, LANES - layers)))

    left, right = gx_trade(soil_edge(slice(-2, None)), soil_edge(slice(0, 2)))

    tile = ig * ny + iy
    flags = jnp.stack([tile > 0, tile < ng * ny - 1, ix > 0, ix < nx - 1]).astype(jnp.int32)
    spot = jnp.stack([iy * own, jnp.where(iy > 0, iy * own - SUBS, srows), (ig > 0).astype(jnp.int32), (ig < ng - 1).astype(jnp.int32)])
    head, pe, ce = soil_interior(flags, tables, pressure, soil_class, up, down, left, right)
    head, water = finish(spot, flags, tables, blocks, top_blocks, pe, ce, head)
    return head, lax.dynamic_slice_in_dim(water, iy * scols, scols, axis=1)


def solution(mesh):
    soil = P(None, ("grp", "gy"), "gx")
    ground = P("grp", ("gx", "gy"))
    return jax.shard_map(
        local,
        mesh=mesh,
        in_specs=(soil, soil, P(), P(), P(), P()) + (ground,) * 6,
        out_specs=(soil, ground),
        check_vma=False,
    )
```

```python
import jax
import jax.numpy as jnp
from jax import lax
from jax.experimental import pallas as pl
from jax.experimental.pallas import tpu as pltpu
from jax.sharding import PartitionSpec as P

PASSES = 3
STORAGE = 0.01
GRAVITY_STEP = 0.5
SUCTION_FLOOR = 0.01
SLOPE_FLOOR = 0.1
SURFACE_STEP = 0.3
LEAKANCE = 0.5

LANES = 128
SUBS = 8
TOP_LAYERS = 4


def shift(x, axis, step):
    size = lax.axis_size(axis)
    return lax.ppermute(x, axis, [(i, (i + step) % size) for i in range(size)])


def class_tables(capacity_range, inverse_entry, shape_index, conductivity):
    pore = 1.0 - 1.0 / shape_index
    expo = 1.0 / (1.0 - pore)
    rows = [
        -inverse_entry,
        expo,
        pore,
        capacity_range,
        2.0 * jnp.sqrt(conductivity),
        capacity_range * pore * expo * inverse_entry,
        conductivity,
        expo - 1.0,
    ]
    return jnp.pad(jnp.stack(rows), ((0, 0), (0, LANES - shape_index.shape[0])))


def pick(tab_ref, row, idx):
    table = jnp.broadcast_to(tab_ref[row : row + 1, :], idx.shape)
    return jnp.take_along_axis(table, idx, axis=1, mode="promise_in_bounds")


def closure(tab_ref, idx, p):
    logs = jnp.log2(jnp.maximum(pick(tab_ref, 0, idx) * p, SUCTION_FLOOR))
    grown = 1.0 + jnp.exp2(pick(tab_ref, 1, idx) * logs)
    drop = pick(tab_ref, 2, idx) * jnp.log2(grown)
    content = pick(tab_ref, 3, idx) * jnp.exp2(-drop)
    ratio = jnp.exp2(pick(tab_ref, 7, idx) * logs - drop)
    capacity = STORAGE + pick(tab_ref, 5, idx) * ratio / grown
    root = pick(tab_ref, 4, idx) * jnp.exp2(-0.25 * drop) * jnp.abs(1.0 - ratio)
    return content, capacity, root


def lateral(x):
    rows, width = x.shape
    return (
        pltpu.roll(x, 1, 0)
        + pltpu.roll(x, rows - 1, 0)
        + pltpu.roll(x, 1, 1)
        + pltpu.roll(x, width - 1, 1)
    )


def chunks(width):
    return [slice(i, i + LANES) for i in range(0, width, LANES)]


def soil_mask(flags_ref, rows, width, own_rows, own_cols):
    r = lax.broadcasted_iota(jnp.int32, (rows, width), 0)
    c = lax.broadcasted_iota(jnp.int32, (rows, width), 1)
    above = jnp.where(r >= rows - 2, flags_ref[0], 0)
    below = jnp.where((r >= own_rows) & (r < own_rows + 2), flags_ref[1], 0)
    left = jnp.where(c >= width - 2, flags_ref[2], 0)
    right = jnp.where((c >= own_cols) & (c < own_cols + 2), flags_ref[3], 0)
    in_rows = jnp.where(r < own_rows, 1, above + below)
    in_cols = jnp.where(c < own_cols, 1, left + right)
    return (in_rows * in_cols).astype(jnp.float32)


def soil_sweeps(layers, p_ref, c_ref, tab_ref, mask_ref, s, gain, out):
    _, rows, width = p_ref.shape
    h_ref, q_ref, n_ref, d_ref, h2_ref, q2_ref, n2_ref, d2_ref, k_ref = s
    zero = jnp.zeros((rows, width), jnp.float32)
    for ref in (h_ref, q_ref, h2_ref, q2_ref):
        ref[0] = zero
        ref[layers + 1] = zero

    def first(z, carry):
        for ch in chunks(width):
            p = p_ref[z, :, ch]
            content, capacity, root = closure(tab_ref, c_ref[z, :, ch], p)
            root = root * mask_ref[:, ch]
            h_ref[z + 1, :, ch] = root
            q_ref[z + 1, :, ch] = root * p
            n_ref[z, :, ch] = capacity * p
            d_ref[z, :, ch] = capacity
            k_ref[z, :, ch] = content
        return carry

    lax.fori_loop(0, layers, first, 0)

    def sums(z, h, q):
        mid, over, under = h[z + 1], h[z], h[z + 2]
        weights = lateral(mid) + over + under
        flows = lateral(q[z + 1]) + q[z] + q[z + 2] + GRAVITY_STEP * (over - under)
        return mid, weights, flows

    def second(z, carry):
        mid, weights, flows = sums(z, h_ref, q_ref)
        top = n_ref[z] + mid * flows
        if gain is not None:
            top = top + jnp.where(z == 0, 1.0, 0.0) * gain
        q2_ref[z + 1] = top / (d_ref[z] + mid * weights)
        for ch in chunks(width):
            p = q2_ref[z + 1, :, ch]
            content, capacity, root = closure(tab_ref, c_ref[z, :, ch], p)
            root = root * mask_ref[:, ch]
            h2_ref[z + 1, :, ch] = root
            q2_ref[z + 1, :, ch] = root * p
            n2_ref[z, :, ch] = capacity * p - (content - k_ref[z, :, ch])
            d2_ref[z, :, ch] = capacity
        return carry

    lax.fori_loop(0, layers, second, 0)

    def third(z, carry):
        mid, weights, flows = sums(z, h2_ref, q2_ref)
        top = n2_ref[z] + mid * flows
        if gain is not None:
            top = top + jnp.where(z == 0, 1.0, 0.0) * gain
        out(z, top / (d2_ref[z] + mid * weights))
        return carry

    return third


def soil_scratch(layers, rows, width):
    tall = pltpu.VMEM((layers + 2, rows, width), jnp.float32)
    flat = pltpu.VMEM((layers, rows, width), jnp.float32)
    return [tall, tall, flat, flat, tall, tall, flat, flat, flat]


def soil_pack_kernel(p_ref, c_ref, next_ref, prev_ref):
    layers, own, _ = p_ref.shape
    for z in range(layers):
        next_ref[0, z] = p_ref[z, own - 2 :, :]
        next_ref[1, z] = c_ref[z, own - 2 :, :].astype(jnp.float32)
        prev_ref[0, z] = p_ref[z, :2, :]
        prev_ref[1, z] = c_ref[z, :2, :].astype(jnp.float32)


def soil_pack(pressure, soil_class):
    layers, _, cols = pressure.shape
    shape = jax.ShapeDtypeStruct((2, layers, 2, cols), jnp.float32)
    return pl.pallas_call(soil_pack_kernel, out_shape=(shape, shape), name="soil_pack")(pressure, soil_class)


def soil_edge_kernel(p_first, c_first, p_last, c_last, up_first, up_last, down_first, down_last, out_ref, box):
    layers, own, _ = p_first.shape
    rows = box.shape[1]
    out = []
    for side in ((p_last, c_last, up_last, down_last), (p_first, c_first, up_first, down_first)):
        for f in range(2):
            for z in range(layers):
                box[z, :own] = side[f][z].astype(jnp.float32)
                box[z, own : own + 2] = side[3][f, z]
                box[z, own + 2 : rows - 2] = jnp.zeros((rows - own - 4, LANES), jnp.float32)
                box[z, rows - 2 :] = side[2][f, z]
            turned = box[...].reshape(layers * rows, LANES).T
            out.append(turned[LANES - 2 :] if len(out) < 2 else turned[:2])
    out_ref[...] = jnp.concatenate(out, axis=0)


def soil_edge(pressure, soil_class, up, down):
    layers, own, cols = pressure.shape
    rows = own + SUBS
    last = cols // LANES - 1
    tile = [pl.BlockSpec((layers, own, LANES), lambda _, i=i: (0, 0, i)) for i in (0, 0, last, last)]
    halo = [pl.BlockSpec((2, layers, 2, LANES), lambda _, i=i: (0, 0, 0, i)) for i in (0, last, 0, last)]
    return pl.pallas_call(
        soil_edge_kernel,
        out_shape=jax.ShapeDtypeStruct((8, layers * rows), jnp.float32),
        grid=(1,),
        in_specs=tile + halo,
        scratch_shapes=[pltpu.VMEM((layers, rows, LANES), jnp.float32)],
        name="soil_edge",
    )(pressure, soil_class, pressure, soil_class, up, up, down, down)


def soil_kernel(flags_ref, tab_ref, p_in, c_in, up_in, down_in, edge_in, out_ref, pe_out, ce_out, pe, ce, mask_ref, turn, *s):
    layers, own, cols = p_in.shape
    _, rows, width = pe.shape
    pad = jnp.zeros((rows - own, cols), jnp.float32)
    turn[...] = jnp.zeros_like(turn)
    for f, dst in enumerate((pe, ce)):
        turn[LANES - 2 :, :] = edge_in[2 * f : 2 * f + 2, :]
        turn[:2, :] = edge_in[4 + 2 * f : 6 + 2 * f, :]
        dst[:, :, cols:] = turn[...].T.reshape(layers, rows, LANES).astype(dst.dtype)

    def build(z, carry):
        for f, (src, dst) in enumerate(((p_in, pe), (c_in, ce))):
            kind = dst.dtype
            dst[z, own:, :cols] = pad.astype(kind)
            dst[z, :own, :cols] = src[z]
            dst[z, own : own + 2, :cols] = down_in[f, z].astype(kind)
            dst[z, rows - 2 :, :cols] = up_in[f, z].astype(kind)
        return carry

    lax.fori_loop(0, layers, build, 0)
    mask_ref[...] = soil_mask(flags_ref, rows, width, own, cols)

    def out(z, p):
        out_ref[z] = p[:own, :cols]

    third = soil_sweeps(layers, pe, ce, tab_ref, mask_ref, s, None, out)
    lax.fori_loop(0, layers, third, 0)
    pe_out[...] = pe[:TOP_LAYERS]
    ce_out[...] = ce[:TOP_LAYERS]


def soil_interior(flags, tables, pressure, soil_class, up, down, edge):
    layers, own, cols = pressure.shape
    rows, width = own + SUBS, cols + LANES
    return pl.pallas_call(
        soil_kernel,
        out_shape=(
            jax.ShapeDtypeStruct(pressure.shape, jnp.float32),
            jax.ShapeDtypeStruct((TOP_LAYERS, rows, width), jnp.float32),
            jax.ShapeDtypeStruct((TOP_LAYERS, rows, width), jnp.int32),
        ),
        in_specs=[pl.BlockSpec(memory_space=pltpu.SMEM)] + [pl.BlockSpec(memory_space=pltpu.VMEM)] * 6,
        out_specs=[pl.BlockSpec(memory_space=pltpu.VMEM)] * 3,
        scratch_shapes=[
            pltpu.VMEM((layers, rows, width), jnp.float32),
            pltpu.VMEM((layers, rows, width), jnp.int32),
            pltpu.VMEM((rows, width), jnp.float32),
            pltpu.VMEM((LANES, layers * rows), jnp.float32),
        ]
        + soil_scratch(layers, rows, width),
        name="soil_interior",
    )(flags, tables, pressure, soil_class, up, down, edge)


def surface_pack_kernel(p_ref, c_ref, depth, level, rough, rain, land, channel, main_ref, next_ref, prev_ref):
    height, width = depth.shape
    _, own, cols = p_ref.shape
    fields = (
        depth[...],
        level[...],
        (1.0 + channel[...].astype(jnp.float32)) / rough[...],
        LEAKANCE * land[...].astype(jnp.float32),
        rain[...],
    )
    for f, x in enumerate(fields):
        main_ref[f * height : (f + 1) * height, :] = x
        next_ref[3 * f : 3 * f + 3, :] = x[height - 3 :]
        prev_ref[3 * f : 3 * f + 3, :] = x[:3]
    base = 5 * height
    for f, x in enumerate((p_ref[0], c_ref[0].astype(jnp.float32))):
        for j, ch in enumerate(chunks(cols)):
            main_ref[base : base + own, :] = x[:, ch]
            base += own
            at = EDGE_ROWS + 2 * (f * (cols // LANES) + j)
            next_ref[at : at + 2, :] = x[own - 2 :, ch]
            prev_ref[at : at + 2, :] = x[:2, ch]


EDGE_ROWS = 16


def surface_pack(pressure, soil_class, depth, level, rough, rain, land, channel):
    _, own, cols = pressure.shape
    height = depth.shape[0]
    top = pl.BlockSpec((1, own, cols), lambda _: (0, 0, 0))
    strip = EDGE_ROWS + 4 * cols // LANES
    f32 = jnp.float32
    return pl.pallas_call(
        surface_pack_kernel,
        out_shape=(
            jax.ShapeDtypeStruct((5 * height + 2 * own * cols // LANES, LANES), f32),
            jax.ShapeDtypeStruct((strip, LANES), f32),
            jax.ShapeDtypeStruct((strip, LANES), f32),
        ),
        grid=(1,),
        in_specs=[top, top] + [pl.BlockSpec(memory_space=pltpu.VMEM)] * 6,
        name="surface_pack",
    )(pressure, soil_class, depth, level, rough, rain, land, channel)


def surface_edge_kernel(main_ref, above_ref, below_ref, out_ref, box, *, height, own, cols):
    n = cols // LANES
    tall = height + SUBS
    box[...] = jnp.zeros_like(box)
    for side, j in enumerate((n - 1, 0)):
        for f in range(2):
            at = (2 * side + f) * 2 * SUBS
            src = 5 * height + (f * n + j) * own
            strip = EDGE_ROWS + 2 * (f * n + j)
            box[at : at + own, :] = main_ref[src : src + own, :]
            box[at + own : at + own + 2, :] = below_ref[strip : strip + 2, :]
            box[at + own + 2 : at + own + 4, :] = above_ref[strip : strip + 2, :]
    for f in range(5):
        at = LANES + f * tall
        box[at : at + height, :] = main_ref[f * height : (f + 1) * height, :]
        box[at + height : at + height + 3, :] = below_ref[3 * f : 3 * f + 3, :]
        box[at + tall - 3 : at + tall, :] = above_ref[3 * f : 3 * f + 3, :]
    turned = box[...].T
    edges = jnp.concatenate([turned[LANES - 3 :], turned[:3], jnp.zeros((2, turned.shape[1]), jnp.float32)], axis=0)
    for j, ch in enumerate(chunks(turned.shape[1])):
        out_ref[j * SUBS : (j + 1) * SUBS, :] = edges[:, ch]


def surface_edge(main, above, below, height, own, cols):
    wide = LANES + 5 * (height + SUBS)
    wide += -wide % LANES

    def body(*refs):
        surface_edge_kernel(*refs, height=height, own=own, cols=cols)

    return pl.pallas_call(
        body,
        out_shape=jax.ShapeDtypeStruct((wide // LANES * SUBS, LANES), jnp.float32),
        scratch_shapes=[pltpu.VMEM((wide, LANES), jnp.float32)],
        name="surface_edge",
    )(main, above, below)


def assemble(spot_ref, mains, strips, surf_ref, tops_ref, turn, own, height, count):
    _, rows, width = surf_ref.shape
    cols = width - LANES
    n = cols // LANES
    tall = height + SUBS
    strip = EDGE_ROWS + 4 * n
    lane = lax.broadcasted_iota(jnp.int32, (SUBS, LANES), 1)
    surf_ref[...] = jnp.zeros_like(surf_ref)
    tops_ref[...] = jnp.zeros_like(tops_ref)
    turn[...] = jnp.zeros_like(turn)
    for s in range(count):
        main, extra = mains[s], strips[s]
        who = spot_ref[4 + s]
        at = pl.multiple_of(who * LANES, LANES)
        first = pl.multiple_of(who * own, own)
        above, below = 0, strip
        for f in range(5):
            surf_ref[f, :height, pl.ds(at, LANES)] = main[f * height : (f + 1) * height, :]
            surf_ref[f, height : height + 3, pl.ds(at, LANES)] = extra[below + 3 * f : below + 3 * f + 3, :]
            surf_ref[f, rows - 3 :, pl.ds(at, LANES)] = extra[above + 3 * f : above + 3 * f + 3, :]
        for f in range(2):
            for j in range(n):
                src = 5 * height + (f * n + j) * own
                tops_ref[f, pl.ds(first, own), j * LANES : (j + 1) * LANES] = main[src : src + own, :]
        turn[LANES - 3 :, :LANES] = extra[2 * strip : 2 * strip + 3, :]
        turn[:3, :LANES] = extra[2 * strip + 3 : 2 * strip + 6, :]
        block = turn[:, :LANES].T
        for f in range(2):
            after = block[2 * (2 + f) * SUBS :][: 2 * SUBS]
            before = block[2 * f * SUBS :][: 2 * SUBS]
            two = jnp.where(lane >= LANES - 2, before[:SUBS], jnp.where(lane < 2, after[:SUBS], 0.0))
            more = jnp.where(lane >= LANES - 2, before[SUBS:], jnp.where(lane < 2, after[SUBS:], 0.0))
            tops_ref[f, pl.ds(first, own), cols:] = two

            @pl.when(who == 0)
            def _(f=f, more=more, extra=extra):
                tops_ref[f, height : height + 2, cols:] = more[:2]
                for j in range(n):
                    src = below + EDGE_ROWS + 2 * (f * n + j)
                    tops_ref[f, height : height + 2, j * LANES : (j + 1) * LANES] = extra[src : src + 2, :]

            @pl.when(who == count - 1)
            def _(f=f, more=more, extra=extra):
                tops_ref[f, rows - 2 :, cols:] = more[2:4]
                for j in range(n):
                    src = above + EDGE_ROWS + 2 * (f * n + j)
                    tops_ref[f, rows - 2 :, j * LANES : (j + 1) * LANES] = extra[src : src + 2, :]

        @pl.when(who == count - 1)
        def _(extra=extra):
            for j in range(1, turn.shape[1] // LANES):
                src = 2 * strip + j * SUBS
                turn[LANES - 3 :, j * LANES : (j + 1) * LANES] = extra[src : src + 3, :]

        @pl.when(who == 0)
        def _(extra=extra):
            for j in range(1, turn.shape[1] // LANES):
                src = 2 * strip + j * SUBS
                turn[:3, j * LANES : (j + 1) * LANES] = extra[src + 3 : src + 6, :]

    block = turn[:, LANES:].T
    for f in range(5):
        surf_ref[f, :, cols:] = block[f * tall : (f + 1) * tall]


def last_kernel(
    spot_ref, flags_ref, tab_ref, surf_ref, tops_ref, pe, ce, head_out, water_ref,
    ex_ref, w_ref, mask_ref, new_ref, sem, *s, own,
):
    _, rows, width = surf_ref.shape
    block_rows, block_cols = rows - SUBS, width - LANES
    r = lax.broadcasted_iota(jnp.int32, (rows, width), 0)
    c = lax.broadcasted_iota(jnp.int32, (rows, width), 1)
    row_ok = jnp.where(r < block_rows, 1, jnp.where(r >= rows - 3, spot_ref[2], jnp.where(r < block_rows + 3, spot_ref[3], 0)))
    col_ok = jnp.where(c < block_cols, 1, jnp.where(c >= width - 3, flags_ref[2], jnp.where(c < block_cols + 3, flags_ref[3], 0)))
    inside = (row_ok * col_ok).astype(jnp.float32)
    level = surf_ref[1]
    convey = jnp.sqrt(surf_ref[2]) * inside
    leak = surf_ref[3]
    rain = surf_ref[4]
    top = tops_ref[0]

    def across(x):
        return pltpu.roll(x, rows - 1, 0)

    def along(x):
        return pltpu.roll(x, width - 1, 1)

    gates = [convey * across(convey), convey * along(convey)]
    parts = []
    for ch in chunks(width):
        _, _, root = closure(tab_ref, tops_ref[1, :, ch].astype(jnp.int32), top[:, ch])
        parts.append(0.25 * root * root)
    leak = leak * jnp.concatenate(parts, axis=1)
    water = surf_ref[0]
    exchange = jnp.zeros_like(water)
    for _ in range(PASSES):
        surface = level + water
        power = jnp.where(water > 0.0, jnp.exp2((5.0 / 3.0) * jnp.log2(jnp.maximum(water, 1e-30))), 0.0)
        outflow = jnp.zeros_like(water)
        for axis, gate, beside in ((0, gates[0], across), (1, gates[1], along)):
            slope = surface - beside(surface)
            carried = jnp.where(slope >= 0.0, power, beside(power))
            flux = gate * carried * slope * lax.rsqrt(jnp.maximum(jnp.abs(slope), SLOPE_FLOOR))
            outflow = outflow + flux - pltpu.roll(flux, 1, axis)
        rate = leak * (water - top)
        exchange = exchange + SURFACE_STEP * rate
        water = jnp.maximum(water + SURFACE_STEP * (rain - rate - outflow), 0.0)
    ex_ref[...] = exchange
    w_ref[...] = water
    if water_ref.shape[1] % LANES:
        water_ref[...] = w_ref[:block_rows, :block_cols]
    else:
        mine = pl.multiple_of(spot_ref[4] * water_ref.shape[1], LANES)
        water_ref[...] = w_ref[:block_rows, pl.ds(mine, water_ref.shape[1])]
    first = pl.multiple_of(spot_ref[0], SUBS)
    after = pl.multiple_of(spot_ref[0] + own, SUBS)
    before = pl.multiple_of(spot_ref[1], SUBS)
    sub = lax.broadcasted_iota(jnp.int32, (SUBS, width), 0)
    rim = jnp.where(sub == SUBS - 1, ex_ref[pl.ds(before, SUBS), :], jnp.where(sub == 0, ex_ref[pl.ds(after, SUBS), :], 0.0))
    gain = jnp.concatenate([ex_ref[pl.ds(first, own), :], rim], axis=0)
    mask_ref[...] = soil_mask(flags_ref, own + SUBS, width, own, block_cols)

    def out(z, p):
        new_ref[z] = p[:own, :block_cols]

    third = soil_sweeps(TOP_LAYERS, pe, ce, tab_ref, mask_ref, s, gain, out)
    lax.fori_loop(0, TOP_LAYERS - 2, third, 0)
    copy = pltpu.make_async_copy(new_ref, head_out.at[: TOP_LAYERS - 2], sem)
    copy.start()
    copy.wait()


def finish(spot, flags, tables, fields, pe, ce, head, block, count):
    own = head.shape[1]
    whole = count == 0
    rows, width = block[0] + SUBS, block[1] + LANES
    n = len(fields)

    def body(spot_ref, flags_ref, tab_ref, *refs):
        given, (pe_ref, ce_ref, _, head_out, water_ref), (box, turn), rest = refs[:n], refs[n : n + 5], refs[n + 5 : n + 7], refs[n + 7 :]
        if whole:
            surf, tops = given
        else:
            surf, tops = box
            assemble(spot_ref, given[:count], given[count:], surf, tops, turn, own, block[0], count)
        last_kernel(spot_ref, flags_ref, tab_ref, surf, tops, pe_ref, ce_ref, head_out, water_ref, *rest, own=own)

    def scratch_body(*refs):
        cut = 3 + n + 5
        body(*refs[:cut], refs[cut : cut + 2], refs[cut + 2], *refs[cut + 3 :])

    tall = LANES + 5 * (block[0] + SUBS)
    tall += -tall % LANES
    small = (1, SUBS, LANES)
    vmem = pl.BlockSpec(memory_space=pltpu.VMEM)
    smem = pl.BlockSpec(memory_space=pltpu.SMEM)
    water = block if whole else (block[0], LANES)
    return pl.pallas_call(
        scratch_body,
        out_shape=(
            jax.ShapeDtypeStruct(head.shape, jnp.float32),
            jax.ShapeDtypeStruct(water, jnp.float32),
        ),
        in_specs=[smem, smem] + [vmem] * (n + 3) + [pl.BlockSpec(memory_space=pl.ANY)],
        out_specs=[pl.BlockSpec(memory_space=pl.ANY), vmem],
        scratch_shapes=[
            pltpu.VMEM(small if whole else (5, rows, width), jnp.float32),
            pltpu.VMEM(small if whole else (2, rows, width), jnp.float32),
            pltpu.VMEM((SUBS, LANES) if whole else (LANES, tall), jnp.float32),
            pltpu.VMEM((rows, width), jnp.float32),
            pltpu.VMEM((rows, width), jnp.float32),
            pltpu.VMEM((own + SUBS, width), jnp.float32),
            pltpu.VMEM((TOP_LAYERS - 2, own, block[1]), jnp.float32),
            pltpu.SemaphoreType.DMA,
        ]
        + soil_scratch(TOP_LAYERS, own + SUBS, width),
        input_output_aliases={n + 5: 0},
        name="surface_and_top",
    )(spot, flags, tables, *fields, pe, ce, head)


def lane_rows(size):
    return -(-size // LANES)


def as_lanes(x):
    if x.shape[-1] % LANES:
        x = jnp.pad(x.reshape(-1), (0, -x.size % LANES))
    return x.reshape(-1, LANES)


def from_lanes(x, shape):
    if shape[-1] % LANES:
        size = 1
        for length in shape:
            size *= length
        x = x.reshape(-1)[:size]
    return x.reshape(shape)


def gx_trade(edges, half):
    got = shift(edges, "gx", 1)
    if lax.axis_size("gx") == 2:
        return got
    return jnp.where(half, got, shift(edges, "gx", -1))


def cyclic_rows(mid, above, below, gap):
    hole = jnp.zeros(mid.shape[:-2] + (gap, mid.shape[-1]), mid.dtype)
    return jnp.concatenate([mid, below, hole, above], axis=-2)


def block_general(pressure, soil_class, depth, elevation, roughness, rain, land_mask, channel_mask):
    ny = lax.axis_size("gy")
    _, own, cols = pressure.shape
    srows, scols = depth.shape
    convey = (1.0 + channel_mask.astype(jnp.float32)) / roughness
    surf = jnp.stack([depth, elevation, convey, LEAKANCE * land_mask.astype(jnp.float32), rain])
    tops = jnp.stack([pressure[0], soil_class[0].astype(jnp.float32)])

    def pack(s, t):
        return jnp.concatenate([as_lanes(s), as_lanes(t)], axis=0)

    def unpack(m):
        cut = lane_rows(15 * scols)
        return from_lanes(m[:cut], (5, 3, scols)), from_lanes(m[cut:], (2, 2, cols))

    s_above, t_above = unpack(shift(pack(surf[:, -3:], tops[:, -2:]), "grp", 1))
    s_below, t_below = unpack(shift(pack(surf[:, :3], tops[:, :2]), "grp", -1))
    surf_rows = cyclic_rows(surf, s_above, s_below, 2)
    tops_rows = jnp.concatenate([tops, t_below, t_above], axis=1)

    def edges(cut):
        a = surf_rows[:, :, cut(3)].transpose(0, 2, 1).reshape(15, -1)
        b = tops_rows[:, :, cut(2)].transpose(0, 2, 1).reshape(4, -1)
        return jnp.concatenate([a, jnp.pad(b, ((0, 0), (0, a.shape[1] - b.shape[1])))], axis=0)

    out = jnp.concatenate([edges(lambda n: slice(-n, None)), edges(lambda n: slice(0, n))])
    got = gx_trade(out, lax.broadcasted_iota(jnp.int32, out.shape, 0) < 19)
    mine = jnp.concatenate(
        [as_lanes(surf_rows), as_lanes(tops_rows), jnp.pad(got, ((0, 0), (0, -got.shape[1] % LANES))).reshape(-1, LANES)]
    )
    every = lax.all_gather(mine, "gy", axis=0, tiled=False)
    n1 = lane_rows(surf_rows.size)
    n2 = n1 + lane_rows(tops_rows.size)
    e_surf = jax.vmap(lambda m: from_lanes(m, (5, srows + SUBS, scols)))(every[:, :n1])
    e_surf = e_surf.transpose(1, 2, 0, 3).reshape(5, srows + SUBS, ny * scols)
    e_tops = every[:, n1:n2].reshape(ny, 2, own + 4, cols)
    e_m = every[:, n2:].reshape(ny, 2, 19, -1)
    main = e_tops[:, :, :own].transpose(1, 0, 2, 3).reshape(2, srows, cols)
    zeros = jnp.zeros((2, 4, cols), jnp.float32)
    f_tops = jnp.concatenate([main, e_tops[0, :, own : own + 2], zeros, e_tops[-1, :, own + 2 :]], axis=1)
    height = srows + SUBS
    c_left = e_m[-1, 0, :15, :height].reshape(5, 3, height).transpose(0, 2, 1)
    c_right = e_m[0, 1, :15, :height].reshape(5, 3, height).transpose(0, 2, 1)
    hole = jnp.zeros((5, height, LANES - 6), jnp.float32)
    blocks = jnp.concatenate([e_surf, c_right, hole, c_left], axis=2)

    def tops_edge(side):
        t = e_m[:, side, 15:, : own + 4].reshape(ny, 2, 2, own + 4)
        mid = t[..., :own].transpose(1, 0, 3, 2).reshape(2, srows, 2)
        low = t[0, :, :, own : own + 2].transpose(0, 2, 1)
        high = t[-1, :, :, own + 2 :].transpose(0, 2, 1)
        return jnp.concatenate([mid, low, jnp.zeros((2, 4, 2), jnp.float32), high], axis=1)

    return blocks, jnp.concatenate(
        [f_tops, tops_edge(1), jnp.zeros((2, height, LANES - 4), jnp.float32), tops_edge(0)], axis=2
    )


def block_parts(pressure, soil_class, depth, elevation, roughness, rain, land_mask, channel_mask):
    ny = lax.axis_size("gy")
    _, own, cols = pressure.shape
    main, after, before = surface_pack(pressure, soil_class, depth, elevation, roughness, rain, land_mask, channel_mask)
    above = shift(after, "grp", 1)
    below = shift(before, "grp", -1)
    mains = [main] + [shift(main, "gy", step) for step in range(1, ny)]
    edge = surface_edge(main, above, below, depth.shape[0], own, cols)
    edge = gx_trade(edge, lax.broadcasted_iota(jnp.int32, edge.shape, 0) % SUBS < 3)
    strip = jnp.concatenate([above, below, edge], axis=0)
    return mains + [strip] + [shift(strip, "gy", step) for step in range(1, ny)]


def local(
    pressure, soil_class, capacity_range, inverse_entry, shape_index, conductivity,
    depth, elevation, roughness, rain, land_mask, channel_mask,
):
    ng, nx, ny = (lax.axis_size(a) for a in ("grp", "gx", "gy"))
    ig, ix, iy = (lax.axis_index(a) for a in ("grp", "gx", "gy"))
    _, own, cols = pressure.shape
    srows, scols = depth.shape
    ground = (depth, elevation, roughness, rain, land_mask, channel_mask)
    tables = class_tables(capacity_range, inverse_entry, shape_index, conductivity)
    tile = ig * ny + iy
    flags = jnp.stack([tile > 0, tile < ng * ny - 1, ix > 0, ix < nx - 1]).astype(jnp.int32)
    spot = [iy * own, jnp.where(iy > 0, iy * own - SUBS, srows), (ig > 0).astype(jnp.int32), (ig < ng - 1).astype(jnp.int32)]
    spot = jnp.stack(spot + [(iy - step) % ny for step in range(ny)])

    even = scols == LANES and own == SUBS
    if even:
        fields = block_parts(pressure, soil_class, *ground)
    else:
        fields = block_general(pressure, soil_class, *ground)

    after, before = soil_pack(pressure, soil_class)
    up = shift(after, ("grp", "gy"), 1)
    down = shift(before, ("grp", "gy"), -1)
    edge = soil_edge(pressure, soil_class, up, down)
    edge = gx_trade(edge, lax.broadcasted_iota(jnp.int32, edge.shape, 0) < 4)
    head, pe, ce = soil_interior(flags, tables, pressure, soil_class, up, down, edge)
    head, water = finish(spot, flags, tables, fields, pe, ce, head, (srows, cols), ny if even else 0)
    if not even:
        water = lax.dynamic_slice_in_dim(water, iy * scols, scols, axis=1)
    return head, water


def solution(mesh):
    soil = P(None, ("grp", "gy"), "gx")
    ground = P("grp", ("gx", "gy"))
    return jax.shard_map(
        local,
        mesh=mesh,
        in_specs=(soil, soil, P(), P(), P(), P()) + (ground,) * 6,
        out_specs=(soil, ground),
        check_vma=False,
    )
```

```python
import jax
import jax.numpy as jnp
from jax import lax
from jax.experimental import pallas as pl
from jax.experimental.pallas import tpu as pltpu
from jax.sharding import PartitionSpec as P

PASSES = 3
STORAGE = 0.01
GRAVITY_STEP = 0.5
SUCTION_FLOOR = 0.01
SLOPE_FLOOR = 0.1
SURFACE_STEP = 0.3
LEAKANCE = 0.5

LANES = 128
SUBS = 8
TOP_LAYERS = 2


def shift(x, axis, step):
    size = lax.axis_size(axis)
    return lax.ppermute(x, axis, [(i, (i + step) % size) for i in range(size)])


def class_tables(capacity_range, inverse_entry, shape_index, conductivity):
    pore = 1.0 - 1.0 / shape_index
    rows = [-inverse_entry, 1.0 / (1.0 - pore), pore, capacity_range, 2.0 * jnp.sqrt(conductivity)]
    return jnp.pad(jnp.stack(rows), ((0, SUBS - len(rows)), (0, LANES - shape_index.shape[0])))


def params(tab_ref, idx):
    return [
        jnp.take_along_axis(jnp.broadcast_to(tab_ref[i : i + 1, :], idx.shape), idx, axis=1, mode="promise_in_bounds")
        for i in range(5)
    ]


def closure(given, p):
    entry, expo, pore, span, scale = given
    logs = jnp.log2(jnp.maximum(entry * p, SUCTION_FLOOR))
    total = jnp.log2(1.0 + jnp.exp2(expo * logs))
    drop = pore * total
    less = expo - 1.0
    power = less * logs - drop
    ratio = jnp.exp2(power)
    content = span * jnp.exp2(-drop)
    capacity = STORAGE - (span * entry * less) * jnp.exp2(power - total)
    root = scale * jnp.exp2(-0.25 * drop) * jnp.abs(1.0 - ratio)
    return content, capacity, root


def chunks(width):
    return [slice(i, i + LANES) for i in range(0, width, LANES)]


def wide(parts):
    return [jnp.concatenate(x, axis=1) for x in zip(*parts)]


def lateral(x):
    rows, width = x.shape
    return (
        pltpu.roll(x, 1, 0)
        + pltpu.roll(x, rows - 1, 0)
        + pltpu.roll(x, 1, 1)
        + pltpu.roll(x, width - 1, 1)
    )


def soil_mask(flags_ref, rows, width, own_rows, own_cols):
    r = lax.broadcasted_iota(jnp.int32, (rows, width), 0)
    c = lax.broadcasted_iota(jnp.int32, (rows, width), 1)
    above = jnp.where(r >= rows - 2, flags_ref[0], 0)
    below = jnp.where((r >= own_rows) & (r < own_rows + 2), flags_ref[1], 0)
    left = jnp.where(c >= width - 2, flags_ref[2], 0)
    right = jnp.where((c >= own_cols) & (c < own_cols + 2), flags_ref[3], 0)
    in_rows = jnp.where(r < own_rows, 1, above + below)
    in_cols = jnp.where(c < own_cols, 1, left + right)
    return (in_rows * in_cols).astype(jnp.float32)


def soil_rows(p_ref, c_ref, next_ref, prev_ref):
    _, own, _ = p_ref.shape
    for f, x in enumerate((p_ref, c_ref)):
        for r in range(2):
            next_ref[f, r] = x[:, own - 2 + r, :].astype(jnp.float32)
            prev_ref[f, r] = x[:, r, :].astype(jnp.float32)


def soil_columns(p_first, c_first, p_last, c_last, up_first, up_last, down_first, down_last, box):
    layers, own, _ = p_first.shape
    rows = box.shape[1]
    out = []
    for side in ((p_last, c_last, up_last, down_last), (p_first, c_first, up_first, down_first)):
        for f in range(2):
            box[:, 2 : 2 + own, :] = side[f][...].astype(jnp.float32)
            box[:, own + 4 :, :] = jnp.zeros((layers, rows - own - 4, LANES), jnp.float32)
            for r in range(2):
                box[:, r, :] = side[2][f, r]
                box[:, own + 2 + r, :] = side[3][f, r]
            turned = box[...].reshape(layers * rows, LANES).T
            out.append(turned[LANES - 2 :] if len(out) < 2 else turned[:2])
    return jnp.concatenate(out, axis=0)


def soil_kernel(
    flags_ref, tab_ref, p_in, c_in, up_in, down_in, got, sent, out_ref, top_out, class_out, next_out,
    h_ref, q_ref, n_ref, d_ref, k_ref, h2_ref, q2_ref, n2_ref, d2_ref, given, corner, turn, near, near2, pe, ce,
):
    layers, own, cols = p_in.shape
    rows = own + SUBS
    span = layers * rows
    f32 = jnp.float32
    ok = [flags_ref[i] for i in range(4)]
    for ref in (h_ref, q_ref, h2_ref, q2_ref):
        ref[0] = jnp.zeros((own, cols), f32)
        ref[layers + 1] = jnp.zeros((own, cols), f32)

    def first(z, carry):
        for ch in chunks(cols):
            p = p_in[z, :, ch]
            values = params(tab_ref, c_in[z, :, ch])
            for i, v in enumerate(values):
                given[i, z, :, ch] = v
            content, capacity, root = closure(values, p)
            h_ref[z + 1, :, ch] = root
            q_ref[z + 1, :, ch] = root * p
            n_ref[z, :, ch] = capacity * p
            d_ref[z, :, ch] = capacity
            k_ref[z, :, ch] = content
        return carry

    lax.fori_loop(0, layers, first, 0)

    gap = jnp.zeros((1, span), f32)
    p = jnp.concatenate([got[0:2], sent[4:5], gap, sent[1:2], got[4:6], gap], axis=0)
    kind = jnp.concatenate([got[2:4], sent[6:7], gap, sent[3:4], got[6:8], gap], axis=0).astype(jnp.int32)
    sub = lax.broadcasted_iota(jnp.int32, (SUBS, span), 0)
    lane = lax.broadcasted_iota(jnp.int32, (SUBS, span), 1)
    row = lane % rows
    row_ok = jnp.where(row < 2, ok[0], jnp.where(row < own + 2, 1, jnp.where(row < own + 4, ok[1], 0)))
    col_ok = jnp.where(sub < 2, ok[2], jnp.where((sub == 2) | (sub == 4), 1, jnp.where((sub == 5) | (sub == 6), ok[3], 0)))
    mask = (row_ok * col_ok).astype(f32)
    values = [params(tab_ref, kind[:, ch]) for ch in chunks(span)]
    content, capacity, root = wide([closure(v, p[:, ch]) for v, ch in zip(values, chunks(span))])
    h, q = root * mask, root * mask * p

    def over(x):
        return jnp.where(lane < rows, 0.0, pltpu.roll(x, rows, 1))

    def under(x):
        return jnp.where(lane >= span - rows, 0.0, pltpu.roll(x, span - rows, 1))

    weights = lateral(h) + over(h) + under(h)
    flows = lateral(q) + over(q) + under(q) + GRAVITY_STEP * (over(h) - under(h))
    p1 = (capacity * p + h * flows) / (capacity + h * weights)
    root = wide([closure(v, p1[:, ch]) for v, ch in zip(values, chunks(span))])[2] * mask
    turn[...] = jnp.zeros_like(turn)
    for i, x in enumerate((h, q, root, root * p1)):
        turn[i * SUBS : (i + 1) * SUBS, :] = x
    corner[...] = turn[...].T.reshape(layers, rows, LANES)

    zsub = lax.broadcasted_iota(jnp.int32, (layers, cols), 0)
    zlane = lax.broadcasted_iota(jnp.int32, (layers, LANES), 1)

    def sides(x, edge, at, lanes):
        left, right = pltpu.roll(x, 1, 1), pltpu.roll(x, cols - 1, 1)
        a = jnp.where(lanes == 0, pltpu.roll(edge, LANES - at, 1), left[:, :LANES])
        b = jnp.where(lanes == LANES - 1, pltpu.roll(edge, LANES - 1 - (at + 4), 1), right[:, cols - LANES :])
        return jnp.concatenate([a, left[:, LANES:]], axis=1) + jnp.concatenate([right[:, : cols - LANES], b], axis=1)

    for side, (halo, close, far, edge_row, valid) in enumerate(((up_in, 1, 0, 1, ok[0]), (down_in, 0, 1, own + 2, ok[1]))):
        inside = valid.astype(f32)
        ours = 0 if side == 0 else own - 1
        values, states, beyond = [], [], []
        for ch in chunks(cols):
            p = halo[0, close, :, ch]
            v = params(tab_ref, halo[1, close, :, ch].astype(jnp.int32))
            content, capacity, root = closure(v, p)
            root = root * inside
            values.append(v)
            states.append((p, capacity, root, root * p))
            p = halo[0, far, :, ch]
            root = closure(params(tab_ref, halo[1, far, :, ch].astype(jnp.int32)), p)[2] * inside
            beyond.append((root, root * p))
        p, capacity, h, q = wide(states)
        far_h, far_q = wide(beyond)
        near[side, 0] = h
        near[side, 1] = q
        edge = corner[:, edge_row, :]
        top_h = jnp.where(zsub == 0, 0.0, pltpu.roll(h, 1, 0))
        low_h = jnp.where(zsub == layers - 1, 0.0, pltpu.roll(h, layers - 1, 0))
        top_q = jnp.where(zsub == 0, 0.0, pltpu.roll(q, 1, 0))
        low_q = jnp.where(zsub == layers - 1, 0.0, pltpu.roll(q, layers - 1, 0))
        weights = far_h + h_ref[1 : layers + 1, ours, :] + sides(h, edge, 1, zlane) + top_h + low_h
        flows = far_q + q_ref[1 : layers + 1, ours, :] + sides(q, edge, 1 + SUBS, zlane) + top_q + low_q + GRAVITY_STEP * (top_h - low_h)
        p1 = (capacity * p + h * flows) / (capacity + h * weights)
        for v, ch in zip(values, chunks(cols)):
            root = closure(v, p1[:, ch])[2] * inside
            near2[side, 0, :, ch] = root
            near2[side, 1, :, ch] = root * p1[:, ch]

    tsub = lax.broadcasted_iota(jnp.int32, (own, cols), 0)
    tlane = lax.broadcasted_iota(jnp.int32, (own, LANES), 1)

    def around(z, h, q, rim, at):
        edge = corner[z, 2 : 2 + own, :]
        out = []
        for i, x in enumerate((h[z + 1], q[z + 1])):
            above = jnp.where(tsub == 0, rim[0, i, pl.ds(z, 1), :], pltpu.roll(x, 1, 0))
            below = jnp.where(tsub == own - 1, rim[1, i, pl.ds(z, 1), :], pltpu.roll(x, own - 1, 0))
            out.append(above + below + sides(x, edge, at + i * SUBS, tlane))
        weights, flows = out
        low = h[z + 2]
        return weights + low, flows + q[z + 2] - GRAVITY_STEP * low

    def second(z, carry):
        mid, top = h_ref[z + 1], h_ref[z]
        weights, flows = around(z, h_ref, q_ref, near, 1)
        flows = flows + q_ref[z] + GRAVITY_STEP * top
        p1 = (n_ref[z] + mid * flows) / (d_ref[z] + mid * (weights + top))
        for ch in chunks(cols):
            p = p1[:, ch]
            content, capacity, root = closure([given[i, z, :, ch] for i in range(5)], p)
            h2_ref[z + 1, :, ch] = root
            q2_ref[z + 1, :, ch] = root * p
            n2_ref[z, :, ch] = capacity * p - (content - k_ref[z, :, ch])
            d2_ref[z, :, ch] = capacity
        return carry

    lax.fori_loop(0, layers, second, 0)

    def third(z, carry):
        mid, top = h2_ref[z + 1], h2_ref[z]
        weights, flows = around(z, h2_ref, q2_ref, near2, 1 + 2 * SUBS)
        flows = flows + q2_ref[z] + GRAVITY_STEP * top
        out_ref[z] = (n2_ref[z] + mid * flows) / (d2_ref[z] + mid * (weights + top))
        return carry

    lax.fori_loop(2, layers, third, 0)

    weights, flows = around(1, h2_ref, q2_ref, near2, 1 + 2 * SUBS)
    for i, x in enumerate((h2_ref[2], q2_ref[2], n2_ref[1], d2_ref[1], weights, flows)):
        next_out[i] = x
    for f, (src, dst, halo_at) in enumerate(((p_in, pe, 0), (c_in, ce, 2))):
        turn[...] = jnp.zeros_like(turn)
        turn[LANES - 2 :, :] = got[halo_at : halo_at + 2]
        turn[:2, :] = got[halo_at + 4 : halo_at + 6]
        block = turn[:, :LANES].T
        for z in range(2):
            dst[z, own:, :cols] = jnp.zeros((SUBS, cols), dst.dtype)
            dst[z, :own, :cols] = src[z]
            dst[z, :, cols:] = jnp.zeros((rows, LANES), dst.dtype)
            dst[z, : own + 2, cols:] = block[z * rows + 2 : z * rows + own + 4].astype(dst.dtype)
            dst[z, rows - 2 :, cols:] = block[z * rows : z * rows + 2].astype(dst.dtype)
            for r in range(2):
                dst[z, own + r : own + r + 1, :cols] = down_in[f, r, z : z + 1, :].astype(dst.dtype)
                dst[z, rows - 2 + r : rows - 1 + r, :cols] = up_in[f, r, z : z + 1, :].astype(dst.dtype)
    width = cols + LANES
    mask = soil_mask(flags_ref, rows, width, own, cols)
    states = []
    for z in range(2):
        content, capacity, root = wide([closure(params(tab_ref, ce[z, :, ch]), pe[z, :, ch]) for ch in chunks(width)])
        states.append((content, capacity, root * mask))
    content, capacity, h = states[0]
    low = states[1][2]
    weights = lateral(h) + low
    flows = lateral(h * pe[0]) + low * pe[1] - GRAVITY_STEP * low
    weight = capacity + h * weights
    top_out[0] = (capacity * pe[0] + h * flows) / weight
    top_out[1] = 1.0 / weight
    top_out[2] = content
    class_out[...] = ce[0]


def soil_interior(flags, tables, pressure, soil_class, up, down, got, sent):
    layers, own, cols = pressure.shape
    rows, width = own + SUBS, cols + LANES
    f32 = jnp.float32
    span = layers * rows
    tall = pltpu.VMEM((layers + 2, own, cols), f32)
    flat = pltpu.VMEM((layers, own, cols), f32)
    edge = pl.BlockSpec((SUBS, span), lambda _: (0, 0))
    vmem = pl.BlockSpec(memory_space=pltpu.VMEM)
    return pl.pallas_call(
        soil_kernel,
        out_shape=(
            jax.ShapeDtypeStruct(pressure.shape, f32),
            jax.ShapeDtypeStruct((3, rows, width), f32),
            jax.ShapeDtypeStruct((rows, width), jnp.int32),
            jax.ShapeDtypeStruct((6, own, cols), f32),
        ),
        grid=(1,),
        in_specs=[pl.BlockSpec(memory_space=pltpu.SMEM)] + [vmem] * 5 + [edge, edge],
        out_specs=[vmem] * 4,
        scratch_shapes=[tall, tall, flat, flat, flat, tall, tall, flat, flat]
        + [
            pltpu.VMEM((5, layers, own, cols), f32),
            pltpu.VMEM((layers, rows, LANES), f32),
            pltpu.VMEM((LANES, span), f32),
            pltpu.VMEM((2, 2, layers, cols), f32),
            pltpu.VMEM((2, 2, layers, cols), f32),
            pltpu.VMEM((2, rows, width), f32),
            pltpu.VMEM((2, rows, width), jnp.int32),
        ],
        name="soil_interior",
    )(flags, tables, pressure, soil_class, up, down, got, sent)


def surface_rows(p_ref, c_ref, depth, level, rough, rain, land, channel, main_ref, next_ref, prev_ref):
    height, width = depth.shape
    _, own, cols = p_ref.shape
    fields = (
        depth[...],
        level[...],
        (1.0 + channel[...].astype(jnp.float32)) / rough[...],
        LEAKANCE * land[...].astype(jnp.float32),
        rain[...],
    )
    for f, x in enumerate(fields):
        main_ref[f * height : (f + 1) * height, :] = x
        next_ref[3 * f : 3 * f + 3, :] = x[height - 3 :]
        prev_ref[3 * f : 3 * f + 3, :] = x[:3]
    base = 5 * height
    for f, x in enumerate((p_ref[0], c_ref[0].astype(jnp.float32))):
        for j, ch in enumerate(chunks(cols)):
            main_ref[base : base + own, :] = x[:, ch]
            base += own
            at = EDGE_ROWS + 2 * (f * (cols // LANES) + j)
            next_ref[at : at + 2, :] = x[own - 2 :, ch]
            prev_ref[at : at + 2, :] = x[:2, ch]


EDGE_ROWS = 16


def pack(pressure, soil_class, *ground):
    layers, own, cols = pressure.shape
    f32 = jnp.float32
    edge = jax.ShapeDtypeStruct((2, 2, layers, cols), f32)
    out = [edge, edge]
    if ground:
        height = ground[0].shape[0]
        strip = jax.ShapeDtypeStruct((EDGE_ROWS + 4 * cols // LANES, LANES), f32)
        out = [jax.ShapeDtypeStruct((5 * height + 2 * own * cols // LANES, LANES), f32), strip, strip] + out

    def body(p_ref, c_ref, *refs):
        if ground:
            surface_rows(p_ref, c_ref, *refs[:-2])
        soil_rows(p_ref, c_ref, *refs[-2:])

    return pl.pallas_call(body, out_shape=out, name="pack")(pressure, soil_class, *ground)


def surface_columns(main_ref, above_ref, below_ref, box, height, own, cols):
    n = cols // LANES
    tall = height + SUBS
    box[...] = jnp.zeros_like(box)
    for side, j in enumerate((n - 1, 0)):
        for f in range(2):
            at = (2 * side + f) * 2 * SUBS
            src = 5 * height + (f * n + j) * own
            strip = EDGE_ROWS + 2 * (f * n + j)
            box[at : at + own, :] = main_ref[src : src + own, :]
            box[at + own : at + own + 2, :] = below_ref[strip : strip + 2, :]
            box[at + own + 2 : at + own + 4, :] = above_ref[strip : strip + 2, :]
    for f in range(5):
        at = LANES + f * tall
        box[at : at + height, :] = main_ref[f * height : (f + 1) * height, :]
        box[at + height : at + height + 3, :] = below_ref[3 * f : 3 * f + 3, :]
        box[at + tall - 3 : at + tall, :] = above_ref[3 * f : 3 * f + 3, :]
    turned = box[...].T
    edges = jnp.concatenate([turned[LANES - 3 :], turned[:3], jnp.zeros((2, turned.shape[1]), jnp.float32)], axis=0)
    return edges


def columns(pressure, soil_class, up, down, surface):
    layers, own, cols = pressure.shape
    rows = own + SUBS
    last = cols // LANES - 1
    tile = [pl.BlockSpec((layers, own, LANES), lambda _, i=i: (0, 0, i)) for i in (0, 0, last, last)]
    halo = [pl.BlockSpec((2, 2, layers, LANES), lambda _, i=i: (0, 0, 0, i)) for i in (0, last, 0, last)]
    span = layers * rows
    scratch = [pltpu.VMEM((layers, rows, LANES), jnp.float32)]
    width = span
    if surface:
        height = (surface[0].shape[0] - 2 * own * cols // LANES) // 5
        tall = LANES + 5 * (height + SUBS)
        tall += -tall % LANES
        width += tall
        scratch.append(pltpu.VMEM((tall, LANES), jnp.float32))

    def body(*refs):
        n = 8 + len(surface)
        out_ref = refs[n]
        out_ref[:, :span] = soil_columns(*refs[:8], refs[n + 1])
        if surface:
            out_ref[:, span:] = surface_columns(*refs[8:n], refs[n + 2], height, own, cols)

    return pl.pallas_call(
        body,
        out_shape=jax.ShapeDtypeStruct((SUBS, width), jnp.float32),
        grid=(1,),
        in_specs=tile + halo + [pl.BlockSpec(memory_space=pltpu.VMEM)] * len(surface),
        scratch_shapes=scratch,
        name="columns",
    )(pressure, soil_class, pressure, soil_class, up, up, down, down, *surface)


def assemble(spot_ref, mains, strips, surf_ref, tops_ref, turn, own, height, count):
    _, rows, width = surf_ref.shape
    cols = width - LANES
    n = cols // LANES
    tall = height + SUBS
    strip = EDGE_ROWS + 4 * n
    lane = lax.broadcasted_iota(jnp.int32, (SUBS, LANES), 1)
    surf_ref[...] = jnp.zeros_like(surf_ref)
    tops_ref[...] = jnp.zeros_like(tops_ref)
    turn[...] = jnp.zeros_like(turn)
    for s in range(count):
        main, extra = mains[s], strips[s]
        who = spot_ref[4 + s]
        at = pl.multiple_of(who * LANES, LANES)
        first = pl.multiple_of(who * own, own)
        above, below = 0, strip
        for f in range(5):
            surf_ref[f, :height, pl.ds(at, LANES)] = main[f * height : (f + 1) * height, :]
            surf_ref[f, height : height + 3, pl.ds(at, LANES)] = extra[below + 3 * f : below + 3 * f + 3, :]
            surf_ref[f, rows - 3 :, pl.ds(at, LANES)] = extra[above + 3 * f : above + 3 * f + 3, :]
        for f in range(2):
            for j in range(n):
                src = 5 * height + (f * n + j) * own
                tops_ref[f, pl.ds(first, own), j * LANES : (j + 1) * LANES] = main[src : src + own, :]
        turn[LANES - 3 :, :LANES] = extra[2 * strip : 2 * strip + 3, :]
        turn[:3, :LANES] = extra[2 * strip + 3 : 2 * strip + 6, :]
        block = turn[:, :LANES].T
        for f in range(2):
            after = block[2 * (2 + f) * SUBS :][: 2 * SUBS]
            before = block[2 * f * SUBS :][: 2 * SUBS]
            two = jnp.where(lane >= LANES - 2, before[:SUBS], jnp.where(lane < 2, after[:SUBS], 0.0))
            more = jnp.where(lane >= LANES - 2, before[SUBS:], jnp.where(lane < 2, after[SUBS:], 0.0))
            tops_ref[f, pl.ds(first, own), cols:] = two

            @pl.when(who == 0)
            def _(f=f, more=more, extra=extra):
                tops_ref[f, height : height + 2, cols:] = more[:2]
                for j in range(n):
                    src = below + EDGE_ROWS + 2 * (f * n + j)
                    tops_ref[f, height : height + 2, j * LANES : (j + 1) * LANES] = extra[src : src + 2, :]

            @pl.when(who == count - 1)
            def _(f=f, more=more, extra=extra):
                tops_ref[f, rows - 2 :, cols:] = more[2:4]
                for j in range(n):
                    src = above + EDGE_ROWS + 2 * (f * n + j)
                    tops_ref[f, rows - 2 :, j * LANES : (j + 1) * LANES] = extra[src : src + 2, :]

        @pl.when(who == count - 1)
        def _(extra=extra):
            for j in range(1, turn.shape[1] // LANES):
                src = 2 * strip + j * SUBS
                turn[LANES - 3 :, j * LANES : (j + 1) * LANES] = extra[src : src + 3, :]

        @pl.when(who == 0)
        def _(extra=extra):
            for j in range(1, turn.shape[1] // LANES):
                src = 2 * strip + j * SUBS
                turn[:3, j * LANES : (j + 1) * LANES] = extra[src + 3 : src + 6, :]

    block = turn[:, LANES:].T
    for f in range(5):
        surf_ref[f, :, cols:] = block[f * tall : (f + 1) * tall]


def last_kernel(
    spot_ref, flags_ref, tab_ref, surf_ref, tops_ref, top_ref, class_ref, next_ref, head_out, water_ref,
    ex_ref, w_ref, new_ref, sem, own,
):
    _, rows, width = surf_ref.shape
    block_rows, block_cols = rows - SUBS, width - LANES
    r = lax.broadcasted_iota(jnp.int32, (rows, width), 0)
    c = lax.broadcasted_iota(jnp.int32, (rows, width), 1)
    row_ok = jnp.where(r < block_rows, 1, jnp.where(r >= rows - 3, spot_ref[2], jnp.where(r < block_rows + 3, spot_ref[3], 0)))
    col_ok = jnp.where(c < block_cols, 1, jnp.where(c >= width - 3, flags_ref[2], jnp.where(c < block_cols + 3, flags_ref[3], 0)))
    inside = (row_ok * col_ok).astype(jnp.float32)
    level = surf_ref[1]
    convey = jnp.sqrt(surf_ref[2]) * inside
    leak = surf_ref[3]
    rain = surf_ref[4]
    top = tops_ref[0]

    def across(x):
        return pltpu.roll(x, rows - 1, 0)

    def along(x):
        return pltpu.roll(x, width - 1, 1)

    gates = [convey * across(convey), convey * along(convey)]
    parts = []
    for ch in chunks(width):
        _, _, root = closure(params(tab_ref, tops_ref[1, :, ch].astype(jnp.int32)), top[:, ch])
        parts.append(0.25 * root * root)
    leak = leak * jnp.concatenate(parts, axis=1)
    water = surf_ref[0]
    exchange = jnp.zeros_like(water)
    for _ in range(PASSES):
        surface = level + water
        power = jnp.where(water > 0.0, jnp.exp2((5.0 / 3.0) * jnp.log2(jnp.maximum(water, 1e-30))), 0.0)
        outflow = jnp.zeros_like(water)
        for axis, gate, beside in ((0, gates[0], across), (1, gates[1], along)):
            slope = surface - beside(surface)
            carried = jnp.where(slope >= 0.0, power, beside(power))
            flux = gate * carried * slope * lax.rsqrt(jnp.maximum(jnp.abs(slope), SLOPE_FLOOR))
            outflow = outflow + flux - pltpu.roll(flux, 1, axis)
        rate = leak * (water - top)
        exchange = exchange + SURFACE_STEP * rate
        water = jnp.maximum(water + SURFACE_STEP * (rain - rate - outflow), 0.0)
    ex_ref[...] = exchange
    w_ref[...] = water
    if water_ref.shape[1] % LANES:
        water_ref[...] = w_ref[:block_rows, :block_cols]
    else:
        mine = pl.multiple_of(spot_ref[4] * water_ref.shape[1], LANES)
        water_ref[...] = w_ref[:block_rows, pl.ds(mine, water_ref.shape[1])]
    first = pl.multiple_of(spot_ref[0], SUBS)
    after = pl.multiple_of(spot_ref[0] + own, SUBS)
    before = pl.multiple_of(spot_ref[1], SUBS)
    sub = lax.broadcasted_iota(jnp.int32, (SUBS, width), 0)
    rim = jnp.where(sub == SUBS - 1, ex_ref[pl.ds(before, SUBS), :], jnp.where(sub == 0, ex_ref[pl.ds(after, SUBS), :], 0.0))
    gain = jnp.concatenate([ex_ref[pl.ds(first, own), :], rim], axis=0)
    mask = soil_mask(flags_ref, own + SUBS, width, own, block_cols)
    p = top_ref[0] + gain * top_ref[1]
    content, capacity, root = wide([closure(params(tab_ref, class_ref[:, ch]), p[:, ch]) for ch in chunks(width)])
    h = root * mask
    q = h * p
    low, low_q, low_n, low_d, weights, flows = (next_ref[i] for i in range(6))

    def tile(x):
        return x[:own, :block_cols]

    top_n = tile(capacity * p - (content - top_ref[2]) + gain + h * lateral(q)) + tile(h) * (low_q - GRAVITY_STEP * low)
    new_ref[0] = top_n / (tile(capacity + h * lateral(h)) + tile(h) * low)
    low_n = low_n + low * (flows + tile(q) + GRAVITY_STEP * tile(h))
    new_ref[1] = low_n / (low_d + low * (weights + tile(h)))
    copy = pltpu.make_async_copy(new_ref, head_out.at[:TOP_LAYERS], sem)
    copy.start()
    copy.wait()


def finish(spot, flags, tables, fields, tops, head, block, count):
    own = head.shape[1]
    whole = count == 0
    rows, width = block[0] + SUBS, block[1] + LANES
    n = len(fields)

    def body(spot_ref, flags_ref, tab_ref, *refs):
        given, known, (head_out, water_ref), (box, turn), rest = refs[:n], refs[n : n + 3], refs[n + 4 : n + 6], refs[n + 6 : n + 8], refs[n + 8 :]
        if whole:
            surf, tops = given
        else:
            surf, tops = box
            cut = given[0].shape[0] - 2 * (EDGE_ROWS + 4 * block[1] // LANES) - turn.shape[1] // LANES * SUBS
            assemble(spot_ref, [x.at[:cut] for x in given], [x.at[cut:] for x in given], surf, tops, turn, own, block[0], count)
        last_kernel(spot_ref, flags_ref, tab_ref, surf, tops, *known, head_out, water_ref, *rest, own=own)

    def scratch_body(*refs):
        cut = 3 + n + 6
        body(*refs[:cut], refs[cut : cut + 2], refs[cut + 2], *refs[cut + 3 :])

    tall = LANES + 5 * (block[0] + SUBS)
    tall += -tall % LANES
    small = (1, SUBS, LANES)
    vmem = pl.BlockSpec(memory_space=pltpu.VMEM)
    smem = pl.BlockSpec(memory_space=pltpu.SMEM)
    water = block if whole else (block[0], LANES)
    return pl.pallas_call(
        scratch_body,
        out_shape=(
            jax.ShapeDtypeStruct(head.shape, jnp.float32),
            jax.ShapeDtypeStruct(water, jnp.float32),
        ),
        in_specs=[smem, smem] + [vmem] * (n + 4) + [pl.BlockSpec(memory_space=pl.ANY)],
        out_specs=[pl.BlockSpec(memory_space=pl.ANY), vmem],
        scratch_shapes=[
            pltpu.VMEM(small if whole else (5, rows, width), jnp.float32),
            pltpu.VMEM(small if whole else (2, rows, width), jnp.float32),
            pltpu.VMEM((SUBS, LANES) if whole else (LANES, tall), jnp.float32),
            pltpu.VMEM((rows, width), jnp.float32),
            pltpu.VMEM((rows, width), jnp.float32),
            pltpu.VMEM((TOP_LAYERS, own, block[1]), jnp.float32),
            pltpu.SemaphoreType.DMA,
        ],
        input_output_aliases={n + 6: 0},
        name="surface_and_top",
    )(spot, flags, tables, *fields, *tops, head)


def lane_rows(size):
    return -(-size // LANES)


def as_lanes(x):
    if x.shape[-1] % LANES:
        x = jnp.pad(x.reshape(-1), (0, -x.size % LANES))
    return x.reshape(-1, LANES)


def from_lanes(x, shape):
    if shape[-1] % LANES:
        size = 1
        for length in shape:
            size *= length
        x = x.reshape(-1)[:size]
    return x.reshape(shape)


def gx_trade(edges, half):
    got = shift(edges, "gx", 1)
    if lax.axis_size("gx") == 2:
        return got
    return jnp.where(half, got, shift(edges, "gx", -1))


def cyclic_rows(mid, above, below, gap):
    hole = jnp.zeros(mid.shape[:-2] + (gap, mid.shape[-1]), mid.dtype)
    return jnp.concatenate([mid, below, hole, above], axis=-2)


def block_general(pressure, soil_class, depth, elevation, roughness, rain, land_mask, channel_mask):
    ny = lax.axis_size("gy")
    _, own, cols = pressure.shape
    srows, scols = depth.shape
    convey = (1.0 + channel_mask.astype(jnp.float32)) / roughness
    surf = jnp.stack([depth, elevation, convey, LEAKANCE * land_mask.astype(jnp.float32), rain])
    tops = jnp.stack([pressure[0], soil_class[0].astype(jnp.float32)])

    def pack(s, t):
        return jnp.concatenate([as_lanes(s), as_lanes(t)], axis=0)

    def unpack(m):
        cut = lane_rows(15 * scols)
        return from_lanes(m[:cut], (5, 3, scols)), from_lanes(m[cut:], (2, 2, cols))

    s_above, t_above = unpack(shift(pack(surf[:, -3:], tops[:, -2:]), "grp", 1))
    s_below, t_below = unpack(shift(pack(surf[:, :3], tops[:, :2]), "grp", -1))
    surf_rows = cyclic_rows(surf, s_above, s_below, 2)
    tops_rows = jnp.concatenate([tops, t_below, t_above], axis=1)

    def edges(cut):
        a = surf_rows[:, :, cut(3)].transpose(0, 2, 1).reshape(15, -1)
        b = tops_rows[:, :, cut(2)].transpose(0, 2, 1).reshape(4, -1)
        return jnp.concatenate([a, jnp.pad(b, ((0, 0), (0, a.shape[1] - b.shape[1])))], axis=0)

    out = jnp.concatenate([edges(lambda n: slice(-n, None)), edges(lambda n: slice(0, n))])
    got = gx_trade(out, lax.broadcasted_iota(jnp.int32, out.shape, 0) < 19)
    mine = jnp.concatenate(
        [as_lanes(surf_rows), as_lanes(tops_rows), jnp.pad(got, ((0, 0), (0, -got.shape[1] % LANES))).reshape(-1, LANES)]
    )
    every = lax.all_gather(mine, "gy", axis=0, tiled=False)
    n1 = lane_rows(surf_rows.size)
    n2 = n1 + lane_rows(tops_rows.size)
    e_surf = jax.vmap(lambda m: from_lanes(m, (5, srows + SUBS, scols)))(every[:, :n1])
    e_surf = e_surf.transpose(1, 2, 0, 3).reshape(5, srows + SUBS, ny * scols)
    e_tops = every[:, n1:n2].reshape(ny, 2, own + 4, cols)
    e_m = every[:, n2:].reshape(ny, 2, 19, -1)
    main = e_tops[:, :, :own].transpose(1, 0, 2, 3).reshape(2, srows, cols)
    zeros = jnp.zeros((2, 4, cols), jnp.float32)
    f_tops = jnp.concatenate([main, e_tops[0, :, own : own + 2], zeros, e_tops[-1, :, own + 2 :]], axis=1)
    height = srows + SUBS
    c_left = e_m[-1, 0, :15, :height].reshape(5, 3, height).transpose(0, 2, 1)
    c_right = e_m[0, 1, :15, :height].reshape(5, 3, height).transpose(0, 2, 1)
    hole = jnp.zeros((5, height, LANES - 6), jnp.float32)
    blocks = jnp.concatenate([e_surf, c_right, hole, c_left], axis=2)

    def tops_edge(side):
        t = e_m[:, side, 15:, : own + 4].reshape(ny, 2, 2, own + 4)
        mid = t[..., :own].transpose(1, 0, 3, 2).reshape(2, srows, 2)
        low = t[0, :, :, own : own + 2].transpose(0, 2, 1)
        high = t[-1, :, :, own + 2 :].transpose(0, 2, 1)
        return jnp.concatenate([mid, low, jnp.zeros((2, 4, 2), jnp.float32), high], axis=1)

    return blocks, jnp.concatenate(
        [f_tops, tops_edge(1), jnp.zeros((2, height, LANES - 4), jnp.float32), tops_edge(0)], axis=2
    )


def local(
    pressure, soil_class, capacity_range, inverse_entry, shape_index, conductivity,
    depth, elevation, roughness, rain, land_mask, channel_mask,
):
    ng, nx, ny = (lax.axis_size(a) for a in ("grp", "gx", "gy"))
    ig, ix, iy = (lax.axis_index(a) for a in ("grp", "gx", "gy"))
    _, own, cols = pressure.shape
    srows, scols = depth.shape
    ground = (depth, elevation, roughness, rain, land_mask, channel_mask)
    tables = class_tables(capacity_range, inverse_entry, shape_index, conductivity)
    tile = ig * ny + iy
    flags = jnp.stack([tile > 0, tile < ng * ny - 1, ix > 0, ix < nx - 1]).astype(jnp.int32)
    spot = [iy * own, jnp.where(iy > 0, iy * own - SUBS, srows), (ig > 0).astype(jnp.int32), (ig < ng - 1).astype(jnp.int32)]
    spot = jnp.stack(spot + [(iy - step) % ny for step in range(ny)])

    even = scols == LANES and own == SUBS
    if even:
        main, strip_after, strip_before, after, before = pack(pressure, soil_class, *ground)
        above = shift(strip_after, "grp", 1)
        below = shift(strip_before, "grp", -1)
        surface = (main, above, below)
    else:
        after, before = pack(pressure, soil_class)
        surface = ()
    up = shift(after, ("grp", "gy"), 1)
    down = shift(before, ("grp", "gy"), -1)
    sent = columns(pressure, soil_class, up, down, surface)
    span = pressure.shape[0] * (own + SUBS)
    half = jnp.where(lax.broadcasted_iota(jnp.int32, sent.shape, 1) < span, 4, 3)
    got = gx_trade(sent, lax.broadcasted_iota(jnp.int32, sent.shape, 0) < half)
    if even:
        strip = jnp.concatenate([above, below] + [got[:, ch] for ch in chunks(sent.shape[1])[span // LANES :]], axis=0)
        strip = jnp.concatenate([main, strip], axis=0)
        fields = [strip] + [shift(strip, "gy", step) for step in range(1, ny)]
    else:
        fields = block_general(pressure, soil_class, *ground)
    head, *tops = soil_interior(flags, tables, pressure, soil_class, up, down, got, sent)
    head, water = finish(spot, flags, tables, fields, tops, head, (srows, cols), ny if even else 0)
    if not even:
        water = lax.dynamic_slice_in_dim(water, iy * scols, scols, axis=1)
    return head, water


def solution(mesh):
    soil = P(None, ("grp", "gy"), "gx")
    ground = P("grp", ("gx", "gy"))
    return jax.shard_map(
        local,
        mesh=mesh,
        in_specs=(soil, soil, P(), P(), P(), P()) + (ground,) * 6,
        out_specs=(soil, ground),
        check_vma=False,
    )
```

```python
import jax
import jax.numpy as jnp
from jax import lax
from jax.experimental import pallas as pl
from jax.experimental.pallas import tpu as pltpu
from jax.sharding import PartitionSpec as P

PASSES = 3
STORAGE = 0.01
GRAVITY_STEP = 0.5
SUCTION_FLOOR = 0.01
SLOPE_FLOOR = 0.1
SURFACE_STEP = 0.3
LEAKANCE = 0.5

LANES = 128
SUBS = 8
UNROLL = 4
TOP_LAYERS = 2


def shift(x, axis, step):
    size = lax.axis_size(axis)
    return lax.ppermute(x, axis, [(i, (i + step) % size) for i in range(size)])


def class_tables(refs):
    lane = lax.broadcasted_iota(jnp.int32, (1, LANES), 1)
    spread = []
    for ref in refs:
        row = jnp.ones((1, LANES), jnp.float32)
        for k in range(ref.shape[0]):
            row = jnp.where(lane == k, ref[k], row)
        spread.append(row)
    span, entry, shape, ks = spread
    pore = 1.0 - 1.0 / shape
    rows = [-entry, 1.0 / (1.0 - pore), pore, span, 2.0 * jnp.sqrt(ks)]
    return jnp.concatenate(rows + [jnp.zeros((SUBS - len(rows), LANES), jnp.float32)], axis=0)


def place():
    tile = lax.axis_index("grp") * lax.axis_size("gy") + lax.axis_index("gy")
    tiles = lax.axis_size("grp") * lax.axis_size("gy")
    column, columns = lax.axis_index("gx"), lax.axis_size("gx")
    tests = (tile > 0, tile < tiles - 1, column > 0, column < columns - 1)
    return [jnp.where(t, 1, 0) for t in tests]


def params(tab_ref, idx):
    return [
        jnp.take_along_axis(jnp.broadcast_to(tab_ref[i : i + 1, :], idx.shape), idx, axis=1, mode="promise_in_bounds")
        for i in range(5)
    ]


def closure(given, p):
    entry, expo, pore, span, scale = given
    logs = jnp.log2(jnp.maximum(entry * p, SUCTION_FLOOR))
    total = jnp.log2(1.0 + jnp.exp2(expo * logs))
    drop = pore * total
    less = expo - 1.0
    power = less * logs - drop
    ratio = jnp.exp2(power)
    content = span * jnp.exp2(-drop)
    capacity = STORAGE - (span * entry * less) * jnp.exp2(power - total)
    root = scale * jnp.exp2(-0.25 * drop) * jnp.abs(1.0 - ratio)
    return content, capacity, root


def chunks(width):
    return [slice(i, i + LANES) for i in range(0, width, LANES)]


def wide(parts):
    return [jnp.concatenate(x, axis=1) for x in zip(*parts)]


def lateral(x):
    rows, width = x.shape
    return (
        pltpu.roll(x, 1, 0)
        + pltpu.roll(x, rows - 1, 0)
        + pltpu.roll(x, 1, 1)
        + pltpu.roll(x, width - 1, 1)
    )


def soil_mask(ok, rows, width, own_rows, own_cols):
    r = lax.broadcasted_iota(jnp.int32, (rows, width), 0)
    c = lax.broadcasted_iota(jnp.int32, (rows, width), 1)
    above = jnp.where(r >= rows - 2, ok[0], 0)
    below = jnp.where((r >= own_rows) & (r < own_rows + 2), ok[1], 0)
    left = jnp.where(c >= width - 2, ok[2], 0)
    right = jnp.where((c >= own_cols) & (c < own_cols + 2), ok[3], 0)
    in_rows = jnp.where(r < own_rows, 1, above + below)
    in_cols = jnp.where(c < own_cols, 1, left + right)
    return (in_rows * in_cols).astype(jnp.float32)


def soil_rows(p_ref, c_ref, next_ref, prev_ref, next_end, prev_end):
    layers, own, cols = p_ref.shape
    start = lax.broadcasted_iota(jnp.int32, (layers, LANES), 1) < LANES // 2
    for f, x in enumerate((p_ref, c_ref)):
        for r in range(2):
            next_ref[f, r] = x[:, own - 2 + r, :].astype(jnp.float32)
            prev_ref[f, r] = x[:, r, :].astype(jnp.float32)
        next_end[f] = jnp.where(start, next_ref[f, 1, :, :LANES], next_ref[f, 1, :, cols - LANES :])
        prev_end[f] = jnp.where(start, prev_ref[f, 0, :, :LANES], prev_ref[f, 0, :, cols - LANES :])


def soil_columns(p_first, c_first, p_last, c_last, up_end, down_end, box):
    layers, own, _ = p_first.shape
    rows = box.shape[1]
    out = []
    for side in ((p_last, c_last), (p_first, c_first)):
        for f in range(2):
            box[:, 2 : 2 + own, :] = side[f][...].astype(jnp.float32)
            box[:, 0, :] = jnp.zeros((layers, LANES), jnp.float32)
            box[:, 1, :] = up_end[f]
            box[:, own + 2, :] = down_end[f]
            box[:, own + 3 :, :] = jnp.zeros((layers, rows - own - 3, LANES), jnp.float32)
            turned = box[...].reshape(layers * rows, LANES).T
            out.append(turned[LANES - 2 :] if len(out) < 2 else turned[:2])
    return jnp.concatenate(out, axis=0)


def soil_kernel(
    tab_ref, p_in, c_in, up_in, down_in, got, sent, out_ref, top_out, class_out, next_out,
    h_ref, q_ref, n_ref, d_ref, k_ref, h2_ref, q2_ref, n2_ref, d2_ref, given, corner, turn, near, near2, pe, ce,
):
    layers, own, cols = p_in.shape
    rows = own + SUBS
    span = layers * rows
    f32 = jnp.float32
    ok = place()
    for ref in (h_ref, q_ref, h2_ref, q2_ref):
        ref[0] = jnp.zeros((own, cols), f32)
        ref[layers + 1] = jnp.zeros((own, cols), f32)

    def first(z, carry):
        for ch in chunks(cols):
            p = p_in[z, :, ch]
            values = params(tab_ref, c_in[z, :, ch])
            for i, v in enumerate(values):
                given[i, z, :, ch] = v
            content, capacity, root = closure(values, p)
            h_ref[z + 1, :, ch] = root
            q_ref[z + 1, :, ch] = root * p
            n_ref[z, :, ch] = capacity * p
            d_ref[z, :, ch] = capacity
            k_ref[z, :, ch] = content
        return carry

    lax.fori_loop(0, layers, first, 0, unroll=UNROLL)

    gap = jnp.zeros((1, span), f32)
    p = jnp.concatenate([got[0:2], sent[4:5], gap, sent[1:2], got[4:6], gap], axis=0)
    kind = jnp.concatenate([got[2:4], sent[6:7], gap, sent[3:4], got[6:8], gap], axis=0).astype(jnp.int32)
    sub = lax.broadcasted_iota(jnp.int32, (SUBS, span), 0)
    lane = lax.broadcasted_iota(jnp.int32, (SUBS, span), 1)
    row = lane % rows
    row_ok = jnp.where(row < 2, ok[0], jnp.where(row < own + 2, 1, jnp.where(row < own + 4, ok[1], 0)))
    col_ok = jnp.where(sub < 2, ok[2], jnp.where((sub == 2) | (sub == 4), 1, jnp.where((sub == 5) | (sub == 6), ok[3], 0)))
    mask = (row_ok * col_ok).astype(f32)
    values = [params(tab_ref, kind[:, ch]) for ch in chunks(span)]
    content, capacity, root = wide([closure(v, p[:, ch]) for v, ch in zip(values, chunks(span))])
    h, q = root * mask, root * mask * p

    def over(x):
        return jnp.where(lane < rows, 0.0, pltpu.roll(x, rows, 1))

    def under(x):
        return jnp.where(lane >= span - rows, 0.0, pltpu.roll(x, span - rows, 1))

    weights = lateral(h) + over(h) + under(h)
    flows = lateral(q) + over(q) + under(q) + GRAVITY_STEP * (over(h) - under(h))
    p1 = (capacity * p + h * flows) / (capacity + h * weights)
    root = wide([closure(v, p1[:, ch]) for v, ch in zip(values, chunks(span))])[2] * mask
    turn[...] = jnp.zeros_like(turn)
    for i, x in enumerate((h, q, root, root * p1)):
        turn[i * SUBS : (i + 1) * SUBS, :] = x
    corner[...] = turn[...].T.reshape(layers, rows, LANES)

    zsub = lax.broadcasted_iota(jnp.int32, (layers, cols), 0)
    zlane = lax.broadcasted_iota(jnp.int32, (layers, LANES), 1)

    def sides(x, edge, at, lanes):
        left, right = pltpu.roll(x, 1, 1), pltpu.roll(x, cols - 1, 1)
        a = jnp.where(lanes == 0, pltpu.roll(edge, LANES - at, 1), left[:, :LANES])
        b = jnp.where(lanes == LANES - 1, pltpu.roll(edge, LANES - 1 - (at + 4), 1), right[:, cols - LANES :])
        return jnp.concatenate([a, left[:, LANES:]], axis=1) + jnp.concatenate([right[:, : cols - LANES], b], axis=1)

    for side, (halo, close, far, edge_row, valid) in enumerate(((up_in, 1, 0, 1, ok[0]), (down_in, 0, 1, own + 2, ok[1]))):
        inside = valid.astype(f32)
        ours = 0 if side == 0 else own - 1
        values, states, beyond = [], [], []
        for ch in chunks(cols):
            p = halo[0, close, :, ch]
            v = params(tab_ref, halo[1, close, :, ch].astype(jnp.int32))
            content, capacity, root = closure(v, p)
            root = root * inside
            values.append(v)
            states.append((p, capacity, root, root * p))
            p = halo[0, far, :, ch]
            root = closure(params(tab_ref, halo[1, far, :, ch].astype(jnp.int32)), p)[2] * inside
            beyond.append((root, root * p))
        p, capacity, h, q = wide(states)
        far_h, far_q = wide(beyond)
        near[side, 0] = h
        near[side, 1] = q
        edge = corner[:, edge_row, :]
        top_h = jnp.where(zsub == 0, 0.0, pltpu.roll(h, 1, 0))
        low_h = jnp.where(zsub == layers - 1, 0.0, pltpu.roll(h, layers - 1, 0))
        top_q = jnp.where(zsub == 0, 0.0, pltpu.roll(q, 1, 0))
        low_q = jnp.where(zsub == layers - 1, 0.0, pltpu.roll(q, layers - 1, 0))
        weights = far_h + h_ref[1 : layers + 1, ours, :] + sides(h, edge, 1, zlane) + top_h + low_h
        flows = far_q + q_ref[1 : layers + 1, ours, :] + sides(q, edge, 1 + SUBS, zlane) + top_q + low_q + GRAVITY_STEP * (top_h - low_h)
        p1 = (capacity * p + h * flows) / (capacity + h * weights)
        for v, ch in zip(values, chunks(cols)):
            root = closure(v, p1[:, ch])[2] * inside
            near2[side, 0, :, ch] = root
            near2[side, 1, :, ch] = root * p1[:, ch]

    tsub = lax.broadcasted_iota(jnp.int32, (own, cols), 0)
    tlane = lax.broadcasted_iota(jnp.int32, (own, LANES), 1)

    def around(z, h, q, rim, at):
        edge = corner[z, 2 : 2 + own, :]
        out = []
        for i, x in enumerate((h[z + 1], q[z + 1])):
            above = jnp.where(tsub == 0, rim[0, i, pl.ds(z, 1), :], pltpu.roll(x, 1, 0))
            below = jnp.where(tsub == own - 1, rim[1, i, pl.ds(z, 1), :], pltpu.roll(x, own - 1, 0))
            out.append(above + below + sides(x, edge, at + i * SUBS, tlane))
        weights, flows = out
        low = h[z + 2]
        return weights + low, flows + q[z + 2] - GRAVITY_STEP * low

    def second(z, carry):
        mid, top = h_ref[z + 1], h_ref[z]
        weights, flows = around(z, h_ref, q_ref, near, 1)
        flows = flows + q_ref[z] + GRAVITY_STEP * top
        p1 = (n_ref[z] + mid * flows) / (d_ref[z] + mid * (weights + top))
        for ch in chunks(cols):
            p = p1[:, ch]
            content, capacity, root = closure([given[i, z, :, ch] for i in range(5)], p)
            h2_ref[z + 1, :, ch] = root
            q2_ref[z + 1, :, ch] = root * p
            n2_ref[z, :, ch] = capacity * p - (content - k_ref[z, :, ch])
            d2_ref[z, :, ch] = capacity
        return carry

    lax.fori_loop(0, layers, second, 0, unroll=UNROLL)

    def third(z, carry):
        mid, top = h2_ref[z + 1], h2_ref[z]
        weights, flows = around(z, h2_ref, q2_ref, near2, 1 + 2 * SUBS)
        flows = flows + q2_ref[z] + GRAVITY_STEP * top
        out_ref[z] = (n2_ref[z] + mid * flows) / (d2_ref[z] + mid * (weights + top))
        return carry

    lax.fori_loop(0, layers, third, 0, unroll=UNROLL)

    weights, flows = around(1, h2_ref, q2_ref, near2, 1 + 2 * SUBS)
    for i, x in enumerate((h2_ref[2], q2_ref[2], n2_ref[1], d2_ref[1], weights, flows)):
        next_out[i] = x
    for f, (src, dst, halo_at) in enumerate(((p_in, pe, 0), (c_in, ce, 2))):
        turn[...] = jnp.zeros_like(turn)
        turn[LANES - 2 :, :] = got[halo_at : halo_at + 2]
        turn[:2, :] = got[halo_at + 4 : halo_at + 6]
        block = turn[:, :LANES].T
        for z in range(2):
            dst[z, own:, :cols] = jnp.zeros((SUBS, cols), dst.dtype)
            dst[z, :own, :cols] = src[z]
            dst[z, :, cols:] = jnp.zeros((rows, LANES), dst.dtype)
            dst[z, : own + 2, cols:] = block[z * rows + 2 : z * rows + own + 4].astype(dst.dtype)
            dst[z, rows - 2 :, cols:] = block[z * rows : z * rows + 2].astype(dst.dtype)
            for r in range(2):
                dst[z, own + r : own + r + 1, :cols] = down_in[f, r, z : z + 1, :].astype(dst.dtype)
                dst[z, rows - 2 + r : rows - 1 + r, :cols] = up_in[f, r, z : z + 1, :].astype(dst.dtype)
    width = cols + LANES
    mask = soil_mask(ok, rows, width, own, cols)
    states = []
    for z in range(2):
        content, capacity, root = wide([closure(params(tab_ref, ce[z, :, ch]), pe[z, :, ch]) for ch in chunks(width)])
        states.append((content, capacity, root * mask))
    content, capacity, h = states[0]
    low = states[1][2]
    weights = lateral(h) + low
    flows = lateral(h * pe[0]) + low * pe[1] - GRAVITY_STEP * low
    weight = capacity + h * weights
    top_out[0] = (capacity * pe[0] + h * flows) / weight
    top_out[1] = 1.0 / weight
    top_out[2] = content
    class_out[...] = ce[0]


def soil_interior(tables, pressure, soil_class, up, down, got, sent):
    layers, own, cols = pressure.shape
    rows, width = own + SUBS, cols + LANES
    f32 = jnp.float32
    span = layers * rows
    tall = pltpu.VMEM((layers + 2, own, cols), f32)
    flat = pltpu.VMEM((layers, own, cols), f32)
    edge = pl.BlockSpec((SUBS, span), lambda _: (0, 0))
    vmem = pl.BlockSpec(memory_space=pltpu.VMEM)
    return pl.pallas_call(
        soil_kernel,
        out_shape=(
            jax.ShapeDtypeStruct(pressure.shape, f32),
            jax.ShapeDtypeStruct((3, rows, width), f32),
            jax.ShapeDtypeStruct((rows, width), jnp.int32),
            jax.ShapeDtypeStruct((6, own, cols), f32),
        ),
        grid=(1,),
        in_specs=[vmem] * 5 + [edge, edge],
        out_specs=[vmem] * 4,
        scratch_shapes=[tall, tall, flat, flat, flat, tall, tall, flat, flat]
        + [
            pltpu.VMEM((5, layers, own, cols), f32),
            pltpu.VMEM((layers, rows, LANES), f32),
            pltpu.VMEM((LANES, span), f32),
            pltpu.VMEM((2, 2, layers, cols), f32),
            pltpu.VMEM((2, 2, layers, cols), f32),
            pltpu.VMEM((2, rows, width), f32),
            pltpu.VMEM((2, rows, width), jnp.int32),
        ],
        name="soil_interior",
    )(tables, pressure, soil_class, up, down, got, sent)


def surface_rows(p_ref, c_ref, depth, level, rough, rain, land, channel, main_ref, next_ref, prev_ref):
    height, width = depth.shape
    _, own, cols = p_ref.shape
    fields = (
        depth[...],
        level[...],
        (1.0 + channel[...].astype(jnp.float32)) / rough[...],
        LEAKANCE * land[...].astype(jnp.float32),
        rain[...],
    )
    for f, x in enumerate(fields):
        main_ref[f * height : (f + 1) * height, :] = x
        next_ref[3 * f : 3 * f + 3, :] = x[height - 3 :]
        prev_ref[3 * f : 3 * f + 3, :] = x[:3]
    base = 5 * height
    for f, x in enumerate((p_ref[0], c_ref[0].astype(jnp.float32))):
        for j, ch in enumerate(chunks(cols)):
            main_ref[base : base + own, :] = x[:, ch]
            base += own
            at = EDGE_ROWS + 2 * (f * (cols // LANES) + j)
            next_ref[at : at + 2, :] = x[own - 2 :, ch]
            prev_ref[at : at + 2, :] = x[:2, ch]


EDGE_ROWS = 16


def pack(pressure, soil_class, classes, ground):
    layers, own, cols = pressure.shape
    f32 = jnp.float32
    edge = jax.ShapeDtypeStruct((2, 2, layers, cols), f32)
    end = jax.ShapeDtypeStruct((2, layers, LANES), f32)
    out = [edge, edge, end, end]
    if ground:
        height = ground[0].shape[0]
        strip = jax.ShapeDtypeStruct((EDGE_ROWS + 4 * cols // LANES, LANES), f32)
        out = [jax.ShapeDtypeStruct((5 * height + 2 * own * cols // LANES, LANES), f32), strip, strip] + out

    def body(*refs):
        tables, rest = refs[: len(classes)], refs[len(classes) :]
        if ground:
            surface_rows(*rest[: 2 + len(ground)], *rest[3 + len(ground) : 6 + len(ground)])
        soil_rows(*rest[:2], *rest[-4:])
        rest[2 + len(ground)][...] = class_tables(tables)

    vmem = pl.BlockSpec(memory_space=pltpu.VMEM)
    smem = pl.BlockSpec(memory_space=pltpu.SMEM)
    return pl.pallas_call(
        body,
        out_shape=[jax.ShapeDtypeStruct((SUBS, LANES), f32)] + out,
        in_specs=[smem] * len(classes) + [vmem] * (2 + len(ground)),
        name="pack",
    )(*classes, pressure, soil_class, *ground)


def surface_columns(main_ref, above_ref, below_ref, box, height, own, cols):
    n = cols // LANES
    tall = height + SUBS
    box[...] = jnp.zeros_like(box)
    for side, j in enumerate((n - 1, 0)):
        for f in range(2):
            at = (2 * side + f) * 2 * SUBS
            src = 5 * height + (f * n + j) * own
            strip = EDGE_ROWS + 2 * (f * n + j)
            box[at : at + own, :] = main_ref[src : src + own, :]
            box[at + own : at + own + 2, :] = below_ref[strip : strip + 2, :]
            box[at + own + 2 : at + own + 4, :] = above_ref[strip : strip + 2, :]
    for f in range(5):
        at = LANES + f * tall
        box[at : at + height, :] = main_ref[f * height : (f + 1) * height, :]
        box[at + height : at + height + 3, :] = below_ref[3 * f : 3 * f + 3, :]
        box[at + tall - 3 : at + tall, :] = above_ref[3 * f : 3 * f + 3, :]
    turned = box[...].T
    edges = jnp.concatenate([turned[LANES - 3 :], turned[:3], jnp.zeros((2, turned.shape[1]), jnp.float32)], axis=0)
    return edges


def columns(pressure, soil_class, up_end, down_end, surface):
    layers, own, cols = pressure.shape
    rows = own + SUBS
    last = cols // LANES - 1
    tile = [pl.BlockSpec((layers, own, LANES), lambda _, i=i: (0, 0, i)) for i in (0, 0, last, last)]
    span = layers * rows
    scratch = [pltpu.VMEM((layers, rows, LANES), jnp.float32)]
    width = span
    if surface:
        height = (surface[0].shape[0] - 2 * own * cols // LANES) // 5
        tall = LANES + 5 * (height + SUBS)
        tall += -tall % LANES
        width += tall
        scratch.append(pltpu.VMEM((tall, LANES), jnp.float32))

    def body(*refs):
        n = 6 + len(surface)
        out_ref = refs[n]
        out_ref[:, :span] = soil_columns(*refs[:6], refs[n + 1])
        if surface:
            out_ref[:, span:] = surface_columns(*refs[6:n], refs[n + 2], height, own, cols)

    return pl.pallas_call(
        body,
        out_shape=jax.ShapeDtypeStruct((SUBS, width), jnp.float32),
        grid=(1,),
        in_specs=tile + [pl.BlockSpec(memory_space=pltpu.VMEM)] * (2 + len(surface)),
        scratch_shapes=scratch,
        name="columns",
    )(pressure, soil_class, pressure, soil_class, up_end, down_end, *surface)


def assemble(mains, strips, surf_ref, tops_ref, turn, own, height, count):
    _, rows, width = surf_ref.shape
    cols = width - LANES
    n = cols // LANES
    tall = height + SUBS
    strip = EDGE_ROWS + 4 * n
    lane = lax.broadcasted_iota(jnp.int32, (SUBS, LANES), 1)
    surf_ref[...] = jnp.zeros_like(surf_ref)
    tops_ref[...] = jnp.zeros_like(tops_ref)
    turn[...] = jnp.zeros_like(turn)
    for s in range(count):
        main, extra = mains[s], strips[s]
        who = (lax.axis_index("gy") - s) % count
        at = pl.multiple_of(who * LANES, LANES)
        first = pl.multiple_of(who * own, own)
        above, below = 0, strip
        for f in range(5):
            surf_ref[f, :height, pl.ds(at, LANES)] = main[f * height : (f + 1) * height, :]
            surf_ref[f, height : height + 3, pl.ds(at, LANES)] = extra[below + 3 * f : below + 3 * f + 3, :]
            surf_ref[f, rows - 3 :, pl.ds(at, LANES)] = extra[above + 3 * f : above + 3 * f + 3, :]
        for f in range(2):
            for j in range(n):
                src = 5 * height + (f * n + j) * own
                tops_ref[f, pl.ds(first, own), j * LANES : (j + 1) * LANES] = main[src : src + own, :]
        turn[LANES - 3 :, :LANES] = extra[2 * strip : 2 * strip + 3, :]
        turn[:3, :LANES] = extra[2 * strip + 3 : 2 * strip + 6, :]
        block = turn[:, :LANES].T
        for f in range(2):
            after = block[2 * (2 + f) * SUBS :][: 2 * SUBS]
            before = block[2 * f * SUBS :][: 2 * SUBS]
            two = jnp.where(lane >= LANES - 2, before[:SUBS], jnp.where(lane < 2, after[:SUBS], 0.0))
            more = jnp.where(lane >= LANES - 2, before[SUBS:], jnp.where(lane < 2, after[SUBS:], 0.0))
            tops_ref[f, pl.ds(first, own), cols:] = two

            @pl.when(who == 0)
            def _(f=f, more=more, extra=extra):
                tops_ref[f, height : height + 2, cols:] = more[:2]
                for j in range(n):
                    src = below + EDGE_ROWS + 2 * (f * n + j)
                    tops_ref[f, height : height + 2, j * LANES : (j + 1) * LANES] = extra[src : src + 2, :]

            @pl.when(who == count - 1)
            def _(f=f, more=more, extra=extra):
                tops_ref[f, rows - 2 :, cols:] = more[2:4]
                for j in range(n):
                    src = above + EDGE_ROWS + 2 * (f * n + j)
                    tops_ref[f, rows - 2 :, j * LANES : (j + 1) * LANES] = extra[src : src + 2, :]

        @pl.when(who == count - 1)
        def _(extra=extra):
            for j in range(1, turn.shape[1] // LANES):
                src = 2 * strip + j * SUBS
                turn[LANES - 3 :, j * LANES : (j + 1) * LANES] = extra[src : src + 3, :]

        @pl.when(who == 0)
        def _(extra=extra):
            for j in range(1, turn.shape[1] // LANES):
                src = 2 * strip + j * SUBS
                turn[:3, j * LANES : (j + 1) * LANES] = extra[src + 3 : src + 6, :]

    block = turn[:, LANES:].T
    for f in range(5):
        surf_ref[f, :, cols:] = block[f * tall : (f + 1) * tall]


def last_kernel(
    tab_ref, surf_ref, tops_ref, top_ref, class_ref, next_ref, head_out, water_ref,
    ex_ref, w_ref, new_ref, sem, own,
):
    _, rows, width = surf_ref.shape
    block_rows, block_cols = rows - SUBS, width - LANES
    r = lax.broadcasted_iota(jnp.int32, (rows, width), 0)
    c = lax.broadcasted_iota(jnp.int32, (rows, width), 1)
    ok = place()
    group, groups, line = lax.axis_index("grp"), lax.axis_size("grp"), lax.axis_index("gy")
    more = [jnp.where(t, 1, 0) for t in (group > 0, group < groups - 1)]
    row_ok = jnp.where(r < block_rows, 1, jnp.where(r >= rows - 3, more[0], jnp.where(r < block_rows + 3, more[1], 0)))
    col_ok = jnp.where(c < block_cols, 1, jnp.where(c >= width - 3, ok[2], jnp.where(c < block_cols + 3, ok[3], 0)))
    inside = (row_ok * col_ok).astype(jnp.float32)
    level = surf_ref[1]
    convey = jnp.sqrt(surf_ref[2]) * inside
    leak = surf_ref[3]
    rain = surf_ref[4]
    top = tops_ref[0]

    def across(x):
        return pltpu.roll(x, rows - 1, 0)

    def along(x):
        return pltpu.roll(x, width - 1, 1)

    gates = [convey * across(convey), convey * along(convey)]
    parts = []
    for ch in chunks(width):
        _, _, root = closure(params(tab_ref, tops_ref[1, :, ch].astype(jnp.int32)), top[:, ch])
        parts.append(0.25 * root * root)
    leak = leak * jnp.concatenate(parts, axis=1)
    water = surf_ref[0]
    exchange = jnp.zeros_like(water)
    for _ in range(PASSES):
        surface = level + water
        power = jnp.where(water > 0.0, jnp.exp2((5.0 / 3.0) * jnp.log2(jnp.maximum(water, 1e-30))), 0.0)
        outflow = jnp.zeros_like(water)
        for axis, gate, beside in ((0, gates[0], across), (1, gates[1], along)):
            slope = surface - beside(surface)
            carried = jnp.where(slope >= 0.0, power, beside(power))
            flux = gate * carried * slope * lax.rsqrt(jnp.maximum(jnp.abs(slope), SLOPE_FLOOR))
            outflow = outflow + flux - pltpu.roll(flux, 1, axis)
        rate = leak * (water - top)
        exchange = exchange + SURFACE_STEP * rate
        water = jnp.maximum(water + SURFACE_STEP * (rain - rate - outflow), 0.0)
    ex_ref[...] = exchange
    w_ref[...] = water
    if water_ref.shape[1] % LANES:
        water_ref[...] = w_ref[:block_rows, :block_cols]
    else:
        mine = pl.multiple_of(line * water_ref.shape[1], LANES)
        water_ref[...] = w_ref[:block_rows, pl.ds(mine, water_ref.shape[1])]
    first = pl.multiple_of(line * own, SUBS)
    after = pl.multiple_of(line * own + own, SUBS)
    before = pl.multiple_of(jnp.where(line > 0, line * own - SUBS, block_rows), SUBS)
    sub = lax.broadcasted_iota(jnp.int32, (SUBS, width), 0)
    rim = jnp.where(sub == SUBS - 1, ex_ref[pl.ds(before, SUBS), :], jnp.where(sub == 0, ex_ref[pl.ds(after, SUBS), :], 0.0))
    gain = jnp.concatenate([ex_ref[pl.ds(first, own), :], rim], axis=0)
    mask = soil_mask(ok, own + SUBS, width, own, block_cols)
    p = top_ref[0] + gain * top_ref[1]
    content, capacity, root = wide([closure(params(tab_ref, class_ref[:, ch]), p[:, ch]) for ch in chunks(width)])
    h = root * mask
    q = h * p
    low, low_q, low_n, low_d, weights, flows = (next_ref[i] for i in range(6))

    def tile(x):
        return x[:own, :block_cols]

    top_n = tile(capacity * p - (content - top_ref[2]) + gain + h * lateral(q)) + tile(h) * (low_q - GRAVITY_STEP * low)
    new_ref[0] = top_n / (tile(capacity + h * lateral(h)) + tile(h) * low)
    low_n = low_n + low * (flows + tile(q) + GRAVITY_STEP * tile(h))
    new_ref[1] = low_n / (low_d + low * (weights + tile(h)))
    copy = pltpu.make_async_copy(new_ref, head_out.at[:TOP_LAYERS], sem)
    copy.start()
    copy.wait()


def finish(tables, fields, tops, head, block, count):
    own = head.shape[1]
    whole = count == 0
    rows, width = block[0] + SUBS, block[1] + LANES
    n = len(fields)

    def body(tab_ref, *refs):
        given, known, (head_out, water_ref), (box, turn), rest = refs[:n], refs[n : n + 3], refs[n + 4 : n + 6], refs[n + 6 : n + 8], refs[n + 8 :]
        if whole:
            surf, tops = given
        else:
            surf, tops = box
            cut = given[0].shape[0] - 2 * (EDGE_ROWS + 4 * block[1] // LANES) - turn.shape[1] // LANES * SUBS
            assemble([x.at[:cut] for x in given], [x.at[cut:] for x in given], surf, tops, turn, own, block[0], count)
        last_kernel(tab_ref, surf, tops, *known, head_out, water_ref, *rest, own=own)

    def scratch_body(*refs):
        cut = 1 + n + 6
        body(*refs[:cut], refs[cut : cut + 2], refs[cut + 2], *refs[cut + 3 :])

    tall = LANES + 5 * (block[0] + SUBS)
    tall += -tall % LANES
    small = (1, SUBS, LANES)
    vmem = pl.BlockSpec(memory_space=pltpu.VMEM)
    water = block if whole else (block[0], LANES)
    return pl.pallas_call(
        scratch_body,
        out_shape=(
            jax.ShapeDtypeStruct(head.shape, jnp.float32),
            jax.ShapeDtypeStruct(water, jnp.float32),
        ),
        in_specs=[vmem] * (n + 4) + [pl.BlockSpec(memory_space=pl.ANY)],
        out_specs=[pl.BlockSpec(memory_space=pl.ANY), vmem],
        scratch_shapes=[
            pltpu.VMEM(small if whole else (5, rows, width), jnp.float32),
            pltpu.VMEM(small if whole else (2, rows, width), jnp.float32),
            pltpu.VMEM((SUBS, LANES) if whole else (LANES, tall), jnp.float32),
            pltpu.VMEM((rows, width), jnp.float32),
            pltpu.VMEM((rows, width), jnp.float32),
            pltpu.VMEM((TOP_LAYERS, own, block[1]), jnp.float32),
            pltpu.SemaphoreType.DMA,
        ],
        input_output_aliases={n + 4: 0},
        name="surface_and_top",
    )(tables, *fields, *tops, head)


def lane_rows(size):
    return -(-size // LANES)


def as_lanes(x):
    if x.shape[-1] % LANES:
        x = jnp.pad(x.reshape(-1), (0, -x.size % LANES))
    return x.reshape(-1, LANES)


def from_lanes(x, shape):
    if shape[-1] % LANES:
        size = 1
        for length in shape:
            size *= length
        x = x.reshape(-1)[:size]
    return x.reshape(shape)


def gx_trade(edges, half):
    got = shift(edges, "gx", 1)
    if lax.axis_size("gx") == 2:
        return got
    return jnp.where(half, got, shift(edges, "gx", -1))


def cyclic_rows(mid, above, below, gap):
    hole = jnp.zeros(mid.shape[:-2] + (gap, mid.shape[-1]), mid.dtype)
    return jnp.concatenate([mid, below, hole, above], axis=-2)


def block_general(pressure, soil_class, depth, elevation, roughness, rain, land_mask, channel_mask):
    ny = lax.axis_size("gy")
    _, own, cols = pressure.shape
    srows, scols = depth.shape
    convey = (1.0 + channel_mask.astype(jnp.float32)) / roughness
    surf = jnp.stack([depth, elevation, convey, LEAKANCE * land_mask.astype(jnp.float32), rain])
    tops = jnp.stack([pressure[0], soil_class[0].astype(jnp.float32)])

    def pack(s, t):
        return jnp.concatenate([as_lanes(s), as_lanes(t)], axis=0)

    def unpack(m):
        cut = lane_rows(15 * scols)
        return from_lanes(m[:cut], (5, 3, scols)), from_lanes(m[cut:], (2, 2, cols))

    s_above, t_above = unpack(shift(pack(surf[:, -3:], tops[:, -2:]), "grp", 1))
    s_below, t_below = unpack(shift(pack(surf[:, :3], tops[:, :2]), "grp", -1))
    surf_rows = cyclic_rows(surf, s_above, s_below, 2)
    tops_rows = jnp.concatenate([tops, t_below, t_above], axis=1)

    def edges(cut):
        a = surf_rows[:, :, cut(3)].transpose(0, 2, 1).reshape(15, -1)
        b = tops_rows[:, :, cut(2)].transpose(0, 2, 1).reshape(4, -1)
        return jnp.concatenate([a, jnp.pad(b, ((0, 0), (0, a.shape[1] - b.shape[1])))], axis=0)

    out = jnp.concatenate([edges(lambda n: slice(-n, None)), edges(lambda n: slice(0, n))])
    got = gx_trade(out, lax.broadcasted_iota(jnp.int32, out.shape, 0) < 19)
    mine = jnp.concatenate(
        [as_lanes(surf_rows), as_lanes(tops_rows), jnp.pad(got, ((0, 0), (0, -got.shape[1] % LANES))).reshape(-1, LANES)]
    )
    every = lax.all_gather(mine, "gy", axis=0, tiled=False)
    n1 = lane_rows(surf_rows.size)
    n2 = n1 + lane_rows(tops_rows.size)
    e_surf = jax.vmap(lambda m: from_lanes(m, (5, srows + SUBS, scols)))(every[:, :n1])
    e_surf = e_surf.transpose(1, 2, 0, 3).reshape(5, srows + SUBS, ny * scols)
    e_tops = every[:, n1:n2].reshape(ny, 2, own + 4, cols)
    e_m = every[:, n2:].reshape(ny, 2, 19, -1)
    main = e_tops[:, :, :own].transpose(1, 0, 2, 3).reshape(2, srows, cols)
    zeros = jnp.zeros((2, 4, cols), jnp.float32)
    f_tops = jnp.concatenate([main, e_tops[0, :, own : own + 2], zeros, e_tops[-1, :, own + 2 :]], axis=1)
    height = srows + SUBS
    c_left = e_m[-1, 0, :15, :height].reshape(5, 3, height).transpose(0, 2, 1)
    c_right = e_m[0, 1, :15, :height].reshape(5, 3, height).transpose(0, 2, 1)
    hole = jnp.zeros((5, height, LANES - 6), jnp.float32)
    blocks = jnp.concatenate([e_surf, c_right, hole, c_left], axis=2)

    def tops_edge(side):
        t = e_m[:, side, 15:, : own + 4].reshape(ny, 2, 2, own + 4)
        mid = t[..., :own].transpose(1, 0, 3, 2).reshape(2, srows, 2)
        low = t[0, :, :, own : own + 2].transpose(0, 2, 1)
        high = t[-1, :, :, own + 2 :].transpose(0, 2, 1)
        return jnp.concatenate([mid, low, jnp.zeros((2, 4, 2), jnp.float32), high], axis=1)

    return blocks, jnp.concatenate(
        [f_tops, tops_edge(1), jnp.zeros((2, height, LANES - 4), jnp.float32), tops_edge(0)], axis=2
    )


def local(
    pressure, soil_class, capacity_range, inverse_entry, shape_index, conductivity,
    depth, elevation, roughness, rain, land_mask, channel_mask,
):
    ny, iy = lax.axis_size("gy"), lax.axis_index("gy")
    _, own, cols = pressure.shape
    srows, scols = depth.shape
    ground = (depth, elevation, roughness, rain, land_mask, channel_mask)
    classes = (capacity_range, inverse_entry, shape_index, conductivity)
    even = scols == LANES and own == SUBS
    tables, *packed = pack(pressure, soil_class, classes, ground if even else ())
    after, before, after_end, before_end = packed[-4:]
    surface = ()
    if even:
        main, strip_after, strip_before = packed[:3]
        above = shift(strip_after, "grp", 1)
        below = shift(strip_before, "grp", -1)
        surface = (main, above, below)
    rows = ("grp", "gy")
    sent = columns(pressure, soil_class, shift(after_end, rows, 1), shift(before_end, rows, -1), surface)
    up = shift(after, rows, 1)
    down = shift(before, rows, -1)
    span = pressure.shape[0] * (own + SUBS)
    half = jnp.where(lax.broadcasted_iota(jnp.int32, sent.shape, 1) < span, 4, 3)
    got = gx_trade(sent, lax.broadcasted_iota(jnp.int32, sent.shape, 0) < half)
    if even:
        strip = jnp.concatenate([above, below] + [got[:, ch] for ch in chunks(sent.shape[1])[span // LANES :]], axis=0)
        strip = jnp.concatenate([main, strip], axis=0)
        fields = [strip] + [shift(strip, "gy", step) for step in range(1, ny)]
    else:
        fields = block_general(pressure, soil_class, *ground)
    head, *tops = soil_interior(tables, pressure, soil_class, up, down, got, sent)
    head, water = finish(tables, fields, tops, head, (srows, cols), ny if even else 0)
    if not even:
        water = lax.dynamic_slice_in_dim(water, iy * scols, scols, axis=1)
    return head, water


def solution(mesh):
    soil = P(None, ("grp", "gy"), "gx")
    ground = P("grp", ("gx", "gy"))
    return jax.shard_map(
        local,
        mesh=mesh,
        in_specs=(soil, soil, P(), P(), P(), P()) + (ground,) * 6,
        out_specs=(soil, ground),
        check_vma=False,
    )
```

```python
import jax
import jax.numpy as jnp
from jax import lax
from jax.experimental import pallas as pl
from jax.experimental.pallas import tpu as pltpu
from jax.sharding import PartitionSpec as P


PASSES = 3
STORAGE = 0.01
GRAVITY_STEP = 0.5
SUCTION_FLOOR = 0.01
SLOPE_FLOOR = 0.1
SURFACE_STEP = 0.3
LEAKANCE = 0.5

LANES = 128
SUBS = 8
UNROLL = 8
TOP_LAYERS = 2


def shift(x, axis, step):
    size = lax.axis_size(axis)
    return lax.ppermute(x, axis, [(i, (i + step) % size) for i in range(size)])


def near(*arrays):
    return [pltpu.with_memory_space_constraint(x, pltpu.VMEM) for x in arrays]


def class_tables(refs):
    lane = lax.broadcasted_iota(jnp.int32, (1, LANES), 1)
    spread = []
    for ref in refs:
        row = jnp.ones((1, LANES), jnp.float32)
        for k in range(ref.shape[0]):
            row = jnp.where(lane == k, ref[k], row)
        spread.append(row)
    span, entry, shape, ks = spread
    pore = 1.0 - 1.0 / shape
    rows = [-entry, 1.0 / (1.0 - pore), pore, span, 2.0 * jnp.sqrt(ks)]
    return jnp.concatenate(rows + [jnp.zeros((SUBS - len(rows), LANES), jnp.float32)], axis=0)


def place():
    tile = lax.axis_index("grp") * lax.axis_size("gy") + lax.axis_index("gy")
    tiles = lax.axis_size("grp") * lax.axis_size("gy")
    column, columns = lax.axis_index("gx"), lax.axis_size("gx")
    tests = (tile > 0, tile < tiles - 1, column > 0, column < columns - 1)
    return [jnp.where(t, 1, 0) for t in tests]


def params(tab_ref, idx):
    return [
        jnp.take_along_axis(jnp.broadcast_to(tab_ref[i : i + 1, :], idx.shape), idx, axis=1, mode="promise_in_bounds")
        for i in range(5)
    ]


def closure(given, p):
    entry, expo, pore, span, scale = given
    logs = jnp.log2(jnp.maximum(entry * p, SUCTION_FLOOR))
    total = jnp.log2(1.0 + jnp.exp2(expo * logs))
    drop = pore * total
    less = expo - 1.0
    power = less * logs - drop
    ratio = jnp.exp2(power)
    content = span * jnp.exp2(-drop)
    capacity = STORAGE - (span * entry * less) * jnp.exp2(power - total)
    root = scale * jnp.exp2(-0.25 * drop) * jnp.abs(1.0 - ratio)
    return content, capacity, root


def chunks(width):
    return [slice(i, i + LANES) for i in range(0, width, LANES)]


def wide(parts):
    return [jnp.concatenate(x, axis=1) for x in zip(*parts)]


def lateral(x):
    rows, width = x.shape
    return (
        pltpu.roll(x, 1, 0)
        + pltpu.roll(x, rows - 1, 0)
        + pltpu.roll(x, 1, 1)
        + pltpu.roll(x, width - 1, 1)
    )


def soil_mask(ok, rows, width, own_rows, own_cols):
    r = lax.broadcasted_iota(jnp.int32, (rows, width), 0)
    c = lax.broadcasted_iota(jnp.int32, (rows, width), 1)
    above = jnp.where(r >= rows - 2, ok[0], 0)
    below = jnp.where((r >= own_rows) & (r < own_rows + 2), ok[1], 0)
    left = jnp.where(c >= width - 2, ok[2], 0)
    right = jnp.where((c >= own_cols) & (c < own_cols + 2), ok[3], 0)
    in_rows = jnp.where(r < own_rows, 1, above + below)
    in_cols = jnp.where(c < own_cols, 1, left + right)
    return (in_rows * in_cols).astype(jnp.float32)


def soil_rows(p_ref, c_ref, next_ref, prev_ref, next_end, prev_end):
    layers, own, cols = p_ref.shape
    start = lax.broadcasted_iota(jnp.int32, (layers, LANES), 1) < LANES // 2
    for f, x in enumerate((p_ref, c_ref)):
        for r in range(2):
            next_ref[f, r] = x[:, own - 2 + r, :].astype(jnp.float32)
            prev_ref[f, r] = x[:, r, :].astype(jnp.float32)
        next_end[f] = jnp.where(start, next_ref[f, 1, :, :LANES], next_ref[f, 1, :, cols - LANES :])
        prev_end[f] = jnp.where(start, prev_ref[f, 0, :, :LANES], prev_ref[f, 0, :, cols - LANES :])


def soil_columns(p_first, c_first, p_last, c_last, up_end, down_end, box):
    layers, own, _ = p_first.shape
    rows = box.shape[1]
    out = []
    for side in ((p_last, c_last), (p_first, c_first)):
        for f in range(2):
            box[:, 2 : 2 + own, :] = side[f][...].astype(jnp.float32)
            box[:, 0, :] = jnp.zeros((layers, LANES), jnp.float32)
            box[:, 1, :] = up_end[f]
            box[:, own + 2, :] = down_end[f]
            box[:, own + 3 :, :] = jnp.zeros((layers, rows - own - 3, LANES), jnp.float32)
            turned = box[...].reshape(layers * rows, LANES).T
            out.append(turned[LANES - 2 :] if len(out) < 2 else turned[:2])
    return jnp.concatenate(out, axis=0)


def soil_kernel(
    tab_ref, p_far, c_far, up_in, down_in, got_in, sent_in, out_far, top_out, class_out, next_out,
    p_in, c_in, out_ref, tile_sem, out_sem, h_ref, q_ref, n_ref, d_ref, k_ref, h2_ref, q2_ref, n2_ref, d2_ref, given, corner, turn, near, near2, pe, ce,
):
    layers, own, cols = p_in.shape
    rows = own + SUBS
    span = layers * rows
    f32 = jnp.float32
    ok = place()

    def tile_copy(i, j):
        part = pl.ds(j * UNROLL, UNROLL)
        far, here = ((p_far, p_in), (c_far, c_in))[i]
        return pltpu.make_async_copy(far.at[part], here.at[part], tile_sem.at[i, j])

    def out_copy(j):
        part = pl.ds(j * UNROLL, UNROLL)
        return pltpu.make_async_copy(out_ref.at[part], out_far.at[part], out_sem.at[j])

    got, sent = got_in[:, :span], sent_in[:, :span]
    groups = layers // UNROLL
    for j in range(groups):
        tile_copy(0, j).start()
        tile_copy(1, j).start()
    for ref in (h_ref, q_ref, h2_ref, q2_ref):
        ref[0] = jnp.zeros((own, cols), f32)
        ref[layers + 1] = jnp.zeros((own, cols), f32)

    def first(z):
        for ch in chunks(cols):
            p = p_in[z, :, ch]
            values = params(tab_ref, c_in[z, :, ch])
            for i, v in enumerate(values):
                given[i, z, :, ch] = v
            content, capacity, root = closure(values, p)
            h_ref[z + 1, :, ch] = root
            q_ref[z + 1, :, ch] = root * p
            n_ref[z, :, ch] = capacity * p
            d_ref[z, :, ch] = capacity
            k_ref[z, :, ch] = content

    def first_group(j, carry):
        tile_copy(0, j).wait()
        tile_copy(1, j).wait()
        for i in range(UNROLL):
            first(j * UNROLL + i)
        return carry

    lax.fori_loop(0, groups, first_group, 0)

    gap = jnp.zeros((1, span), f32)
    p = jnp.concatenate([got[0:2], sent[4:5], gap, sent[1:2], got[4:6], gap], axis=0)
    kind = jnp.concatenate([got[2:4], sent[6:7], gap, sent[3:4], got[6:8], gap], axis=0).astype(jnp.int32)
    sub = lax.broadcasted_iota(jnp.int32, (SUBS, span), 0)
    lane = lax.broadcasted_iota(jnp.int32, (SUBS, span), 1)
    row = lane % rows
    row_ok = jnp.where(row < 2, ok[0], jnp.where(row < own + 2, 1, jnp.where(row < own + 4, ok[1], 0)))
    col_ok = jnp.where(sub < 2, ok[2], jnp.where((sub == 2) | (sub == 4), 1, jnp.where((sub == 5) | (sub == 6), ok[3], 0)))
    mask = (row_ok * col_ok).astype(f32)
    values = [params(tab_ref, kind[:, ch]) for ch in chunks(span)]
    content, capacity, root = wide([closure(v, p[:, ch]) for v, ch in zip(values, chunks(span))])
    h, q = root * mask, root * mask * p

    def over(x):
        return jnp.where(lane < rows, 0.0, pltpu.roll(x, rows, 1))

    def under(x):
        return jnp.where(lane >= span - rows, 0.0, pltpu.roll(x, span - rows, 1))

    weights = lateral(h) + over(h) + under(h)
    flows = lateral(q) + over(q) + under(q) + GRAVITY_STEP * (over(h) - under(h))
    p1 = (capacity * p + h * flows) / (capacity + h * weights)
    root = wide([closure(v, p1[:, ch]) for v, ch in zip(values, chunks(span))])[2] * mask
    turn[...] = jnp.zeros_like(turn)
    for i, x in enumerate((h, q, root, root * p1)):
        turn[i * SUBS : (i + 1) * SUBS, :] = x
    corner[...] = turn[...].T.reshape(layers, rows, LANES)

    zsub = lax.broadcasted_iota(jnp.int32, (layers, cols), 0)
    zlane = lax.broadcasted_iota(jnp.int32, (layers, LANES), 1)

    def sides(x, edge, at, lanes):
        left, right = pltpu.roll(x, 1, 1), pltpu.roll(x, cols - 1, 1)
        a = jnp.where(lanes == 0, pltpu.roll(edge, LANES - at, 1), left[:, :LANES])
        b = jnp.where(lanes == LANES - 1, pltpu.roll(edge, LANES - 1 - (at + 4), 1), right[:, cols - LANES :])
        return jnp.concatenate([a, left[:, LANES:]], axis=1) + jnp.concatenate([right[:, : cols - LANES], b], axis=1)

    for side, (halo, close, far, edge_row, valid) in enumerate(((up_in, 1, 0, 1, ok[0]), (down_in, 0, 1, own + 2, ok[1]))):
        inside = valid.astype(f32)
        ours = 0 if side == 0 else own - 1
        values, states, beyond = [], [], []
        for ch in chunks(cols):
            p = halo[0, close, :, ch]
            v = params(tab_ref, halo[1, close, :, ch].astype(jnp.int32))
            content, capacity, root = closure(v, p)
            root = root * inside
            values.append(v)
            states.append((p, capacity, root, root * p))
            p = halo[0, far, :, ch]
            root = closure(params(tab_ref, halo[1, far, :, ch].astype(jnp.int32)), p)[2] * inside
            beyond.append((root, root * p))
        p, capacity, h, q = wide(states)
        far_h, far_q = wide(beyond)
        near[side, 0] = h
        near[side, 1] = q
        edge = corner[:, edge_row, :]
        top_h = jnp.where(zsub == 0, 0.0, pltpu.roll(h, 1, 0))
        low_h = jnp.where(zsub == layers - 1, 0.0, pltpu.roll(h, layers - 1, 0))
        top_q = jnp.where(zsub == 0, 0.0, pltpu.roll(q, 1, 0))
        low_q = jnp.where(zsub == layers - 1, 0.0, pltpu.roll(q, layers - 1, 0))
        weights = far_h + h_ref[1 : layers + 1, ours, :] + sides(h, edge, 1, zlane) + top_h + low_h
        flows = far_q + q_ref[1 : layers + 1, ours, :] + sides(q, edge, 1 + SUBS, zlane) + top_q + low_q + GRAVITY_STEP * (top_h - low_h)
        p1 = (capacity * p + h * flows) / (capacity + h * weights)
        for v, ch in zip(values, chunks(cols)):
            root = closure(v, p1[:, ch])[2] * inside
            near2[side, 0, :, ch] = root
            near2[side, 1, :, ch] = root * p1[:, ch]

    tsub = lax.broadcasted_iota(jnp.int32, (own, cols), 0)
    tlane = lax.broadcasted_iota(jnp.int32, (own, LANES), 1)

    def around(z, h, q, rim, at):
        edge = corner[z, 2 : 2 + own, :]
        out = []
        for i, x in enumerate((h[z + 1], q[z + 1])):
            above = jnp.where(tsub == 0, rim[0, i, pl.ds(z, 1), :], pltpu.roll(x, 1, 0))
            below = jnp.where(tsub == own - 1, rim[1, i, pl.ds(z, 1), :], pltpu.roll(x, own - 1, 0))
            out.append(above + below + sides(x, edge, at + i * SUBS, tlane))
        weights, flows = out
        low = h[z + 2]
        return weights + low, flows + q[z + 2] - GRAVITY_STEP * low

    def second(z, carry):
        mid, top = h_ref[z + 1], h_ref[z]
        weights, flows = around(z, h_ref, q_ref, near, 1)
        flows = flows + q_ref[z] + GRAVITY_STEP * top
        p1 = (n_ref[z] + mid * flows) / (d_ref[z] + mid * (weights + top))
        for ch in chunks(cols):
            p = p1[:, ch]
            content, capacity, root = closure([given[i, z, :, ch] for i in range(5)], p)
            h2_ref[z + 1, :, ch] = root
            q2_ref[z + 1, :, ch] = root * p
            n2_ref[z, :, ch] = capacity * p - (content - k_ref[z, :, ch])
            d2_ref[z, :, ch] = capacity
        return carry

    lax.fori_loop(0, layers, second, 0, unroll=UNROLL)

    def third(z):
        mid, top = h2_ref[z + 1], h2_ref[z]
        weights, flows = around(z, h2_ref, q2_ref, near2, 1 + 2 * SUBS)
        flows = flows + q2_ref[z] + GRAVITY_STEP * top
        out_ref[z] = (n2_ref[z] + mid * flows) / (d2_ref[z] + mid * (weights + top))

    def third_group(j, carry):
        for i in range(UNROLL):
            third(j * UNROLL + i)
        out_copy(j).start()
        return carry

    lax.fori_loop(0, groups, third_group, 0)

    weights, flows = around(1, h2_ref, q2_ref, near2, 1 + 2 * SUBS)
    for i, x in enumerate((h2_ref[2], q2_ref[2], n2_ref[1], d2_ref[1], weights, flows)):
        next_out[i] = x
    for f, (src, dst, halo_at) in enumerate(((p_in, pe, 0), (c_in, ce, 2))):
        turn[...] = jnp.zeros_like(turn)
        turn[LANES - 2 :, :] = got[halo_at : halo_at + 2]
        turn[:2, :] = got[halo_at + 4 : halo_at + 6]
        block = turn[:, :LANES].T
        for z in range(2):
            dst[z, own:, :cols] = jnp.zeros((SUBS, cols), dst.dtype)
            dst[z, :own, :cols] = src[z]
            dst[z, :, cols:] = jnp.zeros((rows, LANES), dst.dtype)
            dst[z, : own + 2, cols:] = block[z * rows + 2 : z * rows + own + 4].astype(dst.dtype)
            dst[z, rows - 2 :, cols:] = block[z * rows : z * rows + 2].astype(dst.dtype)
            for r in range(2):
                dst[z, own + r : own + r + 1, :cols] = down_in[f, r, z : z + 1, :].astype(dst.dtype)
                dst[z, rows - 2 + r : rows - 1 + r, :cols] = up_in[f, r, z : z + 1, :].astype(dst.dtype)
    width = cols + LANES
    mask = soil_mask(ok, rows, width, own, cols)
    states = []
    for z in range(2):
        content, capacity, root = wide([closure(params(tab_ref, ce[z, :, ch]), pe[z, :, ch]) for ch in chunks(width)])
        states.append((content, capacity, root * mask))
    content, capacity, h = states[0]
    low = states[1][2]
    weights = lateral(h) + low
    flows = lateral(h * pe[0]) + low * pe[1] - GRAVITY_STEP * low
    weight = capacity + h * weights
    top_out[0] = (capacity * pe[0] + h * flows) / weight
    top_out[1] = 1.0 / weight
    top_out[2] = content
    top_out[3] = pe[0]
    top_out[4] = h
    for j in range(groups):
        out_copy(j).wait()
    class_out[...] = ce[0]


def soil_interior(tables, pressure, soil_class, up, down, got, sent):
    layers, own, cols = pressure.shape
    rows, width = own + SUBS, cols + LANES
    f32 = jnp.float32
    span = layers * rows
    tall = pltpu.VMEM((layers + 2, own, cols), f32)
    flat = pltpu.VMEM((layers, own, cols), f32)
    vmem = pl.BlockSpec(memory_space=pltpu.VMEM)
    far = pl.BlockSpec(memory_space=pl.ANY)
    return pl.pallas_call(
        soil_kernel,
        out_shape=(
            jax.ShapeDtypeStruct(pressure.shape, f32),
            pltpu.VMEM((5, rows, width), f32),
            pltpu.VMEM((rows, width), jnp.int32),
            pltpu.VMEM((6, own, cols), f32),
        ),
        in_specs=[vmem] + [far] * 2 + [vmem] * 4,
        out_specs=[far] + [vmem] * 3,
        scratch_shapes=[flat, pltpu.VMEM((layers, own, cols), jnp.int32), flat]
        + [pltpu.SemaphoreType.DMA((2, layers // UNROLL)), pltpu.SemaphoreType.DMA((layers // UNROLL,))]
        + [tall, tall, flat, flat, flat, tall, tall, flat, flat]
        + [
            pltpu.VMEM((5, layers, own, cols), f32),
            pltpu.VMEM((layers, rows, LANES), f32),
            pltpu.VMEM((LANES, span), f32),
            pltpu.VMEM((2, 2, layers, cols), f32),
            pltpu.VMEM((2, 2, layers, cols), f32),
            pltpu.VMEM((2, rows, width), f32),
            pltpu.VMEM((2, rows, width), jnp.int32),
        ],
        name="soil_interior",
    )(*near(tables), pressure, soil_class, *near(up, down, got, sent))


def surface_rows(p_ref, c_ref, depth, level, rough, rain, land, channel, main_ref, next_ref, prev_ref):
    height, _ = depth.shape
    _, own, cols = p_ref.shape
    fields = (
        depth[...],
        level[...],
        (1.0 + channel[...].astype(jnp.float32)) / rough[...],
        LEAKANCE * land[...].astype(jnp.float32),
        rain[...],
    )
    for f, x in enumerate(fields):
        main_ref[f * height : (f + 1) * height, :] = x
        next_ref[3 * f : 3 * f + 3, :] = x[height - 3 :]
        prev_ref[3 * f : 3 * f + 3, :] = x[:3]
    base = 5 * height
    for f, x in enumerate((p_ref[0], c_ref[0].astype(jnp.float32))):
        for j, ch in enumerate(chunks(cols)):
            main_ref[base : base + own, :] = x[:, ch]
            base += own
            at = EDGE_ROWS + 2 * (f * (cols // LANES) + j)
            next_ref[at : at + 2, :] = x[own - 2 :, ch]
            prev_ref[at : at + 2, :] = x[:2, ch]


EDGE_ROWS = 16


def pack(pressure, soil_class, classes, ground):
    layers, own, cols = pressure.shape
    f32 = jnp.float32
    edge = pltpu.VMEM((2, 2, layers, cols), f32)
    end = pltpu.VMEM((2, layers, LANES), f32)
    out = [edge, edge, end, end]
    if ground:
        height = ground[0].shape[0]
        strip = pltpu.VMEM((EDGE_ROWS + 4 * cols // LANES, LANES), f32)
        out = [pltpu.VMEM((5 * height + 2 * own * cols // LANES, LANES), f32), strip, strip] + out

    def body(*refs):
        tables, rest = refs[: len(classes)], refs[len(classes) :]
        if ground:
            surface_rows(*rest[: 2 + len(ground)], *rest[3 + len(ground) : 6 + len(ground)])
        soil_rows(*rest[:2], *rest[-4:])
        rest[2 + len(ground)][...] = class_tables(tables)

    vmem = pl.BlockSpec(memory_space=pltpu.VMEM)
    smem = pl.BlockSpec(memory_space=pltpu.SMEM)
    return pl.pallas_call(
        body,
        out_shape=[pltpu.VMEM((SUBS, LANES), f32)] + out,
        in_specs=[smem] * len(classes) + [vmem] * (2 + len(ground)),
        name="pack",
    )(*classes, pressure, soil_class, *ground)


def surface_columns(main_ref, above_ref, below_ref, box, height, own, cols):
    n = cols // LANES
    tall = height + SUBS
    box[...] = jnp.zeros_like(box)
    for side, j in enumerate((n - 1, 0)):
        for f in range(2):
            at = (2 * side + f) * 2 * SUBS
            src = 5 * height + (f * n + j) * own
            strip = EDGE_ROWS + 2 * (f * n + j)
            box[at : at + own, :] = main_ref[src : src + own, :]
            box[at + own : at + own + 2, :] = below_ref[strip : strip + 2, :]
            box[at + own + 2 : at + own + 4, :] = above_ref[strip : strip + 2, :]
    for f in range(5):
        at = LANES + f * tall
        box[at : at + height, :] = main_ref[f * height : (f + 1) * height, :]
        box[at + height : at + height + 3, :] = below_ref[3 * f : 3 * f + 3, :]
        box[at + tall - 3 : at + tall, :] = above_ref[3 * f : 3 * f + 3, :]
    turned = box[...].T
    edges = jnp.concatenate([turned[LANES - 3 :], turned[:3], jnp.zeros((2, turned.shape[1]), jnp.float32)], axis=0)
    return edges


def columns(pressure, soil_class, up_end, down_end, surface):
    layers, own, cols = pressure.shape
    rows = own + SUBS
    span = layers * rows
    scratch = [pltpu.VMEM((layers, rows, LANES), jnp.float32)]
    width = span
    if surface:
        height = (surface[0].shape[0] - 2 * own * cols // LANES) // 5
        tall = LANES + 5 * (height + SUBS)
        tall += -tall % LANES
        width += tall
        scratch.append(pltpu.VMEM((tall, LANES), jnp.float32))

    n = 4 + len(surface)
    kinds = (pressure.dtype, soil_class.dtype)

    def body(*refs):
        out_ref, box, ends, sems = refs[n], refs[n + 1], refs[-5:-1], refs[-1]
        copies = [
            pltpu.make_async_copy(refs[i % 2].at[:, :, pl.ds(i // 2 * (cols - LANES), LANES)], ends[i], sems.at[i]) for i in range(4)
        ]
        for copy in copies:
            copy.start()
        if surface:
            out_ref[:, span:] = surface_columns(*refs[4:n], refs[n + 2], height, own, cols)
        for copy in copies:
            copy.wait()
        out_ref[:, :span] = soil_columns(*ends, *refs[2:4], box)

    return pl.pallas_call(
        body,
        out_shape=pltpu.VMEM((SUBS, width), jnp.float32),
        in_specs=[pl.BlockSpec(memory_space=pl.ANY)] * 2 + [pl.BlockSpec(memory_space=pltpu.VMEM)] * (2 + len(surface)),
        scratch_shapes=scratch + [pltpu.VMEM((layers, own, LANES), k) for k in kinds * 2] + [pltpu.SemaphoreType.DMA((4,))],
        name="columns",
    )(pressure, soil_class, *near(up_end, down_end, *surface))


def rim(at_end, at_start, lane, count):
    return jnp.where(lane >= LANES - count, at_end, jnp.where(lane < count, at_start, 0.0))


def ring(before, after, sub):
    return jnp.where(sub >= SUBS - 3, before, jnp.where(sub < 3, after, 0.0))


WINDOW = 136


def windows_kernel(main, above, below, got, sent, *refs, span, height, own, count):
    outs, (tall, wide_top, ends, turn) = refs[:count], refs[count:]
    line = lax.axis_index("gy")
    lane = lax.broadcasted_iota(jnp.int32, (SUBS, LANES), 1)
    sub = lax.broadcasted_iota(jnp.int32, (SUBS, LANES), 0)
    tall[...] = jnp.zeros_like(tall)
    ends[...] = jnp.zeros_like(ends)
    turn[...] = jnp.zeros_like(turn)
    for f in range(5):
        tall[f, SUBS : SUBS + height] = main[f * height : (f + 1) * height, :]
        tall[f, SUBS - 3 : SUBS] = above[3 * f : 3 * f + 3, :]
        tall[f, SUBS + height : SUBS + height + 3] = below[3 * f : 3 * f + 3, :]
    turn[LANES - 3 :, :] = got[:3, span : span + LANES]
    turn[:3, :] = got[3:6, span : span + LANES]
    block = turn[...].T
    last = line == count - 1
    for f in range(2):
        before, after = block[2 * f * SUBS :], block[2 * (2 + f) * SUBS :]
        beside = rim(before[:SUBS], after[:SUBS], lane, 2)
        beyond = rim(before[SUBS : 2 * SUBS], after[SUBS : 2 * SUBS], lane, 2)
        beyond = jnp.where(last, beyond[2:4], beyond[:2])
        for j in (0, count + 1):
            wide_top[f, j] = beside
            ends[j, 2 * f : 2 * f + 2] = beyond
        for j in range(count):
            src = 5 * height + (f * count + j) * own
            wide_top[f, j + 1] = main[src : src + own, :]
            at = EDGE_ROWS + 2 * (f * count + j)
            ends[j + 1, 2 * f : 2 * f + 2] = jnp.where(last, above[at : at + 2, :], below[at : at + 2, :])
    for s in range(count):
        who, out = (line + s) % count, outs[s]
        for f in range(5):
            first = pl.multiple_of(who * SUBS, SUBS)
            out[2 * f * SUBS : (2 * f + 1) * SUBS, :] = tall[f, pl.ds(first + SUBS, SUBS), :]
            out[(2 * f + 1) * SUBS : (2 * f + 2) * SUBS, :] = ring(
                tall[f, pl.ds(first, SUBS), :], tall[f, pl.ds(first + 2 * SUBS, SUBS), :], sub
            )
        for f in range(2):
            out[(10 + f) * SUBS : (11 + f) * SUBS, :] = wide_top[f, who + 1]
            out[(12 + f) * SUBS : (13 + f) * SUBS, :] = rim(wide_top[f, who], wide_top[f, who + 2], lane, 2)
        mid, side = ends[who + 1], rim(ends[who], ends[who + 2], lane, 2)
        out[14 * SUBS : 14 * SUBS + 4, :] = mid[:4]
        out[14 * SUBS + 4 : 15 * SUBS, :] = side[:4]
        for j in range(2):
            cut = slice(span + (j + 1) * LANES, span + (j + 2) * LANES)
            at = (15 + j) * SUBS
            out[at : at + 3, :] = jnp.where(last, got[:3, cut], sent[:3, cut])
            out[at + 3 : at + 6, :] = jnp.where(line == 0, got[3:6, cut], sent[3:6, cut])
            out[at + 6 : at + SUBS, :] = jnp.zeros((2, LANES), jnp.float32)


def windows(main, above, below, got, sent, span, height, own, count):
    def body(*refs):
        windows_kernel(*refs, span=span, height=height, own=own, count=count)

    return pl.pallas_call(
        body,
        out_shape=[pltpu.VMEM((WINDOW, LANES), jnp.float32)] * count,
        scratch_shapes=[
            pltpu.VMEM((5, height + 2 * SUBS, LANES), jnp.float32),
            pltpu.VMEM((2, count + 2, own, LANES), jnp.float32),
            pltpu.VMEM((count + 2, SUBS, LANES), jnp.float32),
            pltpu.VMEM((LANES, LANES), jnp.float32),
        ],
        name="windows",
    )(*near(main, above, below, got, sent))


def assemble(main, above, below, sent, strip, tile, tops, turn, flat, own):
    count = len(sent)
    line = lax.axis_index("gy")
    _, _, width = strip.shape
    _, rows, _ = tile.shape
    cols, height = width - LANES, rows - SUBS
    sub = lax.broadcasted_iota(jnp.int32, (SUBS, LANES), 0)
    turn[...] = jnp.zeros_like(turn)
    tops[:, height:, :] = jnp.zeros((2, SUBS, 2 * LANES), jnp.float32)
    for f in range(5):
        tile[f, height:, :LANES] = jnp.zeros((SUBS, LANES), jnp.float32)
        tile[f, :height, :LANES] = main[f * height : (f + 1) * height, :]
        tile[f, height : height + 3, :LANES] = below[3 * f : 3 * f + 3, :]
        tile[f, rows - 3 :, :LANES] = above[3 * f : 3 * f + 3, :]
    for s in range(count):
        part = sent[s]
        who = (line - s) % count
        at = pl.multiple_of(who * LANES, LANES)
        first = pl.multiple_of(who * own, own)
        for f in range(5):
            strip[f, :, pl.ds(at, LANES)] = part[2 * f * SUBS : (2 * f + 2) * SUBS, :]
        for f in range(2):
            tops[f, pl.ds(first, own), :LANES] = part[(10 + f) * SUBS : (11 + f) * SUBS, :]
            tops[f, pl.ds(first, own), LANES:] = part[(12 + f) * SUBS : (13 + f) * SUBS, :]

        @pl.when(who == 0)
        def _(part=part):
            for f in range(2):
                tops[f, height : height + 2, :LANES] = part[14 * SUBS + 2 * f : 14 * SUBS + 2 * f + 2, :]
                tops[f, height : height + 2, LANES:] = part[14 * SUBS + 4 + 2 * f : 14 * SUBS + 6 + 2 * f, :]
            for j in range(2):
                turn[0, :3, j * LANES : (j + 1) * LANES] = part[(15 + j) * SUBS + 3 : (15 + j) * SUBS + 6, :]

        @pl.when(who == count - 1)
        def _(part=part):
            for f in range(2):
                tops[f, rows - 2 :, :LANES] = part[14 * SUBS + 2 * f : 14 * SUBS + 2 * f + 2, :]
                tops[f, rows - 2 :, LANES:] = part[14 * SUBS + 4 + 2 * f : 14 * SUBS + 6 + 2 * f, :]
            for j in range(2):
                turn[0, LANES - 3 :, j * LANES : (j + 1) * LANES] = part[(15 + j) * SUBS : (15 + j) * SUBS + 3, :]

    for j in range(2):
        cut = slice(j * LANES, (j + 1) * LANES)
        turn[1, LANES - 3 :, cut] = sent[1 % count][(15 + j) * SUBS : (15 + j) * SUBS + 3, :]
        turn[1, :3, cut] = sent[-1][(15 + j) * SUBS + 3 : (15 + j) * SUBS + 6, :]
    beside = turn[1].T
    flat[...] = turn[0].T
    first = pl.multiple_of(line * own, SUBS)
    before = pl.multiple_of(jnp.where(line > 0, line * own - SUBS, height), SUBS)
    for f in range(5):
        tile[f, :, LANES:] = beside[f * rows : (f + 1) * rows]
        strip[f, :own, cols:] = flat[pl.ds(first + f * rows, SUBS), :]
        strip[f, own:, cols:] = ring(flat[pl.ds(before + f * rows, SUBS), :], flat[pl.ds(first + f * rows + SUBS, SUBS), :], sub)


def flow(fields, top, conduct, row_flags, col_flags, own_rows, own_cols):
    water, level, convey, land, rain = fields
    rows, width = water.shape
    r = lax.broadcasted_iota(jnp.int32, (rows, width), 0)
    c = lax.broadcasted_iota(jnp.int32, (rows, width), 1)
    row_ok = jnp.where(r < own_rows, 1, jnp.where(r >= rows - 3, row_flags[0], jnp.where(r < own_rows + 3, row_flags[1], 0)))
    col_ok = jnp.where(c < own_cols, 1, jnp.where(c >= width - 3, col_flags[0], jnp.where(c < own_cols + 3, col_flags[1], 0)))
    root = jnp.sqrt(convey) * (row_ok * col_ok).astype(jnp.float32)
    leak = land * conduct
    ahead = [lambda x: pltpu.roll(x, rows - 1, 0), lambda x: pltpu.roll(x, width - 1, 1)]
    gates = [root * f(root) for f in ahead]
    exchange = jnp.zeros_like(water)
    for _ in range(PASSES):
        surface = level + water
        power = jnp.where(water > 0.0, jnp.exp2((5.0 / 3.0) * jnp.log2(jnp.maximum(water, 1e-30))), 0.0)
        outflow = jnp.zeros_like(water)
        for axis in range(2):
            slope = surface - ahead[axis](surface)
            carried = jnp.where(slope >= 0.0, power, ahead[axis](power))
            flux = gates[axis] * carried * slope * lax.rsqrt(jnp.maximum(jnp.abs(slope), SLOPE_FLOOR))
            outflow = outflow + flux - pltpu.roll(flux, 1, axis)
        rate = leak * (water - top)
        exchange = exchange + SURFACE_STEP * rate
        water = jnp.maximum(water + SURFACE_STEP * (rain - rate - outflow), 0.0)
    return water, exchange


def last_kernel(tab_ref, strip, tile, tops, top_ref, class_ref, next_ref, head_out, water_ref, new_ref, sem):
    own = new_ref.shape[1]
    _, rows, width = strip.shape
    cols = width - LANES
    height, across = water_ref.shape
    ok = place()
    group, groups = lax.axis_index("grp"), lax.axis_size("grp")
    column = lax.axis_index("gx") * lax.axis_size("gy") + lax.axis_index("gy")
    columns_all = lax.axis_size("gx") * lax.axis_size("gy")

    def flags(*tests):
        return [jnp.where(t, 1, 0) for t in tests]

    root = top_ref[4]
    _, gain = flow([strip[f] for f in range(5)], top_ref[3], 0.25 * root * root, ok[:2], ok[2:], own, cols)
    mask = soil_mask(ok, rows, width, own, cols)
    p = top_ref[0] + gain * top_ref[1]
    content, capacity, root = wide([closure(params(tab_ref, class_ref[:, ch]), p[:, ch]) for ch in chunks(width)])
    h = root * mask
    q = h * p
    low, low_q, low_n, low_d, weights, flows = (next_ref[i] for i in range(6))

    def inner(x):
        return x[:own, :cols]

    top_n = inner(capacity * p - (content - top_ref[2]) + gain + h * lateral(q)) + inner(h) * (low_q - GRAVITY_STEP * low)
    new_ref[0] = top_n / (inner(capacity + h * lateral(h)) + inner(h) * low)
    low_n = low_n + low * (flows + inner(q) + GRAVITY_STEP * inner(h))
    new_ref[1] = low_n / (low_d + low * (weights + inner(h)))
    copy = pltpu.make_async_copy(new_ref, head_out.at[:TOP_LAYERS], sem)
    copy.start()
    roots = [closure(params(tab_ref, tops[1, :, ch].astype(jnp.int32)), tops[0, :, ch])[2] for ch in chunks(tile.shape[2])]
    root = jnp.concatenate(roots, axis=1)
    water, _ = flow(
        [tile[f] for f in range(5)], tops[0], 0.25 * root * root,
        flags(group > 0, group < groups - 1), flags(column > 0, column < columns_all - 1), height, across,
    )
    water_ref[...] = water[:height, :across]
    copy.wait()


def finish(tables, fields, tops, head, water, count):
    _, own, cols = head.shape
    height, across = water
    whole = count == 0
    rows, width, high, broad = own + SUBS, cols + LANES, height + SUBS, across + LANES
    n = len(fields)

    def body(*refs):
        tab_ref, given, known, (head_out, water_ref) = refs[0], refs[1 : 1 + n], refs[1 + n : 4 + n], refs[5 + n : 7 + n]
        rest = refs[7 + n :]
        if whole:
            strip, tile, above = given
        else:
            strip, tile, above = rest[2:5]
            assemble(*given[:3], given[3:], strip, tile, above, *rest[5:], own)
        last_kernel(tab_ref, strip, tile, above, *known, head_out, water_ref, *rest[:2])

    vmem = pl.BlockSpec(memory_space=pltpu.VMEM)
    scratch = [pltpu.VMEM((TOP_LAYERS, own, cols), jnp.float32), pltpu.SemaphoreType.DMA]
    if not whole:
        scratch += [
            pltpu.VMEM(shape, jnp.float32)
            for shape in ((5, rows, width), (5, high, broad), (2, high, broad), (2, LANES, 2 * LANES), (2 * LANES, LANES))
        ]
    return pl.pallas_call(
        body,
        out_shape=(jax.ShapeDtypeStruct(head.shape, jnp.float32), jax.ShapeDtypeStruct(water, jnp.float32)),
        in_specs=[vmem] * (n + 4) + [pl.BlockSpec(memory_space=pl.ANY)],
        out_specs=[pl.BlockSpec(memory_space=pl.ANY), vmem],
        scratch_shapes=scratch,
        input_output_aliases={n + 4: 0},
        name="surface_and_top",
    )(*near(tables, *fields, *tops), head)


def lane_rows(size):
    return -(-size // LANES)


def as_lanes(x):
    if x.shape[-1] % LANES:
        x = jnp.pad(x.reshape(-1), (0, -x.size % LANES))
    return x.reshape(-1, LANES)


def from_lanes(x, shape):
    if shape[-1] % LANES:
        size = 1
        for length in shape:
            size *= length
        x = x.reshape(-1)[:size]
    return x.reshape(shape)


def gx_trade(edges, half):
    got = shift(edges, "gx", 1)
    if lax.axis_size("gx") == 2:
        return got
    return jnp.where(half, got, shift(edges, "gx", -1))


def cyclic_rows(mid, above, below, gap):
    hole = jnp.zeros(mid.shape[:-2] + (gap, mid.shape[-1]), mid.dtype)
    return jnp.concatenate([mid, below, hole, above], axis=-2)


def block_general(pressure, soil_class, depth, elevation, roughness, rain, land_mask, channel_mask):
    ny = lax.axis_size("gy")
    _, own, cols = pressure.shape
    srows, scols = depth.shape
    convey = (1.0 + channel_mask.astype(jnp.float32)) / roughness
    surf = jnp.stack([depth, elevation, convey, LEAKANCE * land_mask.astype(jnp.float32), rain])
    tops = jnp.stack([pressure[0], soil_class[0].astype(jnp.float32)])

    def pack(s, t):
        return jnp.concatenate([as_lanes(s), as_lanes(t)], axis=0)

    def unpack(m):
        cut = lane_rows(15 * scols)
        return from_lanes(m[:cut], (5, 3, scols)), from_lanes(m[cut:], (2, 2, cols))

    s_above, t_above = unpack(shift(pack(surf[:, -3:], tops[:, -2:]), "grp", 1))
    s_below, t_below = unpack(shift(pack(surf[:, :3], tops[:, :2]), "grp", -1))
    surf_rows = cyclic_rows(surf, s_above, s_below, 2)
    tops_rows = jnp.concatenate([tops, t_below, t_above], axis=1)

    def edges(cut):
        a = surf_rows[:, :, cut(3)].transpose(0, 2, 1).reshape(15, -1)
        b = tops_rows[:, :, cut(2)].transpose(0, 2, 1).reshape(4, -1)
        return jnp.concatenate([a, jnp.pad(b, ((0, 0), (0, a.shape[1] - b.shape[1])))], axis=0)

    out = jnp.concatenate([edges(lambda n: slice(-n, None)), edges(lambda n: slice(0, n))])
    got = gx_trade(out, lax.broadcasted_iota(jnp.int32, out.shape, 0) < 19)
    mine = jnp.concatenate(
        [as_lanes(surf_rows), as_lanes(tops_rows), jnp.pad(got, ((0, 0), (0, -got.shape[1] % LANES))).reshape(-1, LANES)]
    )
    every = lax.all_gather(mine, "gy", axis=0, tiled=False)
    n1 = lane_rows(surf_rows.size)
    n2 = n1 + lane_rows(tops_rows.size)
    e_surf = jax.vmap(lambda m: from_lanes(m, (5, srows + SUBS, scols)))(every[:, :n1])
    e_surf = e_surf.transpose(1, 2, 0, 3).reshape(5, srows + SUBS, ny * scols)
    e_tops = every[:, n1:n2].reshape(ny, 2, own + 4, cols)
    e_m = every[:, n2:].reshape(ny, 2, 19, -1)
    main = e_tops[:, :, :own].transpose(1, 0, 2, 3).reshape(2, srows, cols)
    zeros = jnp.zeros((2, 4, cols), jnp.float32)
    f_tops = jnp.concatenate([main, e_tops[0, :, own : own + 2], zeros, e_tops[-1, :, own + 2 :]], axis=1)
    height = srows + SUBS
    c_left = e_m[-1, 0, :15, :height].reshape(5, 3, height).transpose(0, 2, 1)
    c_right = e_m[0, 1, :15, :height].reshape(5, 3, height).transpose(0, 2, 1)
    hole = jnp.zeros((5, height, LANES - 6), jnp.float32)
    blocks = jnp.concatenate([e_surf, c_right, hole, c_left], axis=2)

    def tops_edge(side):
        t = e_m[:, side, 15:, : own + 4].reshape(ny, 2, 2, own + 4)
        mid = t[..., :own].transpose(1, 0, 3, 2).reshape(2, srows, 2)
        low = t[0, :, :, own : own + 2].transpose(0, 2, 1)
        high = t[-1, :, :, own + 2 :].transpose(0, 2, 1)
        return jnp.concatenate([mid, low, jnp.zeros((2, 4, 2), jnp.float32), high], axis=1)

    top_blocks = jnp.concatenate(
        [f_tops, tops_edge(1), jnp.zeros((2, height, LANES - 4), jnp.float32), tops_edge(0)], axis=2
    )
    line = lax.axis_index("gy")

    def around(first, length, total, room):
        spot = jnp.arange(room)
        return (first + jnp.where(spot < length + 3, spot, spot - room)) % total

    strip = jnp.take(blocks, around(line * own, own, height, own + SUBS), axis=1)
    across = around(line * scols, scols, cols + LANES, -(-(scols + 6) // LANES) * LANES)
    return strip, jnp.take(blocks, across, axis=2), jnp.take(top_blocks, across, axis=2)


def local(
    pressure, soil_class, capacity_range, inverse_entry, shape_index, conductivity,
    depth, elevation, roughness, rain, land_mask, channel_mask,
):
    ny = lax.axis_size("gy")
    _, own, _ = pressure.shape
    srows, scols = depth.shape
    ground = (depth, elevation, roughness, rain, land_mask, channel_mask)
    classes = (capacity_range, inverse_entry, shape_index, conductivity)
    even = scols == LANES and own == SUBS
    tables, *packed = pack(pressure, soil_class, classes, ground if even else ())
    after, before, after_end, before_end = packed[-4:]
    surface = ()
    if even:
        main, strip_after, strip_before = packed[:3]
        above = shift(strip_after, "grp", 1)
        below = shift(strip_before, "grp", -1)
        surface = (main, above, below)
    rows = ("grp", "gy")
    up_end = shift(after_end, rows, 1)
    down_end = shift(before_end, rows, -1)
    sent = columns(pressure, soil_class, up_end, down_end, surface)
    up = shift(after, rows, 1)
    down = shift(before, rows, -1)
    span = pressure.shape[0] * (own + SUBS)
    half = jnp.where(lax.broadcasted_iota(jnp.int32, sent.shape, 1) < span, 4, 3)
    got = gx_trade(sent, lax.broadcasted_iota(jnp.int32, sent.shape, 0) < half)
    if even:
        outs = windows(main, above, below, got, sent, span, srows, own, ny)
        fields = [main, above, below, outs[0]] + [shift(outs[step], "gy", step) for step in range(1, ny)]
    else:
        fields = block_general(pressure, soil_class, *ground)
    head, *tops = soil_interior(tables, pressure, soil_class, up, down, got, sent)
    return finish(tables, fields, tops, head, (srows, scols), ny if even else 0)


def solution(mesh):
    soil = P(None, ("grp", "gy"), "gx")
    ground = P("grp", ("gx", "gy"))

    return jax.shard_map(
        local,
        mesh=mesh,
        in_specs=(soil, soil, P(), P(), P(), P()) + (ground,) * 6,
        out_specs=(soil, ground),
        check_vma=False,
    )
```

```python
import jax
import jax.numpy as jnp
from jax import lax
from jax.experimental import pallas as pl
from jax.experimental.pallas import tpu as pltpu
from jax.sharding import PartitionSpec as P


PASSES = 3
STORAGE = 0.01
GRAVITY_STEP = 0.5
SUCTION_FLOOR = 0.01
SLOPE_FLOOR = 0.1
SURFACE_STEP = 0.3
LEAKANCE = 0.5

LANES = 128
SUBS = 8
UNROLL = 8
TOP_LAYERS = 2


def shift(x, axis, step):
    size = lax.axis_size(axis)
    return lax.ppermute(x, axis, [(i, (i + step) % size) for i in range(size)])


def near(*arrays):
    return [pltpu.with_memory_space_constraint(x, pltpu.VMEM) for x in arrays]


def class_tables(refs):
    lane = lax.broadcasted_iota(jnp.int32, (1, LANES), 1)
    spread = []
    for ref in refs:
        row = jnp.ones((1, LANES), jnp.float32)
        for k in range(ref.shape[0]):
            row = jnp.where(lane == k, ref[k], row)
        spread.append(row)
    span, entry, shape, ks = spread
    pore = 1.0 - 1.0 / shape
    rows = [-entry, 1.0 / (1.0 - pore), pore, span, 2.0 * jnp.sqrt(ks)]
    return jnp.concatenate(rows + [jnp.zeros((SUBS - len(rows), LANES), jnp.float32)], axis=0)


def place():
    tile = lax.axis_index("grp") * lax.axis_size("gy") + lax.axis_index("gy")
    tiles = lax.axis_size("grp") * lax.axis_size("gy")
    column, columns = lax.axis_index("gx"), lax.axis_size("gx")
    tests = (tile > 0, tile < tiles - 1, column > 0, column < columns - 1)
    return [jnp.where(t, 1, 0) for t in tests]


def params(tab_ref, idx):
    return [
        jnp.take_along_axis(jnp.broadcast_to(tab_ref[i : i + 1, :], idx.shape), idx, axis=1, mode="promise_in_bounds")
        for i in range(5)
    ]


def closure(given, p):
    entry, expo, pore, span, scale = given
    logs = jnp.log2(jnp.maximum(entry * p, SUCTION_FLOOR))
    total = jnp.log2(1.0 + jnp.exp2(expo * logs))
    drop = pore * total
    less = expo - 1.0
    power = less * logs - drop
    ratio = jnp.exp2(power)
    content = span * jnp.exp2(-drop)
    capacity = STORAGE - (span * entry * less) * jnp.exp2(power - total)
    root = scale * jnp.exp2(-0.25 * drop) * jnp.abs(1.0 - ratio)
    return content, capacity, root


def chunks(width):
    return [slice(i, i + LANES) for i in range(0, width, LANES)]


def wide(parts):
    return [jnp.concatenate(x, axis=1) for x in zip(*parts)]


def lateral(x):
    rows, width = x.shape
    return (
        pltpu.roll(x, 1, 0)
        + pltpu.roll(x, rows - 1, 0)
        + pltpu.roll(x, 1, 1)
        + pltpu.roll(x, width - 1, 1)
    )


def soil_mask(ok, rows, width, own_rows, own_cols):
    r = lax.broadcasted_iota(jnp.int32, (rows, width), 0)
    c = lax.broadcasted_iota(jnp.int32, (rows, width), 1)
    above = jnp.where(r >= rows - 2, ok[0], 0)
    below = jnp.where((r >= own_rows) & (r < own_rows + 2), ok[1], 0)
    left = jnp.where(c >= width - 2, ok[2], 0)
    right = jnp.where((c >= own_cols) & (c < own_cols + 2), ok[3], 0)
    in_rows = jnp.where(r < own_rows, 1, above + below)
    in_cols = jnp.where(c < own_cols, 1, left + right)
    return (in_rows * in_cols).astype(jnp.float32)


def soil_rows(p_ref, c_ref, blocks, next_ref, prev_ref, next_end, prev_end):
    layers, own, cols = p_ref.shape
    start = lax.broadcasted_iota(jnp.int32, (layers, LANES), 1) < LANES // 2
    for f, x in enumerate((p_ref, c_ref)):
        blocks[f] = x[:, :, :LANES].astype(jnp.float32)
        blocks[2 + f] = x[:, :, cols - LANES :].astype(jnp.float32)
        for r in range(2):
            next_ref[f, r] = x[:, own - 2 + r, :].astype(jnp.float32)
            prev_ref[f, r] = x[:, r, :].astype(jnp.float32)
        next_end[f] = jnp.where(start, next_ref[f, 1, :, :LANES], next_ref[f, 1, :, cols - LANES :])
        prev_end[f] = jnp.where(start, prev_ref[f, 0, :, :LANES], prev_ref[f, 0, :, cols - LANES :])


def soil_columns(blocks, up_end, down_end, box):
    _, layers, own, _ = blocks.shape
    rows = box.shape[1]
    out = []
    for side in (2, 0):
        for f in range(2):
            box[:, 2 : 2 + own, :] = blocks[side + f]
            box[:, 0, :] = jnp.zeros((layers, LANES), jnp.float32)
            box[:, 1, :] = up_end[f]
            box[:, own + 2, :] = down_end[f]
            box[:, own + 3 :, :] = jnp.zeros((layers, rows - own - 3, LANES), jnp.float32)
            turned = box[...].reshape(layers * rows, LANES).T
            out.append(turned[LANES - 2 :] if len(out) < 2 else turned[:2])
    return jnp.concatenate(out, axis=0)


def soil_kernel(
    tab_ref, p_far, c_far, up_in, down_in, got_in, sent_in, out_far, top_out, class_out, next_out,
    p_in, c_in, out_ref, tile_sem, out_sem, h_ref, q_ref, n_ref, d_ref, k_ref, h2_ref, q2_ref, n2_ref, d2_ref, given, corner, turn, near, near2, pe, ce,
):
    layers, own, cols = p_in.shape
    rows = own + SUBS
    span = layers * rows
    f32 = jnp.float32
    ok = place()

    def tile_copy(i, j):
        part = pl.ds(j * UNROLL, UNROLL)
        far, here = ((p_far, p_in), (c_far, c_in))[i]
        return pltpu.make_async_copy(far.at[part], here.at[part], tile_sem.at[i, j])

    def out_copy(j):
        part = pl.ds(j * UNROLL, UNROLL)
        return pltpu.make_async_copy(out_ref.at[part], out_far.at[part], out_sem.at[j])

    got, sent = got_in[:, :span], sent_in[:, :span]
    groups = layers // UNROLL
    for j in range(groups):
        tile_copy(0, j).start()
        tile_copy(1, j).start()
    for ref in (h_ref, q_ref, h2_ref, q2_ref):
        ref[0] = jnp.zeros((own, cols), f32)
        ref[layers + 1] = jnp.zeros((own, cols), f32)

    gap = jnp.zeros((1, span), f32)
    p = jnp.concatenate([got[0:2], sent[4:5], gap, sent[1:2], got[4:6], gap], axis=0)
    kind = jnp.concatenate([got[2:4], sent[6:7], gap, sent[3:4], got[6:8], gap], axis=0).astype(jnp.int32)
    sub = lax.broadcasted_iota(jnp.int32, (SUBS, span), 0)
    lane = lax.broadcasted_iota(jnp.int32, (SUBS, span), 1)
    row = lane % rows
    row_ok = jnp.where(row < 2, ok[0], jnp.where(row < own + 2, 1, jnp.where(row < own + 4, ok[1], 0)))
    col_ok = jnp.where(sub < 2, ok[2], jnp.where((sub == 2) | (sub == 4), 1, jnp.where((sub == 5) | (sub == 6), ok[3], 0)))
    mask = (row_ok * col_ok).astype(f32)
    values = [params(tab_ref, kind[:, ch]) for ch in chunks(span)]
    content, capacity, root = wide([closure(v, p[:, ch]) for v, ch in zip(values, chunks(span))])
    h, q = root * mask, root * mask * p

    def over(x):
        return jnp.where(lane < rows, 0.0, pltpu.roll(x, rows, 1))

    def under(x):
        return jnp.where(lane >= span - rows, 0.0, pltpu.roll(x, span - rows, 1))

    weights = lateral(h) + over(h) + under(h)
    flows = lateral(q) + over(q) + under(q) + GRAVITY_STEP * (over(h) - under(h))
    p1 = (capacity * p + h * flows) / (capacity + h * weights)
    root = wide([closure(v, p1[:, ch]) for v, ch in zip(values, chunks(span))])[2] * mask
    turn[...] = jnp.zeros_like(turn)
    for i, x in enumerate((h, q, root, root * p1)):
        turn[i * SUBS : (i + 1) * SUBS, :] = x
    corner[...] = turn[...].T.reshape(layers, rows, LANES)

    def first(z):
        for ch in chunks(cols):
            p = p_in[z, :, ch]
            values = params(tab_ref, c_in[z, :, ch])
            for i, v in enumerate(values):
                given[i, z, :, ch] = v
            content, capacity, root = closure(values, p)
            h_ref[z + 1, :, ch] = root
            q_ref[z + 1, :, ch] = root * p
            n_ref[z, :, ch] = capacity * p
            d_ref[z, :, ch] = capacity
            k_ref[z, :, ch] = content

    def first_group(j, carry):
        tile_copy(0, j).wait()
        tile_copy(1, j).wait()
        for i in range(UNROLL):
            first(j * UNROLL + i)
        return carry

    lax.fori_loop(0, groups, first_group, 0)

    zsub = lax.broadcasted_iota(jnp.int32, (layers, cols), 0)
    zlane = lax.broadcasted_iota(jnp.int32, (layers, LANES), 1)

    def sides(x, edge, at, lanes):
        left, right = pltpu.roll(x, 1, 1), pltpu.roll(x, cols - 1, 1)
        a = jnp.where(lanes == 0, pltpu.roll(edge, LANES - at, 1), left[:, :LANES])
        b = jnp.where(lanes == LANES - 1, pltpu.roll(edge, LANES - 1 - (at + 4), 1), right[:, cols - LANES :])
        return jnp.concatenate([a, left[:, LANES:]], axis=1) + jnp.concatenate([right[:, : cols - LANES], b], axis=1)

    for side, (halo, close, far, edge_row, valid) in enumerate(((up_in, 1, 0, 1, ok[0]), (down_in, 0, 1, own + 2, ok[1]))):
        inside = valid.astype(f32)
        ours = 0 if side == 0 else own - 1
        values, states, beyond = [], [], []
        for ch in chunks(cols):
            p = halo[0, close, :, ch]
            v = params(tab_ref, halo[1, close, :, ch].astype(jnp.int32))
            content, capacity, root = closure(v, p)
            root = root * inside
            values.append(v)
            states.append((p, capacity, root, root * p))
            p = halo[0, far, :, ch]
            root = closure(params(tab_ref, halo[1, far, :, ch].astype(jnp.int32)), p)[2] * inside
            beyond.append((root, root * p))
        p, capacity, h, q = wide(states)
        far_h, far_q = wide(beyond)
        near[side, 0] = h
        near[side, 1] = q
        edge = corner[:, edge_row, :]
        top_h = jnp.where(zsub == 0, 0.0, pltpu.roll(h, 1, 0))
        low_h = jnp.where(zsub == layers - 1, 0.0, pltpu.roll(h, layers - 1, 0))
        top_q = jnp.where(zsub == 0, 0.0, pltpu.roll(q, 1, 0))
        low_q = jnp.where(zsub == layers - 1, 0.0, pltpu.roll(q, layers - 1, 0))
        weights = far_h + h_ref[1 : layers + 1, ours, :] + sides(h, edge, 1, zlane) + top_h + low_h
        flows = far_q + q_ref[1 : layers + 1, ours, :] + sides(q, edge, 1 + SUBS, zlane) + top_q + low_q + GRAVITY_STEP * (top_h - low_h)
        p1 = (capacity * p + h * flows) / (capacity + h * weights)
        for v, ch in zip(values, chunks(cols)):
            root = closure(v, p1[:, ch])[2] * inside
            near2[side, 0, :, ch] = root
            near2[side, 1, :, ch] = root * p1[:, ch]

    tsub = lax.broadcasted_iota(jnp.int32, (own, cols), 0)
    tlane = lax.broadcasted_iota(jnp.int32, (own, LANES), 1)

    def around(z, h, q, rim, at):
        edge = corner[z, 2 : 2 + own, :]
        out = []
        for i, x in enumerate((h[z + 1], q[z + 1])):
            above = jnp.where(tsub == 0, rim[0, i, pl.ds(z, 1), :], pltpu.roll(x, 1, 0))
            below = jnp.where(tsub == own - 1, rim[1, i, pl.ds(z, 1), :], pltpu.roll(x, own - 1, 0))
            out.append(above + below + sides(x, edge, at + i * SUBS, tlane))
        weights, flows = out
        low = h[z + 2]
        return weights + low, flows + q[z + 2] - GRAVITY_STEP * low

    def second(z, carry):
        mid, top = h_ref[z + 1], h_ref[z]
        weights, flows = around(z, h_ref, q_ref, near, 1)
        flows = flows + q_ref[z] + GRAVITY_STEP * top
        p1 = (n_ref[z] + mid * flows) / (d_ref[z] + mid * (weights + top))
        for ch in chunks(cols):
            p = p1[:, ch]
            content, capacity, root = closure([given[i, z, :, ch] for i in range(5)], p)
            h2_ref[z + 1, :, ch] = root
            q2_ref[z + 1, :, ch] = root * p
            n2_ref[z, :, ch] = capacity * p - (content - k_ref[z, :, ch])
            d2_ref[z, :, ch] = capacity
        return carry

    lax.fori_loop(0, layers, second, 0, unroll=UNROLL)

    def third(z):
        mid, top = h2_ref[z + 1], h2_ref[z]
        weights, flows = around(z, h2_ref, q2_ref, near2, 1 + 2 * SUBS)
        flows = flows + q2_ref[z] + GRAVITY_STEP * top
        out_ref[z] = (n2_ref[z] + mid * flows) / (d2_ref[z] + mid * (weights + top))

    def third_group(j, carry):
        for i in range(UNROLL):
            third(j * UNROLL + i)
        out_copy(j).start()
        return carry

    lax.fori_loop(0, groups, third_group, 0)

    weights, flows = around(1, h2_ref, q2_ref, near2, 1 + 2 * SUBS)
    for i, x in enumerate((h2_ref[2], q2_ref[2], n2_ref[1], d2_ref[1], weights, flows)):
        next_out[i] = x
    for f, (src, dst, halo_at) in enumerate(((p_in, pe, 0), (c_in, ce, 2))):
        turn[...] = jnp.zeros_like(turn)
        turn[LANES - 2 :, :] = got[halo_at : halo_at + 2]
        turn[:2, :] = got[halo_at + 4 : halo_at + 6]
        block = turn[:, :LANES].T
        for z in range(2):
            dst[z, own:, :cols] = jnp.zeros((SUBS, cols), dst.dtype)
            dst[z, :own, :cols] = src[z]
            dst[z, :, cols:] = jnp.zeros((rows, LANES), dst.dtype)
            dst[z, : own + 2, cols:] = block[z * rows + 2 : z * rows + own + 4].astype(dst.dtype)
            dst[z, rows - 2 :, cols:] = block[z * rows : z * rows + 2].astype(dst.dtype)
            for r in range(2):
                dst[z, own + r : own + r + 1, :cols] = down_in[f, r, z : z + 1, :].astype(dst.dtype)
                dst[z, rows - 2 + r : rows - 1 + r, :cols] = up_in[f, r, z : z + 1, :].astype(dst.dtype)
    width = cols + LANES
    mask = soil_mask(ok, rows, width, own, cols)
    states = []
    for z in range(2):
        content, capacity, root = wide([closure(params(tab_ref, ce[z, :, ch]), pe[z, :, ch]) for ch in chunks(width)])
        states.append((content, capacity, root * mask))
    content, capacity, h = states[0]
    low = states[1][2]
    weights = lateral(h) + low
    flows = lateral(h * pe[0]) + low * pe[1] - GRAVITY_STEP * low
    weight = capacity + h * weights
    top_out[0] = (capacity * pe[0] + h * flows) / weight
    top_out[1] = 1.0 / weight
    top_out[2] = content
    top_out[3] = pe[0]
    top_out[4] = h
    for j in range(groups):
        out_copy(j).wait()
    class_out[...] = ce[0]


def soil_interior(tables, pressure, soil_class, up, down, got, sent):
    layers, own, cols = pressure.shape
    rows, width = own + SUBS, cols + LANES
    f32 = jnp.float32
    span = layers * rows
    tall = pltpu.VMEM((layers + 2, own, cols), f32)
    flat = pltpu.VMEM((layers, own, cols), f32)
    vmem = pl.BlockSpec(memory_space=pltpu.VMEM)
    far = pl.BlockSpec(memory_space=pl.ANY)
    return pl.pallas_call(
        soil_kernel,
        out_shape=(
            jax.ShapeDtypeStruct(pressure.shape, f32),
            pltpu.VMEM((5, rows, width), f32),
            pltpu.VMEM((rows, width), jnp.int32),
            pltpu.VMEM((6, own, cols), f32),
        ),
        in_specs=[vmem] + [far] * 2 + [vmem] * 4,
        out_specs=[far] + [vmem] * 3,
        scratch_shapes=[flat, pltpu.VMEM((layers, own, cols), jnp.int32), flat]
        + [pltpu.SemaphoreType.DMA((2, layers // UNROLL)), pltpu.SemaphoreType.DMA((layers // UNROLL,))]
        + [tall, tall, flat, flat, flat, tall, tall, flat, flat]
        + [
            pltpu.VMEM((5, layers, own, cols), f32),
            pltpu.VMEM((layers, rows, LANES), f32),
            pltpu.VMEM((LANES, span), f32),
            pltpu.VMEM((2, 2, layers, cols), f32),
            pltpu.VMEM((2, 2, layers, cols), f32),
            pltpu.VMEM((2, rows, width), f32),
            pltpu.VMEM((2, rows, width), jnp.int32),
        ],
        name="soil_interior",
    )(*near(tables), pressure, soil_class, *near(up, down, got, sent))


def surface_rows(p_ref, c_ref, depth, level, rough, rain, land, channel, main_ref, next_ref, prev_ref):
    height, _ = depth.shape
    _, own, cols = p_ref.shape
    fields = (
        depth[...],
        level[...],
        (1.0 + channel[...].astype(jnp.float32)) / rough[...],
        LEAKANCE * land[...].astype(jnp.float32),
        rain[...],
    )
    for f, x in enumerate(fields):
        main_ref[f * height : (f + 1) * height, :] = x
        next_ref[3 * f : 3 * f + 3, :] = x[height - 3 :]
        prev_ref[3 * f : 3 * f + 3, :] = x[:3]
    base = 5 * height
    for f, x in enumerate((p_ref[0], c_ref[0].astype(jnp.float32))):
        for j, ch in enumerate(chunks(cols)):
            main_ref[base : base + own, :] = x[:, ch]
            base += own
            at = EDGE_ROWS + 2 * (f * (cols // LANES) + j)
            next_ref[at : at + 2, :] = x[own - 2 :, ch]
            prev_ref[at : at + 2, :] = x[:2, ch]


EDGE_ROWS = 16


def pack(pressure, soil_class, classes, ground):
    layers, own, cols = pressure.shape
    f32 = jnp.float32
    edge = pltpu.VMEM((2, 2, layers, cols), f32)
    end = pltpu.VMEM((2, layers, LANES), f32)
    out = [pltpu.VMEM((4, layers, own, LANES), f32), edge, edge, end, end]
    if ground:
        height = ground[0].shape[0]
        strip = pltpu.VMEM((EDGE_ROWS + 4 * cols // LANES, LANES), f32)
        out = [pltpu.VMEM((5 * height + 2 * own * cols // LANES, LANES), f32), strip, strip] + out

    def body(*refs):
        tables, rest = refs[: len(classes)], refs[len(classes) :]
        if ground:
            surface_rows(*rest[: 2 + len(ground)], *rest[3 + len(ground) : 6 + len(ground)])
        soil_rows(*rest[:2], *rest[-5:])
        rest[2 + len(ground)][...] = class_tables(tables)

    vmem = pl.BlockSpec(memory_space=pltpu.VMEM)
    smem = pl.BlockSpec(memory_space=pltpu.SMEM)
    return pl.pallas_call(
        body,
        out_shape=[pltpu.VMEM((SUBS, LANES), f32)] + out,
        in_specs=[smem] * len(classes) + [vmem] * (2 + len(ground)),
        name="pack",
    )(*classes, pressure, soil_class, *ground)


def surface_columns(main_ref, above_ref, below_ref, box, height, own, cols):
    n = cols // LANES
    tall = height + SUBS
    box[...] = jnp.zeros_like(box)
    for side, j in enumerate((n - 1, 0)):
        for f in range(2):
            at = (2 * side + f) * 2 * SUBS
            src = 5 * height + (f * n + j) * own
            strip = EDGE_ROWS + 2 * (f * n + j)
            box[at : at + own, :] = main_ref[src : src + own, :]
            box[at + own : at + own + 2, :] = below_ref[strip : strip + 2, :]
            box[at + own + 2 : at + own + 4, :] = above_ref[strip : strip + 2, :]
    for f in range(5):
        at = LANES + f * tall
        box[at : at + height, :] = main_ref[f * height : (f + 1) * height, :]
        box[at + height : at + height + 3, :] = below_ref[3 * f : 3 * f + 3, :]
        box[at + tall - 3 : at + tall, :] = above_ref[3 * f : 3 * f + 3, :]
    turned = box[...].T
    edges = jnp.concatenate([turned[LANES - 3 :], turned[:3], jnp.zeros((2, turned.shape[1]), jnp.float32)], axis=0)
    return edges


def columns(blocks, cols, up_end, down_end, surface):
    _, layers, own, _ = blocks.shape
    rows = own + SUBS
    span = layers * rows
    scratch = [pltpu.VMEM((layers, rows, LANES), jnp.float32)]
    width = span
    if surface:
        height = (surface[0].shape[0] - 2 * own * cols // LANES) // 5
        tall = LANES + 5 * (height + SUBS)
        tall += -tall % LANES
        width += tall
        scratch.append(pltpu.VMEM((tall, LANES), jnp.float32))

    n = 3 + len(surface)

    def body(*refs):
        out_ref, box = refs[n], refs[n + 1]
        out_ref[:, :span] = soil_columns(*refs[:3], box)
        if surface:
            out_ref[:, span:] = surface_columns(*refs[3:n], refs[n + 2], height, own, cols)

    return pl.pallas_call(
        body,
        out_shape=pltpu.VMEM((SUBS, width), jnp.float32),
        scratch_shapes=scratch,
        name="columns",
    )(*near(blocks, up_end, down_end, *surface))


def rim(at_end, at_start, lane, count):
    return jnp.where(lane >= LANES - count, at_end, jnp.where(lane < count, at_start, 0.0))


def ring(before, after, sub):
    return jnp.where(sub >= SUBS - 3, before, jnp.where(sub < 3, after, 0.0))


WINDOW = 136


def windows_kernel(main, above, below, got, sent, *refs, span, height, own, count):
    outs, (tall, wide_top, ends, turn) = refs[:count], refs[count:]
    line = lax.axis_index("gy")
    lane = lax.broadcasted_iota(jnp.int32, (SUBS, LANES), 1)
    sub = lax.broadcasted_iota(jnp.int32, (SUBS, LANES), 0)
    tall[...] = jnp.zeros_like(tall)
    ends[...] = jnp.zeros_like(ends)
    turn[...] = jnp.zeros_like(turn)
    for f in range(5):
        tall[f, SUBS : SUBS + height] = main[f * height : (f + 1) * height, :]
        tall[f, SUBS - 3 : SUBS] = above[3 * f : 3 * f + 3, :]
        tall[f, SUBS + height : SUBS + height + 3] = below[3 * f : 3 * f + 3, :]
    turn[LANES - 3 :, :] = got[:3, span : span + LANES]
    turn[:3, :] = got[3:6, span : span + LANES]
    block = turn[...].T
    last = line == count - 1
    for f in range(2):
        before, after = block[2 * f * SUBS :], block[2 * (2 + f) * SUBS :]
        beside = rim(before[:SUBS], after[:SUBS], lane, 2)
        beyond = rim(before[SUBS : 2 * SUBS], after[SUBS : 2 * SUBS], lane, 2)
        beyond = jnp.where(last, beyond[2:4], beyond[:2])
        for j in (0, count + 1):
            wide_top[f, j] = beside
            ends[j, 2 * f : 2 * f + 2] = beyond
        for j in range(count):
            src = 5 * height + (f * count + j) * own
            wide_top[f, j + 1] = main[src : src + own, :]
            at = EDGE_ROWS + 2 * (f * count + j)
            ends[j + 1, 2 * f : 2 * f + 2] = jnp.where(last, above[at : at + 2, :], below[at : at + 2, :])
    for s in range(count):
        who, out = (line + s) % count, outs[s]
        for f in range(5):
            first = pl.multiple_of(who * SUBS, SUBS)
            out[2 * f * SUBS : (2 * f + 1) * SUBS, :] = tall[f, pl.ds(first + SUBS, SUBS), :]
            out[(2 * f + 1) * SUBS : (2 * f + 2) * SUBS, :] = ring(
                tall[f, pl.ds(first, SUBS), :], tall[f, pl.ds(first + 2 * SUBS, SUBS), :], sub
            )
        for f in range(2):
            out[(10 + f) * SUBS : (11 + f) * SUBS, :] = wide_top[f, who + 1]
            out[(12 + f) * SUBS : (13 + f) * SUBS, :] = rim(wide_top[f, who], wide_top[f, who + 2], lane, 2)
        mid, side = ends[who + 1], rim(ends[who], ends[who + 2], lane, 2)
        out[14 * SUBS : 14 * SUBS + 4, :] = mid[:4]
        out[14 * SUBS + 4 : 15 * SUBS, :] = side[:4]
        for j in range(2):
            cut = slice(span + (j + 1) * LANES, span + (j + 2) * LANES)
            at = (15 + j) * SUBS
            out[at : at + 3, :] = jnp.where(last, got[:3, cut], sent[:3, cut])
            out[at + 3 : at + 6, :] = jnp.where(line == 0, got[3:6, cut], sent[3:6, cut])
            out[at + 6 : at + SUBS, :] = jnp.zeros((2, LANES), jnp.float32)


def windows(main, above, below, got, sent, span, height, own, count):
    def body(*refs):
        windows_kernel(*refs, span=span, height=height, own=own, count=count)

    return pl.pallas_call(
        body,
        out_shape=[pltpu.VMEM((WINDOW, LANES), jnp.float32)] * count,
        scratch_shapes=[
            pltpu.VMEM((5, height + 2 * SUBS, LANES), jnp.float32),
            pltpu.VMEM((2, count + 2, own, LANES), jnp.float32),
            pltpu.VMEM((count + 2, SUBS, LANES), jnp.float32),
            pltpu.VMEM((LANES, LANES), jnp.float32),
        ],
        name="windows",
    )(*near(main, above, below, got, sent))


def assemble(main, above, below, sent, strip, tile, tops, turn, flat, own):
    count = len(sent)
    line = lax.axis_index("gy")
    _, _, width = strip.shape
    _, rows, _ = tile.shape
    cols, height = width - LANES, rows - SUBS
    sub = lax.broadcasted_iota(jnp.int32, (SUBS, LANES), 0)
    turn[...] = jnp.zeros_like(turn)
    tops[:, height:, :] = jnp.zeros((2, SUBS, 2 * LANES), jnp.float32)
    for f in range(5):
        tile[f, height:, :LANES] = jnp.zeros((SUBS, LANES), jnp.float32)
        tile[f, :height, :LANES] = main[f * height : (f + 1) * height, :]
        tile[f, height : height + 3, :LANES] = below[3 * f : 3 * f + 3, :]
        tile[f, rows - 3 :, :LANES] = above[3 * f : 3 * f + 3, :]
    for s in range(count):
        part = sent[s]
        who = (line - s) % count
        at = pl.multiple_of(who * LANES, LANES)
        first = pl.multiple_of(who * own, own)
        for f in range(5):
            strip[f, :, pl.ds(at, LANES)] = part[2 * f * SUBS : (2 * f + 2) * SUBS, :]
        for f in range(2):
            tops[f, pl.ds(first, own), :LANES] = part[(10 + f) * SUBS : (11 + f) * SUBS, :]
            tops[f, pl.ds(first, own), LANES:] = part[(12 + f) * SUBS : (13 + f) * SUBS, :]

        @pl.when(who == 0)
        def _(part=part):
            for f in range(2):
                tops[f, height : height + 2, :LANES] = part[14 * SUBS + 2 * f : 14 * SUBS + 2 * f + 2, :]
                tops[f, height : height + 2, LANES:] = part[14 * SUBS + 4 + 2 * f : 14 * SUBS + 6 + 2 * f, :]
            for j in range(2):
                turn[0, :3, j * LANES : (j + 1) * LANES] = part[(15 + j) * SUBS + 3 : (15 + j) * SUBS + 6, :]

        @pl.when(who == count - 1)
        def _(part=part):
            for f in range(2):
                tops[f, rows - 2 :, :LANES] = part[14 * SUBS + 2 * f : 14 * SUBS + 2 * f + 2, :]
                tops[f, rows - 2 :, LANES:] = part[14 * SUBS + 4 + 2 * f : 14 * SUBS + 6 + 2 * f, :]
            for j in range(2):
                turn[0, LANES - 3 :, j * LANES : (j + 1) * LANES] = part[(15 + j) * SUBS : (15 + j) * SUBS + 3, :]

    for j in range(2):
        cut = slice(j * LANES, (j + 1) * LANES)
        turn[1, LANES - 3 :, cut] = sent[1 % count][(15 + j) * SUBS : (15 + j) * SUBS + 3, :]
        turn[1, :3, cut] = sent[-1][(15 + j) * SUBS + 3 : (15 + j) * SUBS + 6, :]
    beside = turn[1].T
    flat[...] = turn[0].T
    first = pl.multiple_of(line * own, SUBS)
    before = pl.multiple_of(jnp.where(line > 0, line * own - SUBS, height), SUBS)
    for f in range(5):
        tile[f, :, LANES:] = beside[f * rows : (f + 1) * rows]
        strip[f, :own, cols:] = flat[pl.ds(first + f * rows, SUBS), :]
        strip[f, own:, cols:] = ring(flat[pl.ds(before + f * rows, SUBS), :], flat[pl.ds(first + f * rows + SUBS, SUBS), :], sub)


def flow(fields, top, conduct, row_flags, col_flags, own_rows, own_cols):
    water, level, convey, land, rain = fields
    rows, width = water.shape
    r = lax.broadcasted_iota(jnp.int32, (rows, width), 0)
    c = lax.broadcasted_iota(jnp.int32, (rows, width), 1)
    row_ok = jnp.where(r < own_rows, 1, jnp.where(r >= rows - 3, row_flags[0], jnp.where(r < own_rows + 3, row_flags[1], 0)))
    col_ok = jnp.where(c < own_cols, 1, jnp.where(c >= width - 3, col_flags[0], jnp.where(c < own_cols + 3, col_flags[1], 0)))
    root = jnp.sqrt(convey) * (row_ok * col_ok).astype(jnp.float32)
    leak = land * conduct
    ahead = [lambda x: pltpu.roll(x, rows - 1, 0), lambda x: pltpu.roll(x, width - 1, 1)]
    gates = [root * f(root) for f in ahead]
    exchange = jnp.zeros_like(water)
    for _ in range(PASSES):
        surface = level + water
        power = jnp.where(water > 0.0, jnp.exp2((5.0 / 3.0) * jnp.log2(jnp.maximum(water, 1e-30))), 0.0)
        outflow = jnp.zeros_like(water)
        for axis in range(2):
            slope = surface - ahead[axis](surface)
            carried = jnp.where(slope >= 0.0, power, ahead[axis](power))
            flux = gates[axis] * carried * slope * lax.rsqrt(jnp.maximum(jnp.abs(slope), SLOPE_FLOOR))
            outflow = outflow + flux - pltpu.roll(flux, 1, axis)
        rate = leak * (water - top)
        exchange = exchange + SURFACE_STEP * rate
        water = jnp.maximum(water + SURFACE_STEP * (rain - rate - outflow), 0.0)
    return water, exchange


def last_kernel(tab_ref, strip, tile, tops, top_ref, class_ref, next_ref, head_out, water_ref, new_ref, sem):
    own = new_ref.shape[1]
    _, rows, width = strip.shape
    cols = width - LANES
    height, across = water_ref.shape
    ok = place()
    group, groups = lax.axis_index("grp"), lax.axis_size("grp")
    column = lax.axis_index("gx") * lax.axis_size("gy") + lax.axis_index("gy")
    columns_all = lax.axis_size("gx") * lax.axis_size("gy")

    def flags(*tests):
        return [jnp.where(t, 1, 0) for t in tests]

    root = top_ref[4]
    _, gain = flow([strip[f] for f in range(5)], top_ref[3], 0.25 * root * root, ok[:2], ok[2:], own, cols)
    mask = soil_mask(ok, rows, width, own, cols)
    p = top_ref[0] + gain * top_ref[1]
    content, capacity, root = wide([closure(params(tab_ref, class_ref[:, ch]), p[:, ch]) for ch in chunks(width)])
    h = root * mask
    q = h * p
    low, low_q, low_n, low_d, weights, flows = (next_ref[i] for i in range(6))

    def inner(x):
        return x[:own, :cols]

    top_n = inner(capacity * p - (content - top_ref[2]) + gain + h * lateral(q)) + inner(h) * (low_q - GRAVITY_STEP * low)
    new_ref[0] = top_n / (inner(capacity + h * lateral(h)) + inner(h) * low)
    low_n = low_n + low * (flows + inner(q) + GRAVITY_STEP * inner(h))
    new_ref[1] = low_n / (low_d + low * (weights + inner(h)))
    copy = pltpu.make_async_copy(new_ref, head_out.at[:TOP_LAYERS], sem)
    copy.start()
    roots = [closure(params(tab_ref, tops[1, :, ch].astype(jnp.int32)), tops[0, :, ch])[2] for ch in chunks(tile.shape[2])]
    root = jnp.concatenate(roots, axis=1)
    water, _ = flow(
        [tile[f] for f in range(5)], tops[0], 0.25 * root * root,
        flags(group > 0, group < groups - 1), flags(column > 0, column < columns_all - 1), height, across,
    )
    water_ref[...] = water[:height, :across]
    copy.wait()


def finish(tables, fields, tops, head, water, count):
    _, own, cols = head.shape
    height, across = water
    whole = count == 0
    rows, width, high, broad = own + SUBS, cols + LANES, height + SUBS, across + LANES
    n = len(fields)

    def body(*refs):
        tab_ref, given, known, (head_out, water_ref) = refs[0], refs[1 : 1 + n], refs[1 + n : 4 + n], refs[5 + n : 7 + n]
        rest = refs[7 + n :]
        if whole:
            strip, tile, above = given
        else:
            strip, tile, above = rest[2:5]
            assemble(*given[:3], given[3:], strip, tile, above, *rest[5:], own)
        last_kernel(tab_ref, strip, tile, above, *known, head_out, water_ref, *rest[:2])

    vmem = pl.BlockSpec(memory_space=pltpu.VMEM)
    scratch = [pltpu.VMEM((TOP_LAYERS, own, cols), jnp.float32), pltpu.SemaphoreType.DMA]
    if not whole:
        scratch += [
            pltpu.VMEM(shape, jnp.float32)
            for shape in ((5, rows, width), (5, high, broad), (2, high, broad), (2, LANES, 2 * LANES), (2 * LANES, LANES))
        ]
    return pl.pallas_call(
        body,
        out_shape=(jax.ShapeDtypeStruct(head.shape, jnp.float32), jax.ShapeDtypeStruct(water, jnp.float32)),
        in_specs=[vmem] * (n + 4) + [pl.BlockSpec(memory_space=pl.ANY)],
        out_specs=[pl.BlockSpec(memory_space=pl.ANY), vmem],
        scratch_shapes=scratch,
        input_output_aliases={n + 4: 0},
        name="surface_and_top",
    )(*near(tables, *fields, *tops), head)


def lane_rows(size):
    return -(-size // LANES)


def as_lanes(x):
    if x.shape[-1] % LANES:
        x = jnp.pad(x.reshape(-1), (0, -x.size % LANES))
    return x.reshape(-1, LANES)


def from_lanes(x, shape):
    if shape[-1] % LANES:
        size = 1
        for length in shape:
            size *= length
        x = x.reshape(-1)[:size]
    return x.reshape(shape)


def gx_trade(edges, half):
    got = shift(edges, "gx", 1)
    if lax.axis_size("gx") == 2:
        return got
    return jnp.where(half, got, shift(edges, "gx", -1))


def cyclic_rows(mid, above, below, gap):
    hole = jnp.zeros(mid.shape[:-2] + (gap, mid.shape[-1]), mid.dtype)
    return jnp.concatenate([mid, below, hole, above], axis=-2)


def block_general(pressure, soil_class, depth, elevation, roughness, rain, land_mask, channel_mask):
    ny = lax.axis_size("gy")
    _, own, cols = pressure.shape
    srows, scols = depth.shape
    convey = (1.0 + channel_mask.astype(jnp.float32)) / roughness
    surf = jnp.stack([depth, elevation, convey, LEAKANCE * land_mask.astype(jnp.float32), rain])
    tops = jnp.stack([pressure[0], soil_class[0].astype(jnp.float32)])

    def pack(s, t):
        return jnp.concatenate([as_lanes(s), as_lanes(t)], axis=0)

    def unpack(m):
        cut = lane_rows(15 * scols)
        return from_lanes(m[:cut], (5, 3, scols)), from_lanes(m[cut:], (2, 2, cols))

    s_above, t_above = unpack(shift(pack(surf[:, -3:], tops[:, -2:]), "grp", 1))
    s_below, t_below = unpack(shift(pack(surf[:, :3], tops[:, :2]), "grp", -1))
    surf_rows = cyclic_rows(surf, s_above, s_below, 2)
    tops_rows = jnp.concatenate([tops, t_below, t_above], axis=1)

    def edges(cut):
        a = surf_rows[:, :, cut(3)].transpose(0, 2, 1).reshape(15, -1)
        b = tops_rows[:, :, cut(2)].transpose(0, 2, 1).reshape(4, -1)
        return jnp.concatenate([a, jnp.pad(b, ((0, 0), (0, a.shape[1] - b.shape[1])))], axis=0)

    out = jnp.concatenate([edges(lambda n: slice(-n, None)), edges(lambda n: slice(0, n))])
    got = gx_trade(out, lax.broadcasted_iota(jnp.int32, out.shape, 0) < 19)
    mine = jnp.concatenate(
        [as_lanes(surf_rows), as_lanes(tops_rows), jnp.pad(got, ((0, 0), (0, -got.shape[1] % LANES))).reshape(-1, LANES)]
    )
    every = lax.all_gather(mine, "gy", axis=0, tiled=False)
    n1 = lane_rows(surf_rows.size)
    n2 = n1 + lane_rows(tops_rows.size)
    e_surf = jax.vmap(lambda m: from_lanes(m, (5, srows + SUBS, scols)))(every[:, :n1])
    e_surf = e_surf.transpose(1, 2, 0, 3).reshape(5, srows + SUBS, ny * scols)
    e_tops = every[:, n1:n2].reshape(ny, 2, own + 4, cols)
    e_m = every[:, n2:].reshape(ny, 2, 19, -1)
    main = e_tops[:, :, :own].transpose(1, 0, 2, 3).reshape(2, srows, cols)
    zeros = jnp.zeros((2, 4, cols), jnp.float32)
    f_tops = jnp.concatenate([main, e_tops[0, :, own : own + 2], zeros, e_tops[-1, :, own + 2 :]], axis=1)
    height = srows + SUBS
    c_left = e_m[-1, 0, :15, :height].reshape(5, 3, height).transpose(0, 2, 1)
    c_right = e_m[0, 1, :15, :height].reshape(5, 3, height).transpose(0, 2, 1)
    hole = jnp.zeros((5, height, LANES - 6), jnp.float32)
    blocks = jnp.concatenate([e_surf, c_right, hole, c_left], axis=2)

    def tops_edge(side):
        t = e_m[:, side, 15:, : own + 4].reshape(ny, 2, 2, own + 4)
        mid = t[..., :own].transpose(1, 0, 3, 2).reshape(2, srows, 2)
        low = t[0, :, :, own : own + 2].transpose(0, 2, 1)
        high = t[-1, :, :, own + 2 :].transpose(0, 2, 1)
        return jnp.concatenate([mid, low, jnp.zeros((2, 4, 2), jnp.float32), high], axis=1)

    top_blocks = jnp.concatenate(
        [f_tops, tops_edge(1), jnp.zeros((2, height, LANES - 4), jnp.float32), tops_edge(0)], axis=2
    )
    line = lax.axis_index("gy")

    def around(first, length, total, room):
        spot = jnp.arange(room)
        return (first + jnp.where(spot < length + 3, spot, spot - room)) % total

    strip = jnp.take(blocks, around(line * own, own, height, own + SUBS), axis=1)
    across = around(line * scols, scols, cols + LANES, -(-(scols + 6) // LANES) * LANES)
    return strip, jnp.take(blocks, across, axis=2), jnp.take(top_blocks, across, axis=2)


def local(
    pressure, soil_class, capacity_range, inverse_entry, shape_index, conductivity,
    depth, elevation, roughness, rain, land_mask, channel_mask,
):
    ny = lax.axis_size("gy")
    _, own, cols = pressure.shape
    srows, scols = depth.shape
    ground = (depth, elevation, roughness, rain, land_mask, channel_mask)
    classes = (capacity_range, inverse_entry, shape_index, conductivity)
    even = scols == LANES and own == SUBS
    tables, *packed = pack(pressure, soil_class, classes, ground if even else ())
    blocks, after, before, after_end, before_end = packed[-5:]
    surface = ()
    if even:
        main, strip_after, strip_before = packed[:3]
        above = shift(strip_after, "grp", 1)
        below = shift(strip_before, "grp", -1)
        surface = (main, above, below)
    rows = ("grp", "gy")
    up_end = shift(after_end, rows, 1)
    down_end = shift(before_end, rows, -1)
    sent = columns(blocks, cols, up_end, down_end, surface)
    up = shift(after, rows, 1)
    down = shift(before, rows, -1)
    span = pressure.shape[0] * (own + SUBS)
    half = jnp.where(lax.broadcasted_iota(jnp.int32, sent.shape, 1) < span, 4, 3)
    got = gx_trade(sent, lax.broadcasted_iota(jnp.int32, sent.shape, 0) < half)
    if even:
        outs = windows(main, above, below, got, sent, span, srows, own, ny)
        fields = [main, above, below, outs[0]] + [shift(outs[step], "gy", step) for step in range(1, ny)]
    else:
        fields = block_general(pressure, soil_class, *ground)
    head, *tops = soil_interior(tables, pressure, soil_class, up, down, got, sent)
    return finish(tables, fields, tops, head, (srows, scols), ny if even else 0)


def solution(mesh):
    soil = P(None, ("grp", "gy"), "gx")
    ground = P("grp", ("gx", "gy"))

    return jax.shard_map(
        local,
        mesh=mesh,
        in_specs=(soil, soil, P(), P(), P(), P()) + (ground,) * 6,
        out_specs=(soil, ground),
        check_vma=False,
    )
```

```python
import jax
import jax.numpy as jnp
from jax import lax
from jax.experimental import pallas as pl
from jax.experimental.pallas import tpu as pltpu
from jax.sharding import PartitionSpec as P


PASSES = 3
STORAGE = 0.01
GRAVITY_STEP = 0.5
SUCTION_FLOOR = 0.01
SLOPE_FLOOR = 0.1
SURFACE_STEP = 0.3
LEAKANCE = 0.5

LANES = 128
SUBS = 8
UNROLL = 12
TOP_LAYERS = 2


def shift(x, axis, step):
    size = lax.axis_size(axis)
    return lax.ppermute(x, axis, [(i, (i + step) % size) for i in range(size)])


def near(*arrays):
    return [pltpu.with_memory_space_constraint(x, pltpu.VMEM) for x in arrays]


def class_tables(refs):
    lane = lax.broadcasted_iota(jnp.int32, (1, LANES), 1)
    spread = []
    for ref in refs:
        row = jnp.ones((1, LANES), jnp.float32)
        for k in range(ref.shape[0]):
            row = jnp.where(lane == k, ref[k], row)
        spread.append(row)
    span, entry, shape, ks = spread
    pore = 1.0 - 1.0 / shape
    rows = [-entry, 1.0 / (1.0 - pore), pore, span, 2.0 * jnp.sqrt(ks)]
    return jnp.concatenate(rows + [jnp.zeros((SUBS - len(rows), LANES), jnp.float32)], axis=0)


def place():
    tile = lax.axis_index("grp") * lax.axis_size("gy") + lax.axis_index("gy")
    tiles = lax.axis_size("grp") * lax.axis_size("gy")
    column, columns = lax.axis_index("gx"), lax.axis_size("gx")
    tests = (tile > 0, tile < tiles - 1, column > 0, column < columns - 1)
    return [jnp.where(t, 1, 0) for t in tests]


def params(tab_ref, idx):
    return [
        jnp.take_along_axis(jnp.broadcast_to(tab_ref[i : i + 1, :], idx.shape), idx, axis=1, mode="promise_in_bounds")
        for i in range(5)
    ]


def closure(given, p):
    entry, expo, pore, span, scale = given
    logs = jnp.log2(jnp.maximum(entry * p, SUCTION_FLOOR))
    total = jnp.log2(1.0 + jnp.exp2(expo * logs))
    drop = pore * total
    less = expo - 1.0
    power = less * logs - drop
    ratio = jnp.exp2(power)
    content = span * jnp.exp2(-drop)
    capacity = STORAGE - (span * entry * less) * jnp.exp2(power - total)
    root = scale * jnp.exp2(-0.25 * drop) * jnp.abs(1.0 - ratio)
    return content, capacity, root


def chunks(width):
    return [slice(i, i + LANES) for i in range(0, width, LANES)]


def wide(parts):
    return [jnp.concatenate(x, axis=1) for x in zip(*parts)]


def lateral(x):
    rows, width = x.shape
    return (
        pltpu.roll(x, 1, 0)
        + pltpu.roll(x, rows - 1, 0)
        + pltpu.roll(x, 1, 1)
        + pltpu.roll(x, width - 1, 1)
    )


def soil_mask(ok, rows, width, own_rows, own_cols):
    r = lax.broadcasted_iota(jnp.int32, (rows, width), 0)
    c = lax.broadcasted_iota(jnp.int32, (rows, width), 1)
    above = jnp.where(r >= rows - 2, ok[0], 0)
    below = jnp.where((r >= own_rows) & (r < own_rows + 2), ok[1], 0)
    left = jnp.where(c >= width - 2, ok[2], 0)
    right = jnp.where((c >= own_cols) & (c < own_cols + 2), ok[3], 0)
    in_rows = jnp.where(r < own_rows, 1, above + below)
    in_cols = jnp.where(c < own_cols, 1, left + right)
    return (in_rows * in_cols).astype(jnp.float32)


def soil_rows(p_ref, c_ref, next_ref, prev_ref):
    _, own, cols = p_ref.shape
    n = cols // LANES
    for f, x in enumerate((p_ref, c_ref)):
        for r in range(2):
            last, first = x[:, own - 2 + r, :].astype(jnp.float32), x[:, r, :].astype(jnp.float32)
            for j, ch in enumerate(chunks(cols)):
                next_ref[f, r * n + j] = last[:, ch]
                prev_ref[f, r * n + j] = first[:, ch]


def soil_columns(p_ref, c_ref, box):
    layers, own, cols = p_ref.shape
    rows = box.shape[1]
    box[...] = jnp.zeros_like(box)
    out = []
    for ch in (chunks(cols)[-1], chunks(cols)[0]):
        for x in (p_ref, c_ref):
            box[:, 2 : 2 + own, :] = x[:, :, ch].astype(jnp.float32)
            turned = box[...].reshape(layers * rows, LANES).T
            out.append(turned[LANES - 2 :] if len(out) < 2 else turned[:2])
    return jnp.concatenate(out, axis=0)


def soil_kernel(
    tab_ref, p_far, c_far, up_in, down_in, got_in, sent_in, out_far, top_out, class_out, next_out,
    p_in, c_in, out_ref, tile_sem, out_sem, h_ref, q_ref, n_ref, d_ref, k_ref, h2_ref, q2_ref, n2_ref, d2_ref, given, corner, turn, near, near2, pe, ce,
):
    layers, own, cols = p_in.shape
    rows = own + SUBS
    span = layers * rows
    f32 = jnp.float32
    ok = place()

    def tile_copy(i, j):
        part = pl.ds(j * UNROLL, UNROLL)
        far, here = ((p_far, p_in), (c_far, c_in))[i]
        return pltpu.make_async_copy(far.at[part], here.at[part], tile_sem.at[i, j])

    def out_copy(j):
        part = pl.ds(j * UNROLL, UNROLL)
        return pltpu.make_async_copy(out_ref.at[part], out_far.at[part], out_sem.at[j])

    got, sent = got_in[:, :span], sent_in[:, :span]
    groups = layers // UNROLL
    for j in range(groups):
        tile_copy(0, j).start()
        tile_copy(1, j).start()
    for ref in (h_ref, q_ref, h2_ref, q2_ref):
        ref[0] = jnp.zeros((own, cols), f32)
        ref[layers + 1] = jnp.zeros((own, cols), f32)

    gap = jnp.zeros((1, span), f32)
    p = jnp.concatenate([got[0:2], sent[4:5], gap, sent[1:2], got[4:6], gap], axis=0)
    kind = jnp.concatenate([got[2:4], sent[6:7], gap, sent[3:4], got[6:8], gap], axis=0)
    sub = lax.broadcasted_iota(jnp.int32, (SUBS, span), 0)
    lane = lax.broadcasted_iota(jnp.int32, (SUBS, span), 1)
    row = lane % rows
    row_ok = jnp.where(row < 2, ok[0], jnp.where(row < own + 2, 1, jnp.where(row < own + 4, ok[1], 0)))
    col_ok = jnp.where(sub < 2, ok[2], jnp.where((sub == 2) | (sub == 4), 1, jnp.where((sub == 5) | (sub == 6), ok[3], 0)))
    mask = (row_ok * col_ok).astype(f32)
    n = cols // LANES
    corner[...] = jnp.zeros_like(corner)
    found = []
    for f in range(2):
        corner[:, 1, :] = up_in[f, 2 * n]
        corner[:, own + 2, :] = down_in[f, 2 * n]
        turned = corner[...].reshape(span, LANES).T
        found.append(jnp.concatenate([gap, turned[LANES - 1 :], gap, gap, gap, turned[:1], gap, gap], axis=0))
    p = p + found[0]
    kind = (kind + found[1]).astype(jnp.int32)
    values = [params(tab_ref, kind[:, ch]) for ch in chunks(span)]
    content, capacity, root = wide([closure(v, p[:, ch]) for v, ch in zip(values, chunks(span))])
    h, q = root * mask, root * mask * p

    def over(x):
        return jnp.where(lane < rows, 0.0, pltpu.roll(x, rows, 1))

    def under(x):
        return jnp.where(lane >= span - rows, 0.0, pltpu.roll(x, span - rows, 1))

    weights = lateral(h) + over(h) + under(h)
    flows = lateral(q) + over(q) + under(q) + GRAVITY_STEP * (over(h) - under(h))
    p1 = (capacity * p + h * flows) / (capacity + h * weights)
    root = wide([closure(v, p1[:, ch]) for v, ch in zip(values, chunks(span))])[2] * mask
    turn[...] = jnp.zeros_like(turn)
    for i, x in enumerate((h, q, root, root * p1)):
        turn[i * SUBS : (i + 1) * SUBS, :] = x
    corner[...] = turn[...].T.reshape(layers, rows, LANES)

    def first(z):
        for ch in chunks(cols):
            p = p_in[z, :, ch]
            values = params(tab_ref, c_in[z, :, ch])
            for i, v in enumerate(values):
                given[i, z, :, ch] = v
            content, capacity, root = closure(values, p)
            h_ref[z + 1, :, ch] = root
            q_ref[z + 1, :, ch] = root * p
            n_ref[z, :, ch] = capacity * p
            d_ref[z, :, ch] = capacity
            k_ref[z, :, ch] = content

    def first_group(j, carry):
        tile_copy(0, j).wait()
        tile_copy(1, j).wait()
        for i in range(UNROLL):
            first(j * UNROLL + i)
        return carry

    lax.fori_loop(0, groups, first_group, 0)

    zsub = lax.broadcasted_iota(jnp.int32, (layers, cols), 0)
    zlane = lax.broadcasted_iota(jnp.int32, (layers, LANES), 1)

    def sides(x, edge, at, lanes):
        left, right = pltpu.roll(x, 1, 1), pltpu.roll(x, cols - 1, 1)
        a = jnp.where(lanes == 0, pltpu.roll(edge, LANES - at, 1), left[:, :LANES])
        b = jnp.where(lanes == LANES - 1, pltpu.roll(edge, LANES - 1 - (at + 4), 1), right[:, cols - LANES :])
        return jnp.concatenate([a, left[:, LANES:]], axis=1) + jnp.concatenate([right[:, : cols - LANES], b], axis=1)

    for side, (halo, close, far, edge_row, valid) in enumerate(((up_in, 1, 0, 1, ok[0]), (down_in, 0, 1, own + 2, ok[1]))):
        inside = valid.astype(f32)
        ours = 0 if side == 0 else own - 1
        values, states, beyond = [], [], []
        for j in range(n):
            p = halo[0, close * n + j]
            v = params(tab_ref, halo[1, close * n + j].astype(jnp.int32))
            content, capacity, root = closure(v, p)
            root = root * inside
            values.append(v)
            states.append((p, capacity, root, root * p))
            p = halo[0, far * n + j]
            root = closure(params(tab_ref, halo[1, far * n + j].astype(jnp.int32)), p)[2] * inside
            beyond.append((root, root * p))
        p, capacity, h, q = wide(states)
        far_h, far_q = wide(beyond)
        near[side, 0] = h
        near[side, 1] = q
        edge = corner[:, edge_row, :]
        top_h = jnp.where(zsub == 0, 0.0, pltpu.roll(h, 1, 0))
        low_h = jnp.where(zsub == layers - 1, 0.0, pltpu.roll(h, layers - 1, 0))
        top_q = jnp.where(zsub == 0, 0.0, pltpu.roll(q, 1, 0))
        low_q = jnp.where(zsub == layers - 1, 0.0, pltpu.roll(q, layers - 1, 0))
        weights = far_h + h_ref[1 : layers + 1, ours, :] + sides(h, edge, 1, zlane) + top_h + low_h
        flows = far_q + q_ref[1 : layers + 1, ours, :] + sides(q, edge, 1 + SUBS, zlane) + top_q + low_q + GRAVITY_STEP * (top_h - low_h)
        p1 = (capacity * p + h * flows) / (capacity + h * weights)
        for v, ch in zip(values, chunks(cols)):
            root = closure(v, p1[:, ch])[2] * inside
            near2[side, 0, :, ch] = root
            near2[side, 1, :, ch] = root * p1[:, ch]

    tsub = lax.broadcasted_iota(jnp.int32, (own, cols), 0)
    tlane = lax.broadcasted_iota(jnp.int32, (own, LANES), 1)

    def around(z, h, q, rim, at):
        edge = corner[z, 2 : 2 + own, :]
        out = []
        for i, x in enumerate((h[z + 1], q[z + 1])):
            above = jnp.where(tsub == 0, rim[0, i, pl.ds(z, 1), :], pltpu.roll(x, 1, 0))
            below = jnp.where(tsub == own - 1, rim[1, i, pl.ds(z, 1), :], pltpu.roll(x, own - 1, 0))
            out.append(above + below + sides(x, edge, at + i * SUBS, tlane))
        weights, flows = out
        low = h[z + 2]
        return weights + low, flows + q[z + 2] - GRAVITY_STEP * low

    def second(z, carry):
        mid, top = h_ref[z + 1], h_ref[z]
        weights, flows = around(z, h_ref, q_ref, near, 1)
        flows = flows + q_ref[z] + GRAVITY_STEP * top
        p1 = (n_ref[z] + mid * flows) / (d_ref[z] + mid * (weights + top))
        for ch in chunks(cols):
            p = p1[:, ch]
            content, capacity, root = closure([given[i, z, :, ch] for i in range(5)], p)
            h2_ref[z + 1, :, ch] = root
            q2_ref[z + 1, :, ch] = root * p
            n2_ref[z, :, ch] = capacity * p - (content - k_ref[z, :, ch])
            d2_ref[z, :, ch] = capacity
        return carry

    lax.fori_loop(0, layers, second, 0, unroll=UNROLL)

    def third(z):
        mid, top = h2_ref[z + 1], h2_ref[z]
        weights, flows = around(z, h2_ref, q2_ref, near2, 1 + 2 * SUBS)
        flows = flows + q2_ref[z] + GRAVITY_STEP * top
        out_ref[z] = (n2_ref[z] + mid * flows) / (d2_ref[z] + mid * (weights + top))

    def third_group(j, carry):
        for i in range(UNROLL):
            third(j * UNROLL + i)
        out_copy(j).start()
        return carry

    lax.fori_loop(0, groups, third_group, 0)

    weights, flows = around(1, h2_ref, q2_ref, near2, 1 + 2 * SUBS)
    for i, x in enumerate((h2_ref[2], q2_ref[2], n2_ref[1], d2_ref[1], weights, flows)):
        next_out[i] = x
    for f, (src, dst, halo_at) in enumerate(((p_in, pe, 0), (c_in, ce, 2))):
        turn[...] = jnp.zeros_like(turn)
        turn[LANES - 2 :, :] = got[halo_at : halo_at + 2]
        turn[:2, :] = got[halo_at + 4 : halo_at + 6]
        block = turn[:, :LANES].T
        zlane1 = lax.broadcasted_iota(jnp.int32, (1, LANES), 1)
        for z in range(2):
            dst[z, own:, :cols] = jnp.zeros((SUBS, cols), dst.dtype)
            dst[z, :own, :cols] = src[z]
            dst[z, :, cols:] = jnp.zeros((rows, LANES), dst.dtype)
            dst[z, : own + 2, cols:] = block[z * rows + 2 : z * rows + own + 4].astype(dst.dtype)
            dst[z, rows - 2 :, cols:] = block[z * rows : z * rows + 2].astype(dst.dtype)
            for at, halo in ((own, down_in), (rows - 1, up_in)):
                ends = halo[f, 2 * n, z : z + 1, :]
                dst[z, at : at + 1, cols:] = jnp.where((zlane1 == 0) | (zlane1 == LANES - 1), ends, 0.0).astype(dst.dtype)
            for r in range(2):
                for j, ch in enumerate(chunks(cols)):
                    dst[z, own + r : own + r + 1, ch] = down_in[f, r * n + j, z : z + 1, :].astype(dst.dtype)
                    dst[z, rows - 2 + r : rows - 1 + r, ch] = up_in[f, r * n + j, z : z + 1, :].astype(dst.dtype)
    width = cols + LANES
    mask = soil_mask(ok, rows, width, own, cols)
    states = []
    for z in range(2):
        content, capacity, root = wide([closure(params(tab_ref, ce[z, :, ch]), pe[z, :, ch]) for ch in chunks(width)])
        states.append((content, capacity, root * mask))
    content, capacity, h = states[0]
    low = states[1][2]
    weights = lateral(h) + low
    flows = lateral(h * pe[0]) + low * pe[1] - GRAVITY_STEP * low
    weight = capacity + h * weights
    top_out[0] = (capacity * pe[0] + h * flows) / weight
    top_out[1] = 1.0 / weight
    top_out[2] = content
    top_out[3] = pe[0]
    top_out[4] = h
    for j in range(groups):
        out_copy(j).wait()
    class_out[...] = ce[0]


def soil_interior(tables, pressure, soil_class, up, down, got, sent):
    layers, own, cols = pressure.shape
    rows, width = own + SUBS, cols + LANES
    f32 = jnp.float32
    span = layers * rows
    tall = pltpu.VMEM((layers + 2, own, cols), f32)
    flat = pltpu.VMEM((layers, own, cols), f32)
    vmem = pl.BlockSpec(memory_space=pltpu.VMEM)
    far = pl.BlockSpec(memory_space=pl.ANY)
    return pl.pallas_call(
        soil_kernel,
        out_shape=(
            jax.ShapeDtypeStruct(pressure.shape, f32),
            pltpu.VMEM((5, rows, width), f32),
            pltpu.VMEM((rows, width), jnp.int32),
            pltpu.VMEM((6, own, cols), f32),
        ),
        in_specs=[vmem] + [far] * 2 + [vmem] * 4,
        out_specs=[far] + [vmem] * 3,
        scratch_shapes=[flat, pltpu.VMEM((layers, own, cols), jnp.int32), flat]
        + [pltpu.SemaphoreType.DMA((2, layers // UNROLL)), pltpu.SemaphoreType.DMA((layers // UNROLL,))]
        + [tall, tall, flat, flat, flat, tall, tall, flat, flat]
        + [
            pltpu.VMEM((5, layers, own, cols), f32),
            pltpu.VMEM((layers, rows, LANES), f32),
            pltpu.VMEM((LANES, span), f32),
            pltpu.VMEM((2, 2, layers, cols), f32),
            pltpu.VMEM((2, 2, layers, cols), f32),
            pltpu.VMEM((2, rows, width), f32),
            pltpu.VMEM((2, rows, width), jnp.int32),
        ],
        name="soil_interior",
    )(*near(tables), pressure, soil_class, *near(up, down, got, sent))


def surface_rows(p_ref, c_ref, depth, level, rough, rain, land, channel, main_ref, next_ref, prev_ref):
    height, _ = depth.shape
    _, own, cols = p_ref.shape
    fields = (
        depth[...],
        level[...],
        (1.0 + channel[...].astype(jnp.float32)) / rough[...],
        LEAKANCE * land[...].astype(jnp.float32),
        rain[...],
    )
    for f, x in enumerate(fields):
        main_ref[f * height : (f + 1) * height, :] = x
        next_ref[3 * f : 3 * f + 3, :] = x[height - 3 :]
        prev_ref[3 * f : 3 * f + 3, :] = x[:3]
    base = 5 * height
    for f, x in enumerate((p_ref[0], c_ref[0].astype(jnp.float32))):
        for j, ch in enumerate(chunks(cols)):
            main_ref[base : base + own, :] = x[:, ch]
            base += own
            at = EDGE_ROWS + 2 * (f * (cols // LANES) + j)
            next_ref[at : at + 2, :] = x[own - 2 :, ch]
            prev_ref[at : at + 2, :] = x[:2, ch]


EDGE_ROWS = 16


def pack(pressure, soil_class, classes, ground):
    layers, own, cols = pressure.shape
    f32 = jnp.float32
    rows = own + SUBS
    span = layers * rows
    edge = pltpu.VMEM((2, 2 * cols // LANES, layers, LANES), f32)
    scratch = [pltpu.VMEM((layers, rows, LANES), f32)]
    width, more = span, []
    if ground:
        height = ground[0].shape[0]
        strip = pltpu.VMEM((EDGE_ROWS + 4 * cols // LANES, LANES), f32)
        more = [pltpu.VMEM((5 * height + 2 * own * cols // LANES, LANES), f32), strip, strip]
        tall = LANES + 5 * (height + SUBS)
        tall += -tall % LANES
        width += tall
        scratch.append(pltpu.VMEM((tall, LANES), f32))
    out = [pltpu.VMEM((SUBS, LANES), f32), pltpu.VMEM((SUBS, width), f32), edge, edge] + more
    given = 2 + len(ground)

    def body(*refs):
        tables, rest = refs[: len(classes)], refs[len(classes) :]
        fields, outs, boxes = rest[:given], rest[given : given + len(out)], rest[given + len(out) :]
        outs[1][:, :span] = soil_columns(*fields[:2], boxes[0])
        if ground:
            surface_rows(*fields, *outs[4:])
            outs[1][:, span:] = surface_columns(outs[4], boxes[1], height, own, cols)
        soil_rows(*fields[:2], *outs[2:4])
        outs[0][...] = class_tables(tables)

    vmem = pl.BlockSpec(memory_space=pltpu.VMEM)
    smem = pl.BlockSpec(memory_space=pltpu.SMEM)
    return pl.pallas_call(
        body,
        out_shape=out,
        in_specs=[smem] * len(classes) + [vmem] * given,
        scratch_shapes=scratch,
        name="pack",
    )(*classes, pressure, soil_class, *ground)


def corners_kernel(got, *refs, layers, own, cols, height):
    n = cols // LANES
    rows = own + SUBS
    span = layers * rows
    count = len(refs) // 2 - 1
    given, outs, (turn, box) = refs[:count], refs[count : 2 * count], refs[2 * count :]
    lane = lax.broadcasted_iota(jnp.int32, (layers, LANES), 1)
    turn[...] = jnp.zeros_like(turn)
    turn[:SUBS, :] = got[...]
    turned = turn[...].T
    box[...] = turned[:span].reshape(layers, rows, LANES)
    for i, row in ((0, own + 1), (1, 2)):
        x = box[:, row, :]
        outs[i][:, : 2 * n] = given[i][...]
        for f in range(2):
            left, right = pltpu.roll(x, LANES - 2 - 2 * f, 1), pltpu.roll(x, LANES - 4 - 2 * f, 1)
            outs[i][f, 2 * n] = jnp.where(lane == LANES - 1, left, jnp.where(lane == 0, right, 0.0))
    if count == 2:
        return
    moved = pltpu.roll(turned[span:], LANES - 3, 1)
    lane = lax.broadcasted_iota(jnp.int32, (3, LANES), 1)
    tall = height + SUBS
    for i in range(2):
        out = outs[2 + i]
        base = given[2 + i].shape[0]
        out[:base, :] = given[2 + i][...]
        out[base:, :] = jnp.zeros((out.shape[0] - base, LANES), jnp.float32)
        for f in range(5):
            at = LANES + f * tall + (height - 3 if i == 0 else 0)
            out[base + 3 * f : base + 3 * f + 3, :] = jnp.where((lane < 3) | (lane >= LANES - 3), moved[at : at + 3], 0.0)
        for f in range(2):
            at = own - 2 if i == 0 else 0
            left, right = moved[2 * f * SUBS + at :][:2], moved[2 * (2 + f) * SUBS + at :][:2]
            out[base + 16 + 2 * f : base + 18 + 2 * f, :] = rim(left, right, lane[:2], 2)


CORNERS = 24


def corners(got, layers, own, cols, height, rows, strips):
    f32 = jnp.float32

    def body(*refs):
        corners_kernel(*refs, layers=layers, own=own, cols=cols, height=height)

    return pl.pallas_call(
        body,
        out_shape=[pltpu.VMEM((2, 2 * cols // LANES + 1, layers, LANES), f32)] * 2
        + [pltpu.VMEM((x.shape[0] + CORNERS, LANES), f32) for x in strips],
        scratch_shapes=[pltpu.VMEM((LANES, got.shape[1]), f32), pltpu.VMEM((layers, own + SUBS, LANES), f32)],
        name="corners",
    )(*near(got, *rows, *strips))


def surface_columns(main_ref, box, height, own, cols):
    n = cols // LANES
    tall = height + SUBS
    box[...] = jnp.zeros_like(box)
    for side, j in enumerate((n - 1, 0)):
        for f in range(2):
            at = (2 * side + f) * 2 * SUBS
            src = 5 * height + (f * n + j) * own
            box[at : at + own, :] = main_ref[src : src + own, :]
    for f in range(5):
        at = LANES + f * tall
        box[at : at + height, :] = main_ref[f * height : (f + 1) * height, :]
    turned = box[...].T
    edges = jnp.concatenate([turned[LANES - 3 :], turned[:3], jnp.zeros((2, turned.shape[1]), jnp.float32)], axis=0)
    return edges


def rim(at_end, at_start, lane, count):
    return jnp.where(lane >= LANES - count, at_end, jnp.where(lane < count, at_start, 0.0))


def ring(before, after, sub):
    return jnp.where(sub >= SUBS - 3, before, jnp.where(sub < 3, after, 0.0))


WINDOW = 136


def windows_kernel(main, above, below, got, sent, *refs, span, height, own, count):
    outs, (tall, wide_top, ends, turn, flat) = refs[:count], refs[count:]
    line = lax.axis_index("gy")
    lane = lax.broadcasted_iota(jnp.int32, (SUBS, LANES), 1)
    sub = lax.broadcasted_iota(jnp.int32, (SUBS, LANES), 0)
    tall[...] = jnp.zeros_like(tall)
    ends[...] = jnp.zeros_like(ends)
    turn[...] = jnp.zeros_like(turn)
    for f in range(5):
        tall[f, SUBS : SUBS + height] = main[f * height : (f + 1) * height, :]
        tall[f, SUBS - 3 : SUBS] = above[3 * f : 3 * f + 3, :]
        tall[f, SUBS + height : SUBS + height + 3] = below[3 * f : 3 * f + 3, :]
    turn[LANES - 3 :, :] = got[:3, span : span + LANES]
    turn[:3, :] = got[3:6, span : span + LANES]
    block = turn[...].T
    last = line == count - 1
    for f in range(2):
        before, after = block[2 * f * SUBS :], block[2 * (2 + f) * SUBS :]
        spot = above.shape[0] - CORNERS + 16 + 2 * f
        beside = rim(before[:SUBS], after[:SUBS], lane, 2)
        beyond = jnp.where(last, above[spot : spot + 2, :], below[spot : spot + 2, :])
        for j in (0, count + 1):
            wide_top[f, j] = beside
            ends[j, 2 * f : 2 * f + 2] = beyond
        for j in range(count):
            src = 5 * height + (f * count + j) * own
            wide_top[f, j + 1] = main[src : src + own, :]
            at = EDGE_ROWS + 2 * (f * count + j)
            ends[j + 1, 2 * f : 2 * f + 2] = jnp.where(last, above[at : at + 2, :], below[at : at + 2, :])
    edges = []
    for source, base in ((got, above.shape[0] - CORNERS), (sent, 0)):
        flat[...] = jnp.zeros_like(flat)
        for f in range(5):
            at = f * (height + SUBS) + height
            flat[at : at + 3, :] = below[base + 3 * f : base + 3 * f + 3, :]
            flat[at + SUBS - 3 : at + SUBS, :] = above[base + 3 * f : base + 3 * f + 3, :]
        turned = flat[...].T
        edges.append((source[:3, span + LANES :] + turned[LANES - 3 :], source[3:6, span + LANES :] + turned[:3]))
    before = jnp.where(last, edges[0][0], edges[1][0])
    after = jnp.where(line == 0, edges[0][1], edges[1][1])
    for s in range(count):
        who, out = (line + s) % count, outs[s]
        for f in range(5):
            first = pl.multiple_of(who * SUBS, SUBS)
            out[2 * f * SUBS : (2 * f + 1) * SUBS, :] = tall[f, pl.ds(first + SUBS, SUBS), :]
            out[(2 * f + 1) * SUBS : (2 * f + 2) * SUBS, :] = ring(
                tall[f, pl.ds(first, SUBS), :], tall[f, pl.ds(first + 2 * SUBS, SUBS), :], sub
            )
        for f in range(2):
            out[(10 + f) * SUBS : (11 + f) * SUBS, :] = wide_top[f, who + 1]
            out[(12 + f) * SUBS : (13 + f) * SUBS, :] = rim(wide_top[f, who], wide_top[f, who + 2], lane, 2)
        mid, side = ends[who + 1], rim(ends[who], ends[who + 2], lane, 2)
        out[14 * SUBS : 14 * SUBS + 4, :] = mid[:4]
        out[14 * SUBS + 4 : 15 * SUBS, :] = side[:4]
        for j in range(2):
            at = (15 + j) * SUBS
            out[at : at + 3, :] = before[:, j * LANES : (j + 1) * LANES]
            out[at + 3 : at + 6, :] = after[:, j * LANES : (j + 1) * LANES]
            out[at + 6 : at + SUBS, :] = jnp.zeros((2, LANES), jnp.float32)


def windows(main, above, below, got, sent, span, height, own, count):
    def body(*refs):
        windows_kernel(*refs, span=span, height=height, own=own, count=count)

    return pl.pallas_call(
        body,
        out_shape=[pltpu.VMEM((WINDOW, LANES), jnp.float32)] * count,
        scratch_shapes=[
            pltpu.VMEM((5, height + 2 * SUBS, LANES), jnp.float32),
            pltpu.VMEM((2, count + 2, own, LANES), jnp.float32),
            pltpu.VMEM((count + 2, SUBS, LANES), jnp.float32),
            pltpu.VMEM((LANES, LANES), jnp.float32),
            pltpu.VMEM((2 * LANES, LANES), jnp.float32),
        ],
        name="windows",
    )(*near(main, above, below, got, sent))


def assemble(main, above, below, sent, strip, tile, tops, turn, flat, own):
    count = len(sent)
    line = lax.axis_index("gy")
    _, _, width = strip.shape
    _, rows, _ = tile.shape
    cols, height = width - LANES, rows - SUBS
    sub = lax.broadcasted_iota(jnp.int32, (SUBS, LANES), 0)
    turn[...] = jnp.zeros_like(turn)
    tops[:, height:, :] = jnp.zeros((2, SUBS, 2 * LANES), jnp.float32)
    for f in range(5):
        tile[f, height:, :LANES] = jnp.zeros((SUBS, LANES), jnp.float32)
        tile[f, :height, :LANES] = main[f * height : (f + 1) * height, :]
        tile[f, height : height + 3, :LANES] = below[3 * f : 3 * f + 3, :]
        tile[f, rows - 3 :, :LANES] = above[3 * f : 3 * f + 3, :]
    for s in range(count):
        part = sent[s]
        who = (line - s) % count
        at = pl.multiple_of(who * LANES, LANES)
        first = pl.multiple_of(who * own, own)
        for f in range(5):
            strip[f, :, pl.ds(at, LANES)] = part[2 * f * SUBS : (2 * f + 2) * SUBS, :]
        for f in range(2):
            tops[f, pl.ds(first, own), :LANES] = part[(10 + f) * SUBS : (11 + f) * SUBS, :]
            tops[f, pl.ds(first, own), LANES:] = part[(12 + f) * SUBS : (13 + f) * SUBS, :]

        @pl.when(who == 0)
        def _(part=part):
            for f in range(2):
                tops[f, height : height + 2, :LANES] = part[14 * SUBS + 2 * f : 14 * SUBS + 2 * f + 2, :]
                tops[f, height : height + 2, LANES:] = part[14 * SUBS + 4 + 2 * f : 14 * SUBS + 6 + 2 * f, :]
            for j in range(2):
                turn[0, :3, j * LANES : (j + 1) * LANES] = part[(15 + j) * SUBS + 3 : (15 + j) * SUBS + 6, :]

        @pl.when(who == count - 1)
        def _(part=part):
            for f in range(2):
                tops[f, rows - 2 :, :LANES] = part[14 * SUBS + 2 * f : 14 * SUBS + 2 * f + 2, :]
                tops[f, rows - 2 :, LANES:] = part[14 * SUBS + 4 + 2 * f : 14 * SUBS + 6 + 2 * f, :]
            for j in range(2):
                turn[0, LANES - 3 :, j * LANES : (j + 1) * LANES] = part[(15 + j) * SUBS : (15 + j) * SUBS + 3, :]

    for j in range(2):
        cut = slice(j * LANES, (j + 1) * LANES)
        turn[1, LANES - 3 :, cut] = sent[1 % count][(15 + j) * SUBS : (15 + j) * SUBS + 3, :]
        turn[1, :3, cut] = sent[-1][(15 + j) * SUBS + 3 : (15 + j) * SUBS + 6, :]
    beside = turn[1].T
    flat[...] = turn[0].T
    first = pl.multiple_of(line * own, SUBS)
    before = pl.multiple_of(jnp.where(line > 0, line * own - SUBS, height), SUBS)
    for f in range(5):
        tile[f, :, LANES:] = beside[f * rows : (f + 1) * rows]
        strip[f, :own, cols:] = flat[pl.ds(first + f * rows, SUBS), :]
        strip[f, own:, cols:] = ring(flat[pl.ds(before + f * rows, SUBS), :], flat[pl.ds(first + f * rows + SUBS, SUBS), :], sub)


def flow(fields, top, conduct, row_flags, col_flags, own_rows, own_cols):
    water, level, convey, land, rain = fields
    rows, width = water.shape
    r = lax.broadcasted_iota(jnp.int32, (rows, width), 0)
    c = lax.broadcasted_iota(jnp.int32, (rows, width), 1)
    row_ok = jnp.where(r < own_rows, 1, jnp.where(r >= rows - 3, row_flags[0], jnp.where(r < own_rows + 3, row_flags[1], 0)))
    col_ok = jnp.where(c < own_cols, 1, jnp.where(c >= width - 3, col_flags[0], jnp.where(c < own_cols + 3, col_flags[1], 0)))
    root = jnp.sqrt(convey) * (row_ok * col_ok).astype(jnp.float32)
    leak = land * conduct
    ahead = [lambda x: pltpu.roll(x, rows - 1, 0), lambda x: pltpu.roll(x, width - 1, 1)]
    gates = [root * f(root) for f in ahead]
    exchange = jnp.zeros_like(water)
    for _ in range(PASSES):
        surface = level + water
        power = jnp.where(water > 0.0, jnp.exp2((5.0 / 3.0) * jnp.log2(jnp.maximum(water, 1e-30))), 0.0)
        outflow = jnp.zeros_like(water)
        for axis in range(2):
            slope = surface - ahead[axis](surface)
            carried = jnp.where(slope >= 0.0, power, ahead[axis](power))
            flux = gates[axis] * carried * slope * lax.rsqrt(jnp.maximum(jnp.abs(slope), SLOPE_FLOOR))
            outflow = outflow + flux - pltpu.roll(flux, 1, axis)
        rate = leak * (water - top)
        exchange = exchange + SURFACE_STEP * rate
        water = jnp.maximum(water + SURFACE_STEP * (rain - rate - outflow), 0.0)
    return water, exchange


def last_kernel(tab_ref, strip, tile, tops, top_ref, class_ref, next_ref, head_out, water_ref, new_ref, sem):
    own = new_ref.shape[1]
    _, rows, width = strip.shape
    cols = width - LANES
    height, across = water_ref.shape
    ok = place()
    group, groups = lax.axis_index("grp"), lax.axis_size("grp")
    column = lax.axis_index("gx") * lax.axis_size("gy") + lax.axis_index("gy")
    columns_all = lax.axis_size("gx") * lax.axis_size("gy")

    def flags(*tests):
        return [jnp.where(t, 1, 0) for t in tests]

    root = top_ref[4]
    _, gain = flow([strip[f] for f in range(5)], top_ref[3], 0.25 * root * root, ok[:2], ok[2:], own, cols)
    mask = soil_mask(ok, rows, width, own, cols)
    p = top_ref[0] + gain * top_ref[1]
    content, capacity, root = wide([closure(params(tab_ref, class_ref[:, ch]), p[:, ch]) for ch in chunks(width)])
    h = root * mask
    q = h * p
    low, low_q, low_n, low_d, weights, flows = (next_ref[i] for i in range(6))

    def inner(x):
        return x[:own, :cols]

    top_n = inner(capacity * p - (content - top_ref[2]) + gain + h * lateral(q)) + inner(h) * (low_q - GRAVITY_STEP * low)
    new_ref[0] = top_n / (inner(capacity + h * lateral(h)) + inner(h) * low)
    low_n = low_n + low * (flows + inner(q) + GRAVITY_STEP * inner(h))
    new_ref[1] = low_n / (low_d + low * (weights + inner(h)))
    copy = pltpu.make_async_copy(new_ref, head_out.at[:TOP_LAYERS], sem)
    copy.start()
    roots = [closure(params(tab_ref, tops[1, :, ch].astype(jnp.int32)), tops[0, :, ch])[2] for ch in chunks(tile.shape[2])]
    root = jnp.concatenate(roots, axis=1)
    water, _ = flow(
        [tile[f] for f in range(5)], tops[0], 0.25 * root * root,
        flags(group > 0, group < groups - 1), flags(column > 0, column < columns_all - 1), height, across,
    )
    water_ref[...] = water[:height, :across]
    copy.wait()


def finish(tables, fields, tops, head, water, count):
    _, own, cols = head.shape
    height, across = water
    whole = count == 0
    rows, width, high, broad = own + SUBS, cols + LANES, height + SUBS, across + LANES
    n = len(fields)

    def body(*refs):
        tab_ref, given, known, (head_out, water_ref) = refs[0], refs[1 : 1 + n], refs[1 + n : 4 + n], refs[5 + n : 7 + n]
        rest = refs[7 + n :]
        if whole:
            strip, tile, above = given
        else:
            strip, tile, above = rest[2:5]
            assemble(*given[:3], given[3:], strip, tile, above, *rest[5:], own)
        last_kernel(tab_ref, strip, tile, above, *known, head_out, water_ref, *rest[:2])

    vmem = pl.BlockSpec(memory_space=pltpu.VMEM)
    scratch = [pltpu.VMEM((TOP_LAYERS, own, cols), jnp.float32), pltpu.SemaphoreType.DMA]
    if not whole:
        scratch += [
            pltpu.VMEM(shape, jnp.float32)
            for shape in ((5, rows, width), (5, high, broad), (2, high, broad), (2, LANES, 2 * LANES), (2 * LANES, LANES))
        ]
    return pl.pallas_call(
        body,
        out_shape=(jax.ShapeDtypeStruct(head.shape, jnp.float32), jax.ShapeDtypeStruct(water, jnp.float32)),
        in_specs=[vmem] * (n + 4) + [pl.BlockSpec(memory_space=pl.ANY)],
        out_specs=[pl.BlockSpec(memory_space=pl.ANY), vmem],
        scratch_shapes=scratch,
        input_output_aliases={n + 4: 0},
        name="surface_and_top",
    )(*near(tables, *fields, *tops), head)


def lane_rows(size):
    return -(-size // LANES)


def as_lanes(x):
    if x.shape[-1] % LANES:
        x = jnp.pad(x.reshape(-1), (0, -x.size % LANES))
    return x.reshape(-1, LANES)


def from_lanes(x, shape):
    if shape[-1] % LANES:
        size = 1
        for length in shape:
            size *= length
        x = x.reshape(-1)[:size]
    return x.reshape(shape)


def gx_trade(edges, half):
    got = shift(edges, "gx", 1)
    if lax.axis_size("gx") == 2:
        return got
    return jnp.where(half, got, shift(edges, "gx", -1))


def cyclic_rows(mid, above, below, gap):
    hole = jnp.zeros(mid.shape[:-2] + (gap, mid.shape[-1]), mid.dtype)
    return jnp.concatenate([mid, below, hole, above], axis=-2)


def block_general(pressure, soil_class, depth, elevation, roughness, rain, land_mask, channel_mask):
    ny = lax.axis_size("gy")
    _, own, cols = pressure.shape
    srows, scols = depth.shape
    convey = (1.0 + channel_mask.astype(jnp.float32)) / roughness
    surf = jnp.stack([depth, elevation, convey, LEAKANCE * land_mask.astype(jnp.float32), rain])
    tops = jnp.stack([pressure[0], soil_class[0].astype(jnp.float32)])

    def pack(s, t):
        return jnp.concatenate([as_lanes(s), as_lanes(t)], axis=0)

    def unpack(m):
        cut = lane_rows(15 * scols)
        return from_lanes(m[:cut], (5, 3, scols)), from_lanes(m[cut:], (2, 2, cols))

    s_above, t_above = unpack(shift(pack(surf[:, -3:], tops[:, -2:]), "grp", 1))
    s_below, t_below = unpack(shift(pack(surf[:, :3], tops[:, :2]), "grp", -1))
    surf_rows = cyclic_rows(surf, s_above, s_below, 2)
    tops_rows = jnp.concatenate([tops, t_below, t_above], axis=1)

    def edges(cut):
        a = surf_rows[:, :, cut(3)].transpose(0, 2, 1).reshape(15, -1)
        b = tops_rows[:, :, cut(2)].transpose(0, 2, 1).reshape(4, -1)
        return jnp.concatenate([a, jnp.pad(b, ((0, 0), (0, a.shape[1] - b.shape[1])))], axis=0)

    out = jnp.concatenate([edges(lambda n: slice(-n, None)), edges(lambda n: slice(0, n))])
    got = gx_trade(out, lax.broadcasted_iota(jnp.int32, out.shape, 0) < 19)
    mine = jnp.concatenate(
        [as_lanes(surf_rows), as_lanes(tops_rows), jnp.pad(got, ((0, 0), (0, -got.shape[1] % LANES))).reshape(-1, LANES)]
    )
    every = lax.all_gather(mine, "gy", axis=0, tiled=False)
    n1 = lane_rows(surf_rows.size)
    n2 = n1 + lane_rows(tops_rows.size)
    e_surf = jax.vmap(lambda m: from_lanes(m, (5, srows + SUBS, scols)))(every[:, :n1])
    e_surf = e_surf.transpose(1, 2, 0, 3).reshape(5, srows + SUBS, ny * scols)
    e_tops = every[:, n1:n2].reshape(ny, 2, own + 4, cols)
    e_m = every[:, n2:].reshape(ny, 2, 19, -1)
    main = e_tops[:, :, :own].transpose(1, 0, 2, 3).reshape(2, srows, cols)
    zeros = jnp.zeros((2, 4, cols), jnp.float32)
    f_tops = jnp.concatenate([main, e_tops[0, :, own : own + 2], zeros, e_tops[-1, :, own + 2 :]], axis=1)
    height = srows + SUBS
    c_left = e_m[-1, 0, :15, :height].reshape(5, 3, height).transpose(0, 2, 1)
    c_right = e_m[0, 1, :15, :height].reshape(5, 3, height).transpose(0, 2, 1)
    hole = jnp.zeros((5, height, LANES - 6), jnp.float32)
    blocks = jnp.concatenate([e_surf, c_right, hole, c_left], axis=2)

    def tops_edge(side):
        t = e_m[:, side, 15:, : own + 4].reshape(ny, 2, 2, own + 4)
        mid = t[..., :own].transpose(1, 0, 3, 2).reshape(2, srows, 2)
        low = t[0, :, :, own : own + 2].transpose(0, 2, 1)
        high = t[-1, :, :, own + 2 :].transpose(0, 2, 1)
        return jnp.concatenate([mid, low, jnp.zeros((2, 4, 2), jnp.float32), high], axis=1)

    top_blocks = jnp.concatenate(
        [f_tops, tops_edge(1), jnp.zeros((2, height, LANES - 4), jnp.float32), tops_edge(0)], axis=2
    )
    line = lax.axis_index("gy")

    def around(first, length, total, room):
        spot = jnp.arange(room)
        return (first + jnp.where(spot < length + 3, spot, spot - room)) % total

    strip = jnp.take(blocks, around(line * own, own, height, own + SUBS), axis=1)
    across = around(line * scols, scols, cols + LANES, -(-(scols + 6) // LANES) * LANES)
    return strip, jnp.take(blocks, across, axis=2), jnp.take(top_blocks, across, axis=2)


def local(
    pressure, soil_class, capacity_range, inverse_entry, shape_index, conductivity,
    depth, elevation, roughness, rain, land_mask, channel_mask,
):
    ny = lax.axis_size("gy")
    _, own, cols = pressure.shape
    srows, scols = depth.shape
    ground = (depth, elevation, roughness, rain, land_mask, channel_mask)
    classes = (capacity_range, inverse_entry, shape_index, conductivity)
    even = scols == LANES and own == SUBS
    tables, sent, *packed = pack(pressure, soil_class, classes, ground if even else ())
    span = pressure.shape[0] * (own + SUBS)
    half = jnp.where(lax.broadcasted_iota(jnp.int32, sent.shape, 1) < span, 4, 3)
    got = gx_trade(sent, lax.broadcasted_iota(jnp.int32, sent.shape, 0) < half)
    after, before, *strips = corners(got, pressure.shape[0], own, cols, srows, packed[:2], packed[3:])
    rows = ("grp", "gy")
    up = shift(after, rows, 1)
    down = shift(before, rows, -1)
    if even:
        above = shift(strips[0], "grp", 1)
        below = shift(strips[1], "grp", -1)
        main = packed[2]
        outs = windows(main, above, below, got, sent, span, srows, own, ny)
        fields = [main, above, below, outs[0]] + [shift(outs[step], "gy", step) for step in range(1, ny)]
    else:
        fields = block_general(pressure, soil_class, *ground)
    head, *tops = soil_interior(tables, pressure, soil_class, up, down, got, sent)
    return finish(tables, fields, tops, head, (srows, scols), ny if even else 0)


def solution(mesh):
    soil = P(None, ("grp", "gy"), "gx")
    ground = P("grp", ("gx", "gy"))

    return jax.shard_map(
        local,
        mesh=mesh,
        in_specs=(soil, soil, P(), P(), P(), P()) + (ground,) * 6,
        out_specs=(soil, ground),
        check_vma=False,
    )
```

```python
import jax
import jax.numpy as jnp
from jax import lax
from jax.experimental import pallas as pl
from jax.experimental.pallas import tpu as pltpu
from jax.sharding import PartitionSpec as P


PASSES = 3
STORAGE = 0.01
GRAVITY_STEP = 0.5
SUCTION_FLOOR = 0.01
SLOPE_FLOOR = 0.1
SURFACE_STEP = 0.3
LEAKANCE = 0.5

LANES = 128
SUBS = 8
UNROLL = 24
TOP_LAYERS = 2


def shift(x, axis, step):
    size = lax.axis_size(axis)
    return lax.ppermute(x, axis, [(i, (i + step) % size) for i in range(size)])


def near(*arrays):
    return [pltpu.with_memory_space_constraint(x, pltpu.VMEM) for x in arrays]


def class_tables(refs):
    lane = lax.broadcasted_iota(jnp.int32, (1, LANES), 1)
    spread = []
    for ref in refs:
        row = jnp.ones((1, LANES), jnp.float32)
        for k in range(ref.shape[0]):
            row = jnp.where(lane == k, ref[k], row)
        spread.append(row)
    span, entry, shape, ks = spread
    pore = 1.0 - 1.0 / shape
    rows = [-entry, 1.0 / (1.0 - pore), pore, span, 2.0 * jnp.sqrt(ks)]
    return jnp.concatenate(rows + [jnp.zeros((SUBS - len(rows), LANES), jnp.float32)], axis=0)


def place():
    tile = lax.axis_index("grp") * lax.axis_size("gy") + lax.axis_index("gy")
    tiles = lax.axis_size("grp") * lax.axis_size("gy")
    column, columns = lax.axis_index("gx"), lax.axis_size("gx")
    tests = (tile > 0, tile < tiles - 1, column > 0, column < columns - 1)
    return [jnp.where(t, 1, 0) for t in tests]


def params(tab_ref, idx):
    return [
        jnp.take_along_axis(jnp.broadcast_to(tab_ref[i : i + 1, :], idx.shape), idx, axis=1, mode="promise_in_bounds")
        for i in range(5)
    ]


def closure(given, p):
    entry, expo, pore, span, scale = given
    logs = jnp.log2(jnp.maximum(entry * p, SUCTION_FLOOR))
    total = jnp.log2(1.0 + jnp.exp2(expo * logs))
    drop = pore * total
    less = expo - 1.0
    power = less * logs - drop
    ratio = jnp.exp2(power)
    content = span * jnp.exp2(-drop)
    capacity = STORAGE - (span * entry * less) * jnp.exp2(power - total)
    root = scale * jnp.exp2(-0.25 * drop) * jnp.abs(1.0 - ratio)
    return content, capacity, root


def chunks(width):
    return [slice(i, i + LANES) for i in range(0, width, LANES)]


def wide(parts):
    return [jnp.concatenate(x, axis=1) for x in zip(*parts)]


def lateral(x):
    rows, width = x.shape
    return (
        pltpu.roll(x, 1, 0)
        + pltpu.roll(x, rows - 1, 0)
        + pltpu.roll(x, 1, 1)
        + pltpu.roll(x, width - 1, 1)
    )


def soil_mask(ok, rows, width, own_rows, own_cols):
    r = lax.broadcasted_iota(jnp.int32, (rows, width), 0)
    c = lax.broadcasted_iota(jnp.int32, (rows, width), 1)
    above = jnp.where(r >= rows - 2, ok[0], 0)
    below = jnp.where((r >= own_rows) & (r < own_rows + 2), ok[1], 0)
    left = jnp.where(c >= width - 2, ok[2], 0)
    right = jnp.where((c >= own_cols) & (c < own_cols + 2), ok[3], 0)
    in_rows = jnp.where(r < own_rows, 1, above + below)
    in_cols = jnp.where(c < own_cols, 1, left + right)
    return (in_rows * in_cols).astype(jnp.float32)


def soil_rows(p_ref, c_ref, next_ref, prev_ref):
    _, own, cols = p_ref.shape
    n = cols // LANES
    for f, x in enumerate((p_ref, c_ref)):
        for r in range(2):
            last, first = x[:, own - 2 + r, :].astype(jnp.float32), x[:, r, :].astype(jnp.float32)
            for j, ch in enumerate(chunks(cols)):
                next_ref[(2 * f + r) * n + j] = last[:, ch]
                prev_ref[(2 * f + r) * n + j] = first[:, ch]


def soil_columns(p_ref, c_ref, box):
    layers, own, cols = p_ref.shape
    rows = box.shape[1]
    box[...] = jnp.zeros_like(box)
    out = []
    for ch in (chunks(cols)[-1], chunks(cols)[0]):
        for x in (p_ref, c_ref):
            box[:, 2 : 2 + own, :] = x[:, :, ch].astype(jnp.float32)
            turned = box[...].reshape(layers * rows, LANES).T
            out.append(turned[LANES - 2 :] if len(out) < 2 else turned[:2])
    return jnp.concatenate(out, axis=0)


def soil_kernel(
    tab_ref, p_far, c_far, up_in, down_in, got_in, sent_in, out_far, top_out, class_out, next_out,
    p_in, c_in, out_ref, tile_sem, out_sem, h_ref, q_ref, n_ref, d_ref, k_ref, h2_ref, q2_ref, n2_ref, d2_ref, given, corner, turn, near, near2, pe, ce,
):
    layers, own, cols = p_in.shape
    rows = own + SUBS
    span = layers * rows
    f32 = jnp.float32
    ok = place()

    def tile_copy(i, j):
        part = pl.ds(j * UNROLL, UNROLL)
        far, here = ((p_far, p_in), (c_far, c_in))[i]
        return pltpu.make_async_copy(far.at[part], here.at[part], tile_sem.at[i, j])

    def out_copy(j):
        part = pl.ds(j * UNROLL, UNROLL)
        return pltpu.make_async_copy(out_ref.at[part], out_far.at[part], out_sem.at[j])

    got, sent = got_in[:, :span], sent_in[:, :span]
    groups = layers // UNROLL
    for j in range(groups):
        tile_copy(0, j).start()
        tile_copy(1, j).start()
    for ref in (h_ref, q_ref, h2_ref, q2_ref):
        ref[0] = jnp.zeros((own, cols), f32)
        ref[layers + 1] = jnp.zeros((own, cols), f32)

    gap = jnp.zeros((1, span), f32)
    p = jnp.concatenate([got[0:2], sent[4:5], gap, sent[1:2], got[4:6], gap], axis=0)
    kind = jnp.concatenate([got[2:4], sent[6:7], gap, sent[3:4], got[6:8], gap], axis=0)
    sub = lax.broadcasted_iota(jnp.int32, (SUBS, span), 0)
    lane = lax.broadcasted_iota(jnp.int32, (SUBS, span), 1)
    row = lane % rows
    row_ok = jnp.where(row < 2, ok[0], jnp.where(row < own + 2, 1, jnp.where(row < own + 4, ok[1], 0)))
    col_ok = jnp.where(sub < 2, ok[2], jnp.where((sub == 2) | (sub == 4), 1, jnp.where((sub == 5) | (sub == 6), ok[3], 0)))
    mask = (row_ok * col_ok).astype(f32)
    n = cols // LANES
    corner[...] = jnp.zeros_like(corner)
    corner[:, 1, :] = up_in[4 * n]
    corner[:, own + 2, :] = down_in[4 * n]
    turned = corner[...].reshape(span, LANES).T
    found = [
        jnp.concatenate([gap, turned[LANES - 1 - f : LANES - f], gap, gap, gap, turned[f : f + 1], gap, gap], axis=0) for f in range(2)
    ]
    p = p + found[0]
    kind = (kind + found[1]).astype(jnp.int32)
    values = [params(tab_ref, kind[:, ch]) for ch in chunks(span)]
    content, capacity, root = wide([closure(v, p[:, ch]) for v, ch in zip(values, chunks(span))])
    h, q = root * mask, root * mask * p

    def over(x):
        return jnp.where(lane < rows, 0.0, pltpu.roll(x, rows, 1))

    def under(x):
        return jnp.where(lane >= span - rows, 0.0, pltpu.roll(x, span - rows, 1))

    weights = lateral(h) + over(h) + under(h)
    flows = lateral(q) + over(q) + under(q) + GRAVITY_STEP * (over(h) - under(h))
    p1 = (capacity * p + h * flows) / (capacity + h * weights)
    root = wide([closure(v, p1[:, ch]) for v, ch in zip(values, chunks(span))])[2] * mask
    turn[...] = jnp.zeros_like(turn)
    for i, x in enumerate((h, q, root, root * p1)):
        turn[i * SUBS : (i + 1) * SUBS, :] = x
    corner[...] = turn[...].T.reshape(layers, rows, LANES)

    def first(z):
        for ch in chunks(cols):
            p = p_in[z, :, ch]
            values = params(tab_ref, c_in[z, :, ch])
            for i, v in enumerate(values):
                given[i, z, :, ch] = v
            content, capacity, root = closure(values, p)
            h_ref[z + 1, :, ch] = root
            q_ref[z + 1, :, ch] = root * p
            n_ref[z, :, ch] = capacity * p
            d_ref[z, :, ch] = capacity
            k_ref[z, :, ch] = content

    def first_group(j, carry):
        tile_copy(0, j).wait()
        tile_copy(1, j).wait()
        for i in range(UNROLL):
            first(j * UNROLL + i)
        return carry

    lax.fori_loop(0, groups, first_group, 0)

    zsub = lax.broadcasted_iota(jnp.int32, (layers, cols), 0)
    zlane = lax.broadcasted_iota(jnp.int32, (layers, LANES), 1)

    def sides(x, edge, at, lanes):
        left, right = pltpu.roll(x, 1, 1), pltpu.roll(x, cols - 1, 1)
        a = jnp.where(lanes == 0, pltpu.roll(edge, LANES - at, 1), left[:, :LANES])
        b = jnp.where(lanes == LANES - 1, pltpu.roll(edge, LANES - 1 - (at + 4), 1), right[:, cols - LANES :])
        return jnp.concatenate([a, left[:, LANES:]], axis=1) + jnp.concatenate([right[:, : cols - LANES], b], axis=1)

    for side, (halo, close, far, edge_row, valid) in enumerate(((up_in, 1, 0, 1, ok[0]), (down_in, 0, 1, own + 2, ok[1]))):
        inside = valid.astype(f32)
        ours = 0 if side == 0 else own - 1
        values, states, beyond = [], [], []
        for j in range(n):
            p = halo[close * n + j]
            v = params(tab_ref, halo[(2 + close) * n + j].astype(jnp.int32))
            content, capacity, root = closure(v, p)
            root = root * inside
            values.append(v)
            states.append((p, capacity, root, root * p))
            p = halo[far * n + j]
            root = closure(params(tab_ref, halo[(2 + far) * n + j].astype(jnp.int32)), p)[2] * inside
            beyond.append((root, root * p))
        p, capacity, h, q = wide(states)
        far_h, far_q = wide(beyond)
        near[side, 0] = h
        near[side, 1] = q
        edge = corner[:, edge_row, :]
        top_h = jnp.where(zsub == 0, 0.0, pltpu.roll(h, 1, 0))
        low_h = jnp.where(zsub == layers - 1, 0.0, pltpu.roll(h, layers - 1, 0))
        top_q = jnp.where(zsub == 0, 0.0, pltpu.roll(q, 1, 0))
        low_q = jnp.where(zsub == layers - 1, 0.0, pltpu.roll(q, layers - 1, 0))
        weights = far_h + h_ref[1 : layers + 1, ours, :] + sides(h, edge, 1, zlane) + top_h + low_h
        flows = far_q + q_ref[1 : layers + 1, ours, :] + sides(q, edge, 1 + SUBS, zlane) + top_q + low_q + GRAVITY_STEP * (top_h - low_h)
        p1 = (capacity * p + h * flows) / (capacity + h * weights)
        for v, ch in zip(values, chunks(cols)):
            root = closure(v, p1[:, ch])[2] * inside
            near2[side, 0, :, ch] = root
            near2[side, 1, :, ch] = root * p1[:, ch]

    tsub = lax.broadcasted_iota(jnp.int32, (own, cols), 0)
    tlane = lax.broadcasted_iota(jnp.int32, (own, LANES), 1)

    def around(z, h, q, rim, at):
        edge = corner[z, 2 : 2 + own, :]
        out = []
        for i, x in enumerate((h[z + 1], q[z + 1])):
            above = jnp.where(tsub == 0, rim[0, i, pl.ds(z, 1), :], pltpu.roll(x, 1, 0))
            below = jnp.where(tsub == own - 1, rim[1, i, pl.ds(z, 1), :], pltpu.roll(x, own - 1, 0))
            out.append(above + below + sides(x, edge, at + i * SUBS, tlane))
        weights, flows = out
        low = h[z + 2]
        return weights + low, flows + q[z + 2] - GRAVITY_STEP * low

    def second(z, carry):
        mid, top = h_ref[z + 1], h_ref[z]
        weights, flows = around(z, h_ref, q_ref, near, 1)
        flows = flows + q_ref[z] + GRAVITY_STEP * top
        p1 = (n_ref[z] + mid * flows) / (d_ref[z] + mid * (weights + top))
        for ch in chunks(cols):
            p = p1[:, ch]
            content, capacity, root = closure([given[i, z, :, ch] for i in range(5)], p)
            h2_ref[z + 1, :, ch] = root
            q2_ref[z + 1, :, ch] = root * p
            n2_ref[z, :, ch] = capacity * p - (content - k_ref[z, :, ch])
            d2_ref[z, :, ch] = capacity
        return carry

    lax.fori_loop(0, layers, second, 0, unroll=UNROLL)

    def third(z):
        mid, top = h2_ref[z + 1], h2_ref[z]
        weights, flows = around(z, h2_ref, q2_ref, near2, 1 + 2 * SUBS)
        flows = flows + q2_ref[z] + GRAVITY_STEP * top
        out_ref[z] = (n2_ref[z] + mid * flows) / (d2_ref[z] + mid * (weights + top))

    def third_group(j, carry):
        for i in range(UNROLL):
            third(j * UNROLL + i)
        out_copy(j).start()
        return carry

    lax.fori_loop(0, groups, third_group, 0)

    weights, flows = around(1, h2_ref, q2_ref, near2, 1 + 2 * SUBS)
    for i, x in enumerate((h2_ref[2], q2_ref[2], n2_ref[1], d2_ref[1], weights, flows)):
        next_out[i] = x
    for f, (src, dst, halo_at) in enumerate(((p_in, pe, 0), (c_in, ce, 2))):
        turn[...] = jnp.zeros_like(turn)
        turn[LANES - 2 :, :] = got[halo_at : halo_at + 2]
        turn[:2, :] = got[halo_at + 4 : halo_at + 6]
        block = turn[:, :LANES].T
        zlane1 = lax.broadcasted_iota(jnp.int32, (1, LANES), 1)
        for z in range(2):
            dst[z, own:, :cols] = jnp.zeros((SUBS, cols), dst.dtype)
            dst[z, :own, :cols] = src[z]
            dst[z, :, cols:] = jnp.zeros((rows, LANES), dst.dtype)
            dst[z, : own + 2, cols:] = block[z * rows + 2 : z * rows + own + 4].astype(dst.dtype)
            dst[z, rows - 2 :, cols:] = block[z * rows : z * rows + 2].astype(dst.dtype)
            for at, halo in ((own, down_in), (rows - 1, up_in)):
                ends = halo[4 * n, z : z + 1, :]
                start, stop = pltpu.roll(ends, LANES - f, 1) if f else ends, pltpu.roll(ends, f, 1) if f else ends
                dst[z, at : at + 1, cols:] = jnp.where(zlane1 == 0, start, jnp.where(zlane1 == LANES - 1, stop, 0.0)).astype(dst.dtype)
            for r in range(2):
                for j, ch in enumerate(chunks(cols)):
                    dst[z, own + r : own + r + 1, ch] = down_in[(2 * f + r) * n + j, z : z + 1, :].astype(dst.dtype)
                    dst[z, rows - 2 + r : rows - 1 + r, ch] = up_in[(2 * f + r) * n + j, z : z + 1, :].astype(dst.dtype)
    width = cols + LANES
    mask = soil_mask(ok, rows, width, own, cols)
    states = []
    for z in range(2):
        content, capacity, root = wide([closure(params(tab_ref, ce[z, :, ch]), pe[z, :, ch]) for ch in chunks(width)])
        states.append((content, capacity, root * mask))
    content, capacity, h = states[0]
    low = states[1][2]
    weights = lateral(h) + low
    flows = lateral(h * pe[0]) + low * pe[1] - GRAVITY_STEP * low
    weight = capacity + h * weights
    top_out[0] = (capacity * pe[0] + h * flows) / weight
    top_out[1] = 1.0 / weight
    top_out[2] = content
    top_out[3] = pe[0]
    top_out[4] = h
    for j in range(groups):
        out_copy(j).wait()
    class_out[...] = ce[0]


def soil_interior(tables, pressure, soil_class, up, down, got, sent):
    layers, own, cols = pressure.shape
    rows, width = own + SUBS, cols + LANES
    f32 = jnp.float32
    span = layers * rows
    tall = pltpu.VMEM((layers + 2, own, cols), f32)
    flat = pltpu.VMEM((layers, own, cols), f32)
    vmem = pl.BlockSpec(memory_space=pltpu.VMEM)
    far = pl.BlockSpec(memory_space=pl.ANY)
    return pl.pallas_call(
        soil_kernel,
        out_shape=(
            jax.ShapeDtypeStruct(pressure.shape, f32),
            pltpu.VMEM((5, rows, width), f32),
            pltpu.VMEM((rows, width), jnp.int32),
            pltpu.VMEM((6, own, cols), f32),
        ),
        in_specs=[vmem] + [far] * 2 + [vmem] * 4,
        out_specs=[far] + [vmem] * 3,
        scratch_shapes=[flat, pltpu.VMEM((layers, own, cols), jnp.int32), flat]
        + [pltpu.SemaphoreType.DMA((2, layers // UNROLL)), pltpu.SemaphoreType.DMA((layers // UNROLL,))]
        + [tall, tall, flat, flat, flat, tall, tall, flat, flat]
        + [
            pltpu.VMEM((5, layers, own, cols), f32),
            pltpu.VMEM((layers, rows, LANES), f32),
            pltpu.VMEM((LANES, span), f32),
            pltpu.VMEM((2, 2, layers, cols), f32),
            pltpu.VMEM((2, 2, layers, cols), f32),
            pltpu.VMEM((2, rows, width), f32),
            pltpu.VMEM((2, rows, width), jnp.int32),
        ],
        name="soil_interior",
    )(*near(tables), pressure, soil_class, *near(up, down, got, sent))


def surface_rows(p_ref, c_ref, depth, level, rough, rain, land, channel, main_ref, next_ref, prev_ref):
    height, _ = depth.shape
    _, own, cols = p_ref.shape
    fields = (
        depth[...],
        level[...],
        (1.0 + channel[...].astype(jnp.float32)) / rough[...],
        LEAKANCE * land[...].astype(jnp.float32),
        rain[...],
    )
    for f, x in enumerate(fields):
        main_ref[f * height : (f + 1) * height, :] = x
        next_ref[3 * f : 3 * f + 3, :] = x[height - 3 :]
        prev_ref[3 * f : 3 * f + 3, :] = x[:3]
    base = 5 * height
    for f, x in enumerate((p_ref[0], c_ref[0].astype(jnp.float32))):
        for j, ch in enumerate(chunks(cols)):
            main_ref[base : base + own, :] = x[:, ch]
            base += own
            at = EDGE_ROWS + 2 * (f * (cols // LANES) + j)
            next_ref[at : at + 2, :] = x[own - 2 :, ch]
            prev_ref[at : at + 2, :] = x[:2, ch]


EDGE_ROWS = 16


def pack(pressure, soil_class, classes, ground):
    layers, own, cols = pressure.shape
    f32 = jnp.float32
    rows = own + SUBS
    span = layers * rows
    edge = pltpu.VMEM((4 * cols // LANES, layers, LANES), f32)
    scratch = [pltpu.VMEM((layers, rows, LANES), f32)]
    width, more = span, []
    if ground:
        height = ground[0].shape[0]
        strip = pltpu.VMEM((EDGE_ROWS + 4 * cols // LANES, LANES), f32)
        more = [pltpu.VMEM((5 * height + 2 * own * cols // LANES, LANES), f32), strip, strip]
        tall = LANES + 5 * (height + SUBS)
        tall += -tall % LANES
        width += tall
        scratch.append(pltpu.VMEM((tall, LANES), f32))
    out = [pltpu.VMEM((SUBS, LANES), f32), pltpu.VMEM((SUBS, width), f32), edge, edge] + more
    given = 2 + len(ground)

    def body(*refs):
        tables, rest = refs[: len(classes)], refs[len(classes) :]
        fields, outs, boxes = rest[:given], rest[given : given + len(out)], rest[given + len(out) :]
        outs[1][:, :span] = soil_columns(*fields[:2], boxes[0])
        if ground:
            surface_rows(*fields, *outs[4:])
            outs[1][:, span:] = surface_columns(outs[4], boxes[1], height, own, cols)
        soil_rows(*fields[:2], *outs[2:4])
        outs[0][...] = class_tables(tables)

    vmem = pl.BlockSpec(memory_space=pltpu.VMEM)
    smem = pl.BlockSpec(memory_space=pltpu.SMEM)
    return pl.pallas_call(
        body,
        out_shape=out,
        in_specs=[smem] * len(classes) + [vmem] * given,
        scratch_shapes=scratch,
        name="pack",
    )(*classes, pressure, soil_class, *ground)


def corners_kernel(got, *refs, layers, own, cols, height):
    n = cols // LANES
    rows = own + SUBS
    span = layers * rows
    count = len(refs) // 2 - 1
    given, outs, (turn, box) = refs[:count], refs[count : 2 * count], refs[2 * count :]
    lane = lax.broadcasted_iota(jnp.int32, (layers, LANES), 1)
    turn[...] = jnp.zeros_like(turn)
    turn[:SUBS, :] = got[...]
    turned = turn[...].T
    box[...] = turned[:span].reshape(layers, rows, LANES)
    for i, row in ((0, own + 1), (1, 2)):
        x = box[:, row, :]
        outs[i][: 4 * n] = given[i][...]
        found = jnp.zeros_like(x)
        for f in range(2):
            left, right = pltpu.roll(x, LANES - 2 - 3 * f, 1), pltpu.roll(x, LANES - 4 - f, 1)
            found = jnp.where(lane == LANES - 1 - f, left, jnp.where(lane == f, right, found))
        outs[i][4 * n] = found
    if count == 2:
        return
    moved = pltpu.roll(turned[span:], LANES - 3, 1)
    lane = lax.broadcasted_iota(jnp.int32, (3, LANES), 1)
    tall = height + SUBS
    for i in range(2):
        out = outs[2 + i]
        base = given[2 + i].shape[0]
        out[:base, :] = given[2 + i][...]
        out[base:, :] = jnp.zeros((out.shape[0] - base, LANES), jnp.float32)
        for f in range(5):
            at = LANES + f * tall + (height - 3 if i == 0 else 0)
            out[base + 3 * f : base + 3 * f + 3, :] = jnp.where((lane < 3) | (lane >= LANES - 3), moved[at : at + 3], 0.0)
        for f in range(2):
            at = own - 2 if i == 0 else 0
            left, right = moved[2 * f * SUBS + at :][:2], moved[2 * (2 + f) * SUBS + at :][:2]
            out[base + 16 + 2 * f : base + 18 + 2 * f, :] = rim(left, right, lane[:2], 2)


CORNERS = 24


def corners(got, layers, own, cols, height, rows, strips):
    f32 = jnp.float32

    def body(*refs):
        corners_kernel(*refs, layers=layers, own=own, cols=cols, height=height)

    return pl.pallas_call(
        body,
        out_shape=[pltpu.VMEM((4 * cols // LANES + 1, layers, LANES), f32)] * 2
        + [pltpu.VMEM((x.shape[0] + CORNERS, LANES), f32) for x in strips],
        scratch_shapes=[pltpu.VMEM((LANES, got.shape[1]), f32), pltpu.VMEM((layers, own + SUBS, LANES), f32)],
        name="corners",
    )(*near(got, *rows, *strips))


def surface_columns(main_ref, box, height, own, cols):
    n = cols // LANES
    tall = height + SUBS
    box[...] = jnp.zeros_like(box)
    for side, j in enumerate((n - 1, 0)):
        for f in range(2):
            at = (2 * side + f) * 2 * SUBS
            src = 5 * height + (f * n + j) * own
            box[at : at + own, :] = main_ref[src : src + own, :]
    for f in range(5):
        at = LANES + f * tall
        box[at : at + height, :] = main_ref[f * height : (f + 1) * height, :]
    turned = box[...].T
    edges = jnp.concatenate([turned[LANES - 3 :], turned[:3], jnp.zeros((2, turned.shape[1]), jnp.float32)], axis=0)
    return edges


def rim(at_end, at_start, lane, count):
    return jnp.where(lane >= LANES - count, at_end, jnp.where(lane < count, at_start, 0.0))


def ring(before, after, sub):
    return jnp.where(sub >= SUBS - 3, before, jnp.where(sub < 3, after, 0.0))


WINDOW = 136


def windows_kernel(main, above, below, got, sent, *refs, span, height, own, count):
    outs, (tall, wide_top, ends, turn, flat) = refs[:count], refs[count:]
    line = lax.axis_index("gy")
    lane = lax.broadcasted_iota(jnp.int32, (SUBS, LANES), 1)
    sub = lax.broadcasted_iota(jnp.int32, (SUBS, LANES), 0)
    tall[...] = jnp.zeros_like(tall)
    ends[...] = jnp.zeros_like(ends)
    turn[...] = jnp.zeros_like(turn)
    for f in range(5):
        tall[f, SUBS : SUBS + height] = main[f * height : (f + 1) * height, :]
        tall[f, SUBS - 3 : SUBS] = above[3 * f : 3 * f + 3, :]
        tall[f, SUBS + height : SUBS + height + 3] = below[3 * f : 3 * f + 3, :]
    turn[LANES - 3 :, :] = got[:3, span : span + LANES]
    turn[:3, :] = got[3:6, span : span + LANES]
    block = turn[...].T
    last = line == count - 1
    for f in range(2):
        before, after = block[2 * f * SUBS :], block[2 * (2 + f) * SUBS :]
        spot = above.shape[0] - CORNERS + 16 + 2 * f
        beside = rim(before[:SUBS], after[:SUBS], lane, 2)
        beyond = jnp.where(last, above[spot : spot + 2, :], below[spot : spot + 2, :])
        for j in (0, count + 1):
            wide_top[f, j] = beside
            ends[j, 2 * f : 2 * f + 2] = beyond
        for j in range(count):
            src = 5 * height + (f * count + j) * own
            wide_top[f, j + 1] = main[src : src + own, :]
            at = EDGE_ROWS + 2 * (f * count + j)
            ends[j + 1, 2 * f : 2 * f + 2] = jnp.where(last, above[at : at + 2, :], below[at : at + 2, :])
    edges = []
    for source, base in ((got, above.shape[0] - CORNERS), (sent, 0)):
        flat[...] = jnp.zeros_like(flat)
        for f in range(5):
            at = f * (height + SUBS) + height
            flat[at : at + 3, :] = below[base + 3 * f : base + 3 * f + 3, :]
            flat[at + SUBS - 3 : at + SUBS, :] = above[base + 3 * f : base + 3 * f + 3, :]
        turned = flat[...].T
        edges.append((source[:3, span + LANES :] + turned[LANES - 3 :], source[3:6, span + LANES :] + turned[:3]))
    before = jnp.where(last, edges[0][0], edges[1][0])
    after = jnp.where(line == 0, edges[0][1], edges[1][1])
    for s in range(count):
        who, out = (line + s) % count, outs[s]
        for f in range(5):
            first = pl.multiple_of(who * SUBS, SUBS)
            out[2 * f * SUBS : (2 * f + 1) * SUBS, :] = tall[f, pl.ds(first + SUBS, SUBS), :]
            out[(2 * f + 1) * SUBS : (2 * f + 2) * SUBS, :] = ring(
                tall[f, pl.ds(first, SUBS), :], tall[f, pl.ds(first + 2 * SUBS, SUBS), :], sub
            )
        for f in range(2):
            out[(10 + f) * SUBS : (11 + f) * SUBS, :] = wide_top[f, who + 1]
            out[(12 + f) * SUBS : (13 + f) * SUBS, :] = rim(wide_top[f, who], wide_top[f, who + 2], lane, 2)
        mid, side = ends[who + 1], rim(ends[who], ends[who + 2], lane, 2)
        out[14 * SUBS : 14 * SUBS + 4, :] = mid[:4]
        out[14 * SUBS + 4 : 15 * SUBS, :] = side[:4]
        for j in range(2):
            at = (15 + j) * SUBS
            out[at : at + 3, :] = before[:, j * LANES : (j + 1) * LANES]
            out[at + 3 : at + 6, :] = after[:, j * LANES : (j + 1) * LANES]
            out[at + 6 : at + SUBS, :] = jnp.zeros((2, LANES), jnp.float32)


def windows(main, above, below, got, sent, span, height, own, count):
    def body(*refs):
        windows_kernel(*refs, span=span, height=height, own=own, count=count)

    return pl.pallas_call(
        body,
        out_shape=[pltpu.VMEM((WINDOW, LANES), jnp.float32)] * count,
        scratch_shapes=[
            pltpu.VMEM((5, height + 2 * SUBS, LANES), jnp.float32),
            pltpu.VMEM((2, count + 2, own, LANES), jnp.float32),
            pltpu.VMEM((count + 2, SUBS, LANES), jnp.float32),
            pltpu.VMEM((LANES, LANES), jnp.float32),
            pltpu.VMEM((2 * LANES, LANES), jnp.float32),
        ],
        name="windows",
    )(*near(main, above, below, got, sent))


def assemble(main, above, below, sent, strip, tile, tops, turn, flat, own):
    count = len(sent)
    line = lax.axis_index("gy")
    _, _, width = strip.shape
    _, rows, _ = tile.shape
    cols, height = width - LANES, rows - SUBS
    sub = lax.broadcasted_iota(jnp.int32, (SUBS, LANES), 0)
    turn[...] = jnp.zeros_like(turn)
    tops[:, height:, :] = jnp.zeros((2, SUBS, 2 * LANES), jnp.float32)
    for f in range(5):
        tile[f, height:, :LANES] = jnp.zeros((SUBS, LANES), jnp.float32)
        tile[f, :height, :LANES] = main[f * height : (f + 1) * height, :]
        tile[f, height : height + 3, :LANES] = below[3 * f : 3 * f + 3, :]
        tile[f, rows - 3 :, :LANES] = above[3 * f : 3 * f + 3, :]
    for s in range(count):
        part = sent[s]
        who = (line - s) % count
        at = pl.multiple_of(who * LANES, LANES)
        first = pl.multiple_of(who * own, own)
        for f in range(5):
            strip[f, :, pl.ds(at, LANES)] = part[2 * f * SUBS : (2 * f + 2) * SUBS, :]
        for f in range(2):
            tops[f, pl.ds(first, own), :LANES] = part[(10 + f) * SUBS : (11 + f) * SUBS, :]
            tops[f, pl.ds(first, own), LANES:] = part[(12 + f) * SUBS : (13 + f) * SUBS, :]

        @pl.when(who == 0)
        def _(part=part):
            for f in range(2):
                tops[f, height : height + 2, :LANES] = part[14 * SUBS + 2 * f : 14 * SUBS + 2 * f + 2, :]
                tops[f, height : height + 2, LANES:] = part[14 * SUBS + 4 + 2 * f : 14 * SUBS + 6 + 2 * f, :]
            for j in range(2):
                turn[0, :3, j * LANES : (j + 1) * LANES] = part[(15 + j) * SUBS + 3 : (15 + j) * SUBS + 6, :]

        @pl.when(who == count - 1)
        def _(part=part):
            for f in range(2):
                tops[f, rows - 2 :, :LANES] = part[14 * SUBS + 2 * f : 14 * SUBS + 2 * f + 2, :]
                tops[f, rows - 2 :, LANES:] = part[14 * SUBS + 4 + 2 * f : 14 * SUBS + 6 + 2 * f, :]
            for j in range(2):
                turn[0, LANES - 3 :, j * LANES : (j + 1) * LANES] = part[(15 + j) * SUBS : (15 + j) * SUBS + 3, :]

    for j in range(2):
        cut = slice(j * LANES, (j + 1) * LANES)
        turn[1, LANES - 3 :, cut] = sent[1 % count][(15 + j) * SUBS : (15 + j) * SUBS + 3, :]
        turn[1, :3, cut] = sent[-1][(15 + j) * SUBS + 3 : (15 + j) * SUBS + 6, :]
    beside = turn[1].T
    flat[...] = turn[0].T
    first = pl.multiple_of(line * own, SUBS)
    before = pl.multiple_of(jnp.where(line > 0, line * own - SUBS, height), SUBS)
    for f in range(5):
        tile[f, :, LANES:] = beside[f * rows : (f + 1) * rows]
        strip[f, :own, cols:] = flat[pl.ds(first + f * rows, SUBS), :]
        strip[f, own:, cols:] = ring(flat[pl.ds(before + f * rows, SUBS), :], flat[pl.ds(first + f * rows + SUBS, SUBS), :], sub)


def flow(fields, top, conduct, row_flags, col_flags, own_rows, own_cols):
    water, level, convey, land, rain = fields
    rows, width = water.shape
    r = lax.broadcasted_iota(jnp.int32, (rows, width), 0)
    c = lax.broadcasted_iota(jnp.int32, (rows, width), 1)
    row_ok = jnp.where(r < own_rows, 1, jnp.where(r >= rows - 3, row_flags[0], jnp.where(r < own_rows + 3, row_flags[1], 0)))
    col_ok = jnp.where(c < own_cols, 1, jnp.where(c >= width - 3, col_flags[0], jnp.where(c < own_cols + 3, col_flags[1], 0)))
    root = jnp.sqrt(convey) * (row_ok * col_ok).astype(jnp.float32)
    leak = land * conduct
    ahead = [lambda x: pltpu.roll(x, rows - 1, 0), lambda x: pltpu.roll(x, width - 1, 1)]
    gates = [root * f(root) for f in ahead]
    exchange = jnp.zeros_like(water)
    for _ in range(PASSES):
        surface = level + water
        power = jnp.where(water > 0.0, jnp.exp2((5.0 / 3.0) * jnp.log2(jnp.maximum(water, 1e-30))), 0.0)
        outflow = jnp.zeros_like(water)
        for axis in range(2):
            slope = surface - ahead[axis](surface)
            carried = jnp.where(slope >= 0.0, power, ahead[axis](power))
            flux = gates[axis] * carried * slope * lax.rsqrt(jnp.maximum(jnp.abs(slope), SLOPE_FLOOR))
            outflow = outflow + flux - pltpu.roll(flux, 1, axis)
        rate = leak * (water - top)
        exchange = exchange + SURFACE_STEP * rate
        water = jnp.maximum(water + SURFACE_STEP * (rain - rate - outflow), 0.0)
    return water, exchange


def last_kernel(tab_ref, strip, tile, tops, top_ref, class_ref, next_ref, head_out, water_out, new_ref, water_ref, sem):
    own = new_ref.shape[1]
    _, rows, width = strip.shape
    cols = width - LANES
    height, across = water_ref.shape
    ok = place()
    group, groups = lax.axis_index("grp"), lax.axis_size("grp")
    column = lax.axis_index("gx") * lax.axis_size("gy") + lax.axis_index("gy")
    columns_all = lax.axis_size("gx") * lax.axis_size("gy")

    def flags(*tests):
        return [jnp.where(t, 1, 0) for t in tests]

    roots = [closure(params(tab_ref, tops[1, :, ch].astype(jnp.int32)), tops[0, :, ch])[2] for ch in chunks(tile.shape[2])]
    root = jnp.concatenate(roots, axis=1)
    water, _ = flow(
        [tile[f] for f in range(5)], tops[0], 0.25 * root * root,
        flags(group > 0, group < groups - 1), flags(column > 0, column < columns_all - 1), height, across,
    )
    water_ref[...] = water[:height, :across]
    done = pltpu.make_async_copy(water_ref, water_out, sem.at[1])
    done.start()
    root = top_ref[4]
    _, gain = flow([strip[f] for f in range(5)], top_ref[3], 0.25 * root * root, ok[:2], ok[2:], own, cols)
    mask = soil_mask(ok, rows, width, own, cols)
    p = top_ref[0] + gain * top_ref[1]
    content, capacity, root = wide([closure(params(tab_ref, class_ref[:, ch]), p[:, ch]) for ch in chunks(width)])
    h = root * mask
    q = h * p
    low, low_q, low_n, low_d, weights, flows = (next_ref[i] for i in range(6))

    def inner(x):
        return x[:own, :cols]

    top_n = inner(capacity * p - (content - top_ref[2]) + gain + h * lateral(q)) + inner(h) * (low_q - GRAVITY_STEP * low)
    new_ref[0] = top_n / (inner(capacity + h * lateral(h)) + inner(h) * low)
    low_n = low_n + low * (flows + inner(q) + GRAVITY_STEP * inner(h))
    new_ref[1] = low_n / (low_d + low * (weights + inner(h)))
    copy = pltpu.make_async_copy(new_ref, head_out.at[:TOP_LAYERS], sem.at[0])
    copy.start()
    done.wait()
    copy.wait()


def finish(tables, fields, tops, head, water, count):
    _, own, cols = head.shape
    height, across = water
    whole = count == 0
    rows, width, high, broad = own + SUBS, cols + LANES, height + SUBS, across + LANES
    n = len(fields)

    def body(*refs):
        tab_ref, given, known, (head_out, water_ref) = refs[0], refs[1 : 1 + n], refs[1 + n : 4 + n], refs[5 + n : 7 + n]
        rest = refs[7 + n :]
        if whole:
            strip, tile, above = given
        else:
            strip, tile, above = rest[3:6]
            assemble(*given[:3], given[3:], strip, tile, above, *rest[6:], own)
        last_kernel(tab_ref, strip, tile, above, *known, head_out, water_ref, *rest[:3])

    vmem = pl.BlockSpec(memory_space=pltpu.VMEM)
    scratch = [pltpu.VMEM((TOP_LAYERS, own, cols), jnp.float32), pltpu.VMEM(water, jnp.float32), pltpu.SemaphoreType.DMA((2,))]
    if not whole:
        scratch += [
            pltpu.VMEM(shape, jnp.float32)
            for shape in ((5, rows, width), (5, high, broad), (2, high, broad), (2, LANES, 2 * LANES), (2 * LANES, LANES))
        ]
    return pl.pallas_call(
        body,
        out_shape=(jax.ShapeDtypeStruct(head.shape, jnp.float32), jax.ShapeDtypeStruct(water, jnp.float32)),
        in_specs=[vmem] * (n + 4) + [pl.BlockSpec(memory_space=pl.ANY)],
        out_specs=[pl.BlockSpec(memory_space=pl.ANY)] * 2,
        scratch_shapes=scratch,
        input_output_aliases={n + 4: 0},
        name="surface_and_top",
    )(*near(tables, *fields, *tops), head)


def lane_rows(size):
    return -(-size // LANES)


def as_lanes(x):
    if x.shape[-1] % LANES:
        x = jnp.pad(x.reshape(-1), (0, -x.size % LANES))
    return x.reshape(-1, LANES)


def from_lanes(x, shape):
    if shape[-1] % LANES:
        size = 1
        for length in shape:
            size *= length
        x = x.reshape(-1)[:size]
    return x.reshape(shape)


def gx_trade(edges, half):
    got = shift(edges, "gx", 1)
    if lax.axis_size("gx") == 2:
        return got
    return jnp.where(half, got, shift(edges, "gx", -1))


def cyclic_rows(mid, above, below, gap):
    hole = jnp.zeros(mid.shape[:-2] + (gap, mid.shape[-1]), mid.dtype)
    return jnp.concatenate([mid, below, hole, above], axis=-2)


def block_general(pressure, soil_class, depth, elevation, roughness, rain, land_mask, channel_mask):
    ny = lax.axis_size("gy")
    _, own, cols = pressure.shape
    srows, scols = depth.shape
    convey = (1.0 + channel_mask.astype(jnp.float32)) / roughness
    surf = jnp.stack([depth, elevation, convey, LEAKANCE * land_mask.astype(jnp.float32), rain])
    tops = jnp.stack([pressure[0], soil_class[0].astype(jnp.float32)])

    def pack(s, t):
        return jnp.concatenate([as_lanes(s), as_lanes(t)], axis=0)

    def unpack(m):
        cut = lane_rows(15 * scols)
        return from_lanes(m[:cut], (5, 3, scols)), from_lanes(m[cut:], (2, 2, cols))

    s_above, t_above = unpack(shift(pack(surf[:, -3:], tops[:, -2:]), "grp", 1))
    s_below, t_below = unpack(shift(pack(surf[:, :3], tops[:, :2]), "grp", -1))
    surf_rows = cyclic_rows(surf, s_above, s_below, 2)
    tops_rows = jnp.concatenate([tops, t_below, t_above], axis=1)

    def edges(cut):
        a = surf_rows[:, :, cut(3)].transpose(0, 2, 1).reshape(15, -1)
        b = tops_rows[:, :, cut(2)].transpose(0, 2, 1).reshape(4, -1)
        return jnp.concatenate([a, jnp.pad(b, ((0, 0), (0, a.shape[1] - b.shape[1])))], axis=0)

    out = jnp.concatenate([edges(lambda n: slice(-n, None)), edges(lambda n: slice(0, n))])
    got = gx_trade(out, lax.broadcasted_iota(jnp.int32, out.shape, 0) < 19)
    mine = jnp.concatenate(
        [as_lanes(surf_rows), as_lanes(tops_rows), jnp.pad(got, ((0, 0), (0, -got.shape[1] % LANES))).reshape(-1, LANES)]
    )
    every = lax.all_gather(mine, "gy", axis=0, tiled=False)
    n1 = lane_rows(surf_rows.size)
    n2 = n1 + lane_rows(tops_rows.size)
    e_surf = jax.vmap(lambda m: from_lanes(m, (5, srows + SUBS, scols)))(every[:, :n1])
    e_surf = e_surf.transpose(1, 2, 0, 3).reshape(5, srows + SUBS, ny * scols)
    e_tops = every[:, n1:n2].reshape(ny, 2, own + 4, cols)
    e_m = every[:, n2:].reshape(ny, 2, 19, -1)
    main = e_tops[:, :, :own].transpose(1, 0, 2, 3).reshape(2, srows, cols)
    zeros = jnp.zeros((2, 4, cols), jnp.float32)
    f_tops = jnp.concatenate([main, e_tops[0, :, own : own + 2], zeros, e_tops[-1, :, own + 2 :]], axis=1)
    height = srows + SUBS
    c_left = e_m[-1, 0, :15, :height].reshape(5, 3, height).transpose(0, 2, 1)
    c_right = e_m[0, 1, :15, :height].reshape(5, 3, height).transpose(0, 2, 1)
    hole = jnp.zeros((5, height, LANES - 6), jnp.float32)
    blocks = jnp.concatenate([e_surf, c_right, hole, c_left], axis=2)

    def tops_edge(side):
        t = e_m[:, side, 15:, : own + 4].reshape(ny, 2, 2, own + 4)
        mid = t[..., :own].transpose(1, 0, 3, 2).reshape(2, srows, 2)
        low = t[0, :, :, own : own + 2].transpose(0, 2, 1)
        high = t[-1, :, :, own + 2 :].transpose(0, 2, 1)
        return jnp.concatenate([mid, low, jnp.zeros((2, 4, 2), jnp.float32), high], axis=1)

    top_blocks = jnp.concatenate(
        [f_tops, tops_edge(1), jnp.zeros((2, height, LANES - 4), jnp.float32), tops_edge(0)], axis=2
    )
    line = lax.axis_index("gy")

    def around(first, length, total, room):
        spot = jnp.arange(room)
        return (first + jnp.where(spot < length + 3, spot, spot - room)) % total

    strip = jnp.take(blocks, around(line * own, own, height, own + SUBS), axis=1)
    across = around(line * scols, scols, cols + LANES, -(-(scols + 6) // LANES) * LANES)
    return strip, jnp.take(blocks, across, axis=2), jnp.take(top_blocks, across, axis=2)


def local(
    pressure, soil_class, capacity_range, inverse_entry, shape_index, conductivity,
    depth, elevation, roughness, rain, land_mask, channel_mask,
):
    ny = lax.axis_size("gy")
    _, own, cols = pressure.shape
    srows, scols = depth.shape
    ground = (depth, elevation, roughness, rain, land_mask, channel_mask)
    classes = (capacity_range, inverse_entry, shape_index, conductivity)
    even = scols == LANES and own == SUBS
    tables, sent, *packed = pack(pressure, soil_class, classes, ground if even else ())
    span = pressure.shape[0] * (own + SUBS)
    half = jnp.where(lax.broadcasted_iota(jnp.int32, sent.shape, 1) < span, 4, 3)
    got = gx_trade(sent, lax.broadcasted_iota(jnp.int32, sent.shape, 0) < half)
    after, before, *strips = corners(got, pressure.shape[0], own, cols, srows, packed[:2], packed[3:])
    rows = ("grp", "gy")
    up = shift(after, rows, 1)
    down = shift(before, rows, -1)
    if even:
        above = shift(strips[0], "grp", 1)
        below = shift(strips[1], "grp", -1)
        main = packed[2]
        outs = windows(main, above, below, got, sent, span, srows, own, ny)
        fields = [main, above, below, outs[0]] + [shift(outs[step], "gy", step) for step in range(1, ny)]
    else:
        fields = block_general(pressure, soil_class, *ground)
    head, *tops = soil_interior(tables, pressure, soil_class, up, down, got, sent)
    return finish(tables, fields, tops, head, (srows, scols), ny if even else 0)


def solution(mesh):
    soil = P(None, ("grp", "gy"), "gx")
    ground = P("grp", ("gx", "gy"))

    return jax.shard_map(
        local,
        mesh=mesh,
        in_specs=(soil, soil, P(), P(), P(), P()) + (ground,) * 6,
        out_specs=(soil, ground),
        check_vma=False,
    )
```
